16 devices in a mesh: col: 2 (over z), row: 8 (over y, x, core).
Axes of the slice: x: 2, y: 2, z: 2, core: 2. Of those that a mesh axis runs over, the one named last changes fastest.
Arguments:
- vel_u: float32 [31, 256, 1024], P(None, 'row', 'col')
- vel_v: float32 [31, 256, 1024], P(None, 'row', 'col')
- temperature: float32 [31, 256, 1024], P(None, 'row', 'col')
- salinity: float32 [31, 256, 1024], P(None, 'row', 'col')
- surf_eta: float32 [256, 1024], P('row', 'col')
- trans_u: float32 [256, 1024], P('row', 'col')
- trans_v: float32 [256, 1024], P('row', 'col')
- bottom_depth: float32 [256, 1024], P('row', 'col')
- level_count: int32 [256, 1024], P('row', 'col')
- avg_weights: float32 [30], replicated
Outputs:
- output 1: float32 [256, 1024], P('row', 'col')
- output 2: float32 [256, 1024], P('row', 'col')
- output 3: float32 [256, 1024], P('row', 'col')
- output 4: float32 [31, 256, 1024], P(None, 'row', 'col')
- output 5: float32 [31, 256, 1024], P(None, 'row', 'col')
- output 6: float32 [31, 256, 1024], P(None, 'row', 'col')
- output 7: float32 [31, 256, 1024], P(None, 'row', 'col')
All inputs are finite; a program needn't handle non-finite values.
Results may differ from the reference program's by a relative error of at most 0.001.
Values sent between devices are 32-bit elements.
A program may use at most 1 GiB of HBM per device.

```python
import jax
import jax.numpy as jnp
from jax import lax

LEVELS = 31
SUBCYCLES = 30
GRID_Y = 256
GRID_X = 1024

TIME_STEP = 1.0
GRAVITY = 16.0
BC_GRAVITY = 4.0
EXPAND_T = 0.2
CONTRACT_S = 0.6
CORIO_F0 = 0.4
CORIO_BETA = 0.4
VISC_R = 2.0
DIFF_R = 0.5


def setup_inputs(seed: int = 0) -> dict:
    keys = jax.random.split(jax.random.key(seed), 10)
    shape3 = (LEVELS, GRID_Y, GRID_X)
    shape2 = (GRID_Y, GRID_X)
    north_open = (jnp.arange(GRID_Y) < GRID_Y - 1).astype(jnp.float32)[:, None]
    vel_u = 0.3 * jax.random.normal(keys[0], shape3, jnp.float32)
    vel_v = 0.3 * jax.random.normal(keys[1], shape3, jnp.float32) * north_open
    temperature = jax.random.normal(keys[2], shape3, jnp.float32)
    salinity = 0.5 * jax.random.normal(keys[3], shape3, jnp.float32)
    surf_eta = 0.1 * jax.random.normal(keys[4], shape2, jnp.float32)
    trans_u = 0.3 * jax.random.normal(keys[5], shape2, jnp.float32)
    trans_v = 0.3 * jax.random.normal(keys[6], shape2, jnp.float32) * north_open
    bottom_depth = jax.random.uniform(keys[7], shape2, jnp.float32, 0.5, 1.5)
    level_count = jax.random.randint(keys[8], shape2, 1, LEVELS + 1, dtype=jnp.int32)
    level_count = level_count.at[0, 0].set(1).at[0, 1].set(LEVELS)
    ramp = (jnp.arange(SUBCYCLES) + 1.0) / SUBCYCLES
    raw_weights = ramp * jax.random.uniform(keys[9], (SUBCYCLES,), jnp.float32, 0.5, 1.5)
    avg_weights = raw_weights / jnp.sum(raw_weights)
    return {'vel_u': vel_u, 'vel_v': vel_v, 'temperature': temperature, 'salinity': salinity, 'surf_eta': surf_eta, 'trans_u': trans_u, 'trans_v': trans_v, 'bottom_depth': bottom_depth, 'level_count': level_count, 'avg_weights': avg_weights}


def pad_halo(field):
    wrapped = jnp.concatenate([field[..., -1:], field, field[..., :1]], axis=-1)
    ghost = jnp.zeros_like(wrapped[..., :1, :])
    return jnp.concatenate([ghost, wrapped, ghost], axis=-2)


def shifted(padded, step_y, step_x):
    n_rows = padded.shape[-2] - 2
    n_cols = padded.shape[-1] - 2
    return padded[..., 1 + step_y:1 + step_y + n_rows, 1 + step_x:1 + step_x + n_cols]


def tri_solve(right_side, active, strength):
    link = strength * active[1:]
    zero_row = jnp.zeros_like(right_side[:1])
    low_links = jnp.concatenate([zero_row, link], axis=0)
    up_links = jnp.concatenate([link, zero_row], axis=0)

    def down(carry, level):
        ratio_prev, value_prev = carry
        low_link, up_link, target = level
        denominator = 1.0 + low_link + up_link + low_link * ratio_prev
        ratio = -up_link / denominator
        value = (target + low_link * value_prev) / denominator
        return (ratio, value), (ratio, value)

    start = (jnp.zeros_like(right_side[0]), jnp.zeros_like(right_side[0]))
    _, (ratios, values) = lax.scan(down, start, (low_links, up_links, right_side))

    def back(below, level):
        ratio, value = level
        solved = value - ratio * below
        return solved, solved

    _, solved_all = lax.scan(back, jnp.zeros_like(right_side[0]), (ratios, values), reverse=True)
    return solved_all


def ocean_columns(u_pad, v_pad, temperature_pad, salinity_pad, count_pad, depth_pad, coriolis_u, coriolis_v):
    n_levels = u_pad.shape[0]
    count_mid = shifted(count_pad, 0, 0)
    levels_u = jnp.minimum(count_mid, shifted(count_pad, 0, 1))
    levels_uw = jnp.minimum(shifted(count_pad, 0, -1), count_mid)
    levels_v = jnp.minimum(count_mid, shifted(count_pad, 1, 0))
    levels_vs = jnp.minimum(shifted(count_pad, -1, 0), count_mid)
    level_index = jnp.arange(n_levels)[:, None, None]
    mask_mid = (level_index < count_mid).astype(jnp.float32)
    mask_u = (level_index < levels_u).astype(jnp.float32)
    mask_uw = (level_index < levels_uw).astype(jnp.float32)
    mask_v = (level_index < levels_v).astype(jnp.float32)
    mask_vs = (level_index < levels_vs).astype(jnp.float32)
    u_mid = shifted(u_pad, 0, 0)
    v_mid = shifted(v_pad, 0, 0)
    u_west = shifted(u_pad, 0, -1)
    v_south = shifted(v_pad, -1, 0)
    v_at_u = 0.25 * (v_mid + shifted(v_pad, 0, 1) + v_south + shifted(v_pad, -1, 1))
    u_at_v = 0.25 * (u_mid + u_west + shifted(u_pad, 1, 0) + shifted(u_pad, 1, -1))
    inertia_u = 0.5 * (u_mid * (shifted(u_pad, 0, 1) - u_west) + v_at_u * (shifted(u_pad, 1, 0) - shifted(u_pad, -1, 0)))
    inertia_v = 0.5 * (u_at_v * (shifted(v_pad, 0, 1) - shifted(v_pad, 0, -1)) + v_mid * (shifted(v_pad, 1, 0) - v_south))
    density = CONTRACT_S * salinity_pad - EXPAND_T * temperature_pad
    pressure = (BC_GRAVITY / n_levels) * (jnp.cumsum(density, axis=0) - 0.5 * density)
    pressure_mid = shifted(pressure, 0, 0)
    u_star = u_mid + TIME_STEP * (coriolis_u * v_at_u - inertia_u - shifted(pressure, 0, 1) + pressure_mid)
    v_star = v_mid + TIME_STEP * (-coriolis_v * u_at_v - inertia_v - shifted(pressure, 1, 0) + pressure_mid)
    u_visc = tri_solve(u_star, mask_u, VISC_R)
    v_visc = tri_solve(v_star, mask_v, VISC_R)
    count_u = jnp.maximum(jnp.sum(mask_u, axis=0), 1.0)
    count_v = jnp.maximum(jnp.sum(mask_v, axis=0), 1.0)
    depth_mid = shifted(depth_pad, 0, 0)
    depth_u = 0.5 * (depth_mid + shifted(depth_pad, 0, 1))
    depth_v = 0.5 * (depth_mid + shifted(depth_pad, 1, 0))
    force_u = depth_u * jnp.sum(mask_u * (u_visc - u_mid), axis=0) / count_u / TIME_STEP
    force_v = depth_v * jnp.sum(mask_v * (v_visc - v_mid), axis=0) / count_v / TIME_STEP
    shear_u = u_visc - jnp.sum(mask_u * u_visc, axis=0) / count_u
    shear_v = v_visc - jnp.sum(mask_v * v_visc, axis=0) / count_v
    wet_u = (levels_u > 0).astype(jnp.float32)
    wet_v = (levels_v > 0).astype(jnp.float32)

    def advect(tracer_pad):
        tracer_mid = shifted(tracer_pad, 0, 0)
        flux_east = mask_u * u_mid * (tracer_mid + shifted(tracer_pad, 0, 1))
        flux_west = mask_uw * u_west * (shifted(tracer_pad, 0, -1) + tracer_mid)
        flux_north = mask_v * v_mid * (tracer_mid + shifted(tracer_pad, 1, 0))
        flux_south = mask_vs * v_south * (shifted(tracer_pad, -1, 0) + tracer_mid)
        return tracer_mid - 0.5 * TIME_STEP * (flux_east - flux_west + flux_north - flux_south)

    temperature_new = tri_solve(advect(temperature_pad), mask_mid, DIFF_R)
    salinity_new = tri_solve(advect(salinity_pad), mask_mid, DIFF_R)
    return (shear_u, shear_v, mask_u, mask_v, depth_u, depth_v, wet_u, wet_v, force_u, force_v, temperature_new, salinity_new)


def fast_update(stack_pad, force_u, force_v, depth_u, depth_v, wet_u, wet_v, coriolis_u, coriolis_v, dt_fast):
    eta_pad = stack_pad[0]
    trans_u_pad = stack_pad[1]
    trans_v_pad = stack_pad[2]
    eta_ext = eta_pad[1:, 1:] - dt_fast * (trans_u_pad[1:, 1:] - trans_u_pad[1:, :-1] + trans_v_pad[1:, 1:] - trans_v_pad[:-1, 1:])
    eta_new = eta_ext[:-1, :-1]
    trans_u_old = shifted(trans_u_pad, 0, 0)
    trans_v_old = shifted(trans_v_pad, 0, 0)
    v_at_u = 0.25 * (trans_v_old + shifted(trans_v_pad, 0, 1) + shifted(trans_v_pad, -1, 0) + shifted(trans_v_pad, -1, 1))
    u_at_v = 0.25 * (trans_u_old + shifted(trans_u_pad, 0, -1) + shifted(trans_u_pad, 1, 0) + shifted(trans_u_pad, 1, -1))
    trans_u_new = wet_u * (trans_u_old + dt_fast * (coriolis_u * v_at_u + force_u - GRAVITY * depth_u * (eta_ext[:-1, 1:] - eta_new)))
    trans_v_new = wet_v * (trans_v_old + dt_fast * (force_v - coriolis_v * u_at_v - GRAVITY * depth_v * (eta_ext[1:, :-1] - eta_new)))
    return eta_new, trans_u_new, trans_v_new


def reference(vel_u, vel_v, temperature, salinity, surf_eta, trans_u, trans_v, bottom_depth, level_count, avg_weights):
    n_rows = surf_eta.shape[0]
    dt_fast = TIME_STEP / avg_weights.shape[0]
    row_pos = jnp.arange(n_rows).astype(jnp.float32)[:, None]
    coriolis_u = CORIO_F0 + CORIO_BETA * ((row_pos + 0.5) / n_rows - 0.5)
    coriolis_v = CORIO_F0 + CORIO_BETA * ((row_pos + 1.0) / n_rows - 0.5)
    columns = ocean_columns(pad_halo(vel_u), pad_halo(vel_v), pad_halo(temperature), pad_halo(salinity), pad_halo(level_count), pad_halo(bottom_depth), coriolis_u, coriolis_v)
    shear_u, shear_v, mask_u, mask_v, depth_u, depth_v, wet_u, wet_v, force_u, force_v, temperature_new, salinity_new = columns

    def subcycle(carry, weight):
        eta_old, trans_u_old, trans_v_old, acc_u, acc_v = carry
        stack_pad = pad_halo(jnp.stack([eta_old, trans_u_old, trans_v_old]))
        eta_new, trans_u_new, trans_v_new = fast_update(stack_pad, force_u, force_v, depth_u, depth_v, wet_u, wet_v, coriolis_u, coriolis_v, dt_fast)
        return (eta_new, trans_u_new, trans_v_new, acc_u + weight * trans_u_new, acc_v + weight * trans_v_new), None

    zero_field = jnp.zeros_like(surf_eta)
    final, _ = lax.scan(subcycle, (surf_eta, trans_u, trans_v, zero_field, zero_field), avg_weights)
    eta_fin, trans_u_fin, trans_v_fin, bar_u, bar_v = final
    vel_u_new = mask_u * (shear_u + bar_u / depth_u)
    vel_v_new = mask_v * (shear_v + bar_v / depth_v)
    return (eta_fin, trans_u_fin, trans_v_fin, vel_u_new, vel_v_new, temperature_new, salinity_new)
```

```python
import functools

import jax
import jax.numpy as jnp
from jax import lax
from jax.experimental import pallas as pl
from jax.experimental.pallas import tpu as pltpu
from jax.sharding import PartitionSpec as P

TIME_STEP = 1.0
GRAVITY = 16.0
BC_GRAVITY = 4.0
EXPAND_T = 0.2
CONTRACT_S = 0.6
CORIO_F0 = 0.4
CORIO_BETA = 0.4
VISC_R = 2.0
DIFF_R = 0.5

MESH = pl.DeviceIdType.MESH
F32 = jnp.float32

SUB = 8
LANE = 128
ZERO = 0.0
ONE = 1.0
NL = 31
NR = 32
NT = 4
RO = 8
WO = 40
WR = 112
N_COPY = 25
VMEM_MAIN = 40 * 1024 * 1024
VMEM_FINISH = 12 * 1024 * 1024


def factors(strength):
    inner, last = [], []
    before = ZERO
    for level in range(NL):
        low = ZERO if level == 0 else strength
        inner.append(strength / (ONE + low + strength - low * before))
        last.append(strength / (ONE + low - low * before))
        before = inner[-1]
    return inner, last


VISC_IN, VISC_END = factors(VISC_R)
DIFF_IN, DIFF_END = factors(DIFF_R)


def lanes():
    return lax.broadcasted_iota(jnp.int32, (SUB, LANE), 1)


def west_of(own, left):
    return pltpu.roll(jnp.where(lanes() == 127, left, own), 1, 1)


def east_of(own, right):
    return pltpu.roll(jnp.where(lanes() == 0, right, own), 127, 1)


def corio(first, total_rows):
    pos = (first + lax.broadcasted_iota(jnp.int32, (SUB, LANE), 0)).astype(F32)
    fu = CORIO_F0 + CORIO_BETA * ((pos + 0.5) / total_rows - 0.5)
    fv = CORIO_F0 + CORIO_BETA * ((pos + ONE) / total_rows - 0.5)
    return fu, fv


def ocean_kernel(n_row, n_sub,
                 u_in, v_in, t_in, s_in, eta_in, tu_in, tv_in, dep_in, cnt_in,
                 us_o, vs_o, tn_o, sn_o, wide, abuf, lu_o, lv_o, hu_s, hv_s, mu_s, mv_s,
                 ub, vb, tb, sb, pb, wsend, cnt_i, pk_s, pk_r, asend,
                 in_sem, w_sem, send, recv):
    row = lax.axis_index('row')
    col = lax.axis_index('col')
    ocol = 1 - col
    has_s = row > 0
    has_n = row < n_row - 1
    dtb = TIME_STEP / n_sub
    total_rows = float(n_row * NR)

    def dev(step, c):
        return {'row': row + step, 'col': c}

    def remote(idx, src, dst, device):
        return pltpu.make_async_remote_copy(src, dst, send.at[idx], recv.at[idx], device_id=device, device_id_type=MESH)

    fields = ((u_in, ub), (v_in, vb), (t_in, tb), (s_in, sb))
    loads = {}
    for f in (0, 1, 2, 3):
        for t in (0, 3, 1, 2):
            src, dst = fields[f]
            loads[f, t] = pltpu.make_async_copy(src.at[:, :, pl.ds(LANE * t, LANE)], dst.at[t + 1, :, pl.ds(RO, NR), :], in_sem.at[f * 4 + t])
    wloads = {}
    for f, src in enumerate((eta_in, tu_in, tv_in, dep_in, cnt_in)):
        for t in range(NT):
            dst = wide.at[f, t, pl.ds(WO, NR), :] if f < 4 else cnt_i.at[t]
            wloads[f, t] = pltpu.make_async_copy(src.at[:, pl.ds(LANE * t, LANE)], dst, w_sem.at[f * 4 + t])
    for f in (4, 3, 0, 1, 2):
        for t in range(NT):
            wloads[f, t].start()
    for f in (0, 1, 2, 3):
        for t in (0, 3, 1, 2):
            loads[f, t].start()

    barrier = pltpu.get_barrier_semaphore()
    pl.semaphore_signal(barrier, inc=1, device_id=dev(0, ocol), device_id_type=MESH)

    @pl.when(has_n)
    def _():
        for c in (col, ocol):
            pl.semaphore_signal(barrier, inc=1, device_id=dev(1, c), device_id_type=MESH)

    @pl.when(has_s)
    def _():
        for c in (col, ocol):
            pl.semaphore_signal(barrier, inc=1, device_id=dev(-1, c), device_id_type=MESH)

    zero8 = jnp.zeros((SUB, LANE), F32)

    def fill(start3, start2, n2):
        def body3(i, _):
            t = i // NL
            k = lax.rem(i, NL)
            for buf in (ub, vb, tb, sb):
                buf[t, k, pl.ds(start3, SUB), :] = zero8
            return 0
        lax.fori_loop(0, 6 * NL, body3, 0)

        def body2(i, _):
            for f in range(5):
                for rr in range(n2):
                    wide[f, i, pl.ds(start2 + SUB * rr, SUB), :] = zero8
            for f in range(2):
                for rr in range(n2):
                    abuf[f, i, pl.ds(start2 + SUB * rr, SUB), :] = zero8
            return 0
        lax.fori_loop(0, 5, body2, 0)

    @pl.when(jnp.logical_not(has_s))
    def _():
        fill(0, SUB, 4)

    @pl.when(jnp.logical_not(has_n))
    def _():
        fill(40, 72, 4)

    for f in range(5):
        for t in range(5):
            wide[f, t, pl.ds(0, SUB), :] = zero8
            wide[f, t, pl.ds(104, SUB), :] = zero8

    for f in range(5):
        for t in range(NT):
            wloads[f, t].wait()
    for t in range(NT):
        for j in range(4):
            wide[4, t, pl.ds(WO + SUB * j, SUB), :] = cnt_i[t, pl.ds(SUB * j, SUB), :].astype(F32)
    half = lanes() < 64
    for f in range(5):
        for j in range(4):
            rows = pl.ds(WO + SUB * j, SUB)
            wsend[f, pl.ds(SUB * j, SUB), :] = jnp.where(half, wide[f, 0, rows, :], wide[f, 3, rows, :])

    for f in (0, 1, 2, 3):
        for t in (0, 3, 1, 2):
            loads[f, t].wait()
    bufs = (ub, vb, tb, sb)

    def pack(k, accs):
        out = []
        lane = lanes()
        for f in range(4):
            for e in range(2):
                acc = accs[f * 2 + e]
                for j in range(4):
                    slot = 4 * k + j
                    tile = bufs[f][1 + 3 * e, k, pl.ds(RO + SUB * j, SUB), :]
                    moved = pltpu.roll(tile, slot if e == 0 else slot + 1, 1)
                    acc = jnp.where(lane == slot, moved, acc)
                out.append(acc)
        return tuple(out)

    packed = lax.fori_loop(0, NL, pack, (zero8,) * SUB)
    for i in range(SUB):
        pk_s[i] = packed[i]

    barrier_count = 1 + 2 * has_n.astype(jnp.int32) + 2 * has_s.astype(jnp.int32)
    pl.semaphore_wait(barrier, barrier_count)

    east_w = [
        remote(0, pk_s, pk_r, dev(0, ocol)),
        remote(1, wsend, wide.at[:, 4, pl.ds(WO, NR), :], dev(0, ocol)),
    ]
    own4 = pl.ds(0, NT)
    mid4 = pl.ds(1, NT)

    def rows3(buf, a, b):
        return buf.at[mid4, :, pl.ds(a, 1), :], buf.at[mid4, :, pl.ds(b, 1), :]

    def rows2(f, nf, a, b, n):
        return wide.at[pl.ds(f, nf), own4, pl.ds(a, n), :], wide.at[pl.ds(f, nf), own4, pl.ds(b, n), :]

    to_n = [
        remote(2, *rows2(3, 2, WO + 24, WO - SUB, SUB), dev(1, col)),
        remote(3, *rows3(ub, 39, 7), dev(1, col)),
        remote(4, *rows3(vb, 39, 7), dev(1, col)),
        remote(16, vb.at[1, :, pl.ds(39, 1), :], vb.at[5, :, pl.ds(7, 1), :], dev(1, ocol)),
        remote(5, *rows3(tb, 39, 7), dev(1, col)),
        remote(6, *rows3(sb, 39, 7), dev(1, col)),
        remote(7, *rows2(3, 2, WO, WO - NR, 24), dev(1, col)),
        remote(SUB, *rows2(0, 3, WO, WO - NR, NR), dev(1, col)),
        remote(17, wsend, wide.at[:, 4, pl.ds(WO - NR, NR), :], dev(1, ocol)),
    ]
    to_s = [
        remote(9, *rows2(3, 2, WO, WO + NR, SUB), dev(-1, col)),
        remote(10, *rows3(ub, SUB, 40), dev(-1, col)),
        remote(11, *rows3(vb, SUB, 40), dev(-1, col)),
        remote(18, ub.at[4, :, pl.ds(SUB, 1), :], ub.at[0, :, pl.ds(40, 1), :], dev(-1, ocol)),
        remote(12, *rows3(tb, SUB, 40), dev(-1, col)),
        remote(13, *rows3(sb, SUB, 40), dev(-1, col)),
        remote(14, *rows2(3, 2, WO + SUB, WO + 40, 24), dev(-1, col)),
        remote(15, *rows2(0, 3, WO, WO + NR, NR), dev(-1, col)),
        remote(19, wsend, wide.at[:, 4, pl.ds(WO + NR, NR), :], dev(-1, ocol)),
    ]
    for cp in east_w:
        cp.start()

    @pl.when(has_n)
    def _():
        for cp in to_n:
            cp.start()

    @pl.when(has_s)
    def _():
        for cp in to_s:
            cp.start()

    p_unit = 0.5 * BC_GRAVITY / NL

    def pressure(t, start):
        rows = pl.ds(start, SUB)
        total = zero8
        for k in range(NL):
            part = (p_unit * CONTRACT_S) * sb[t, k, rows, :] - (p_unit * EXPAND_T) * tb[t, k, rows, :]
            here = total + part
            pb[t, k, rows, :] = here
            total = here + part

    def pressure_own(i, _):
        pressure(1 + i // 4, pl.multiple_of(RO + SUB * lax.rem(i, 4), SUB))
        return 0
    lax.fori_loop(0, 16, pressure_own, 0)

    for cp in east_w:
        cp.wait_recv()

    def unpack(k, _):
        for f in range(4):
            for e in range(2):
                got = pk_r[f * 2 + e]
                for j in range(4):
                    slot = 4 * k + j
                    if e == 0:
                        bufs[f][5, k, pl.ds(RO + SUB * j, SUB), :] = pltpu.roll(got, LANE - slot, 1)
                    else:
                        bufs[f][0, k, pl.ds(RO + SUB * j, SUB), :] = pltpu.roll(got, 127 - slot, 1)
        return 0
    lax.fori_loop(0, NL, unpack, 0)

    def pressure_east(i, _):
        pressure(5, pl.multiple_of(RO + SUB * i, SUB))
        return 0
    lax.fori_loop(0, 4, pressure_east, 0)

    def near2d(f, t, j):
        c = wide[f, t, pl.ds(WO + SUB * j, SUB), :]
        e = east_of(c, wide[f, t + 1, pl.ds(WO + SUB * j, SUB), :])
        n = wide[f, t, pl.ds(WO + 1 + SUB * j, SUB), :]
        return c, e, n

    def momentum(lt, j):
        rc, rn, rs = pl.ds(RO + SUB * j, SUB), pl.ds(RO + 1 + SUB * j, SUB), pl.ds(RO - 1 + SUB * j, SUB)
        ro = pl.ds(SUB * j, SUB)
        t = lt + 1
        fu, fv = corio(row * NR + SUB * j, total_rows)
        fu4 = 0.25 * fu
        fv4 = 0.25 * fv
        c0, ce, cn = near2d(4, lt, j)
        lu = jnp.minimum(c0, ce)
        lv = jnp.minimum(c0, cn)
        d0, de, dn = near2d(3, lt, j)
        hu = 0.5 * (d0 + de)
        hv = 0.5 * (d0 + dn)
        lu_o[lt, ro, :] = lu
        lv_o[lt, ro, :] = lv
        hu_s[lt, ro, :] = hu
        hv_s[lt, ro, :] = hv
        yu, yv = zero8, zero8
        su, sv = zero8, zero8
        for k in range(NL):
            u = ub[t, k, rc, :]
            v = vb[t, k, rc, :]
            uw = west_of(u, ub[t - 1, k, rc, :])
            ue = east_of(u, ub[t + 1, k, rc, :])
            un = ub[t, k, rn, :]
            us = ub[t, k, rs, :]
            unw = west_of(un, ub[t - 1, k, rn, :])
            vw = west_of(v, vb[t - 1, k, rc, :])
            vright = vb[t + 1, k, rc, :]
            ve = east_of(v, vright)
            vn = vb[t, k, rn, :]
            vs = vb[t, k, rs, :]
            v2 = v + vs
            v4 = v2 + east_of(v2, vright + vb[t + 1, k, rs, :])
            u4 = (u + uw) + (un + unw)
            p = pb[t, k, rc, :]
            pe = east_of(p, pb[t + 1, k, rc, :])
            pn = pb[t, k, rn, :]
            ustar = u + (v4 * (fu4 - 0.125 * (un - us)) - 0.5 * u * (ue - uw) - (pe - p))
            vstar = v - (u4 * (fv4 + 0.125 * (ve - vw)) + 0.5 * v * (vn - vs) + (pn - p))
            yu = (ustar + yu) * (jnp.where(lu > k + 1, VISC_IN[k], VISC_END[k]) if k < NL - 1 else VISC_END[k])
            yv = (vstar + yv) * (jnp.where(lv > k + 1, VISC_IN[k], VISC_END[k]) if k < NL - 1 else VISC_END[k])
            us_o[lt, k, ro, :] = yu
            vs_o[lt, k, ro, :] = yv
            su = su + jnp.where(lu > k, u, ZERO)
            sv = sv + jnp.where(lv > k, v, ZERO)
        mu, mv = zero8, zero8
        xu, xv = zero8, zero8
        for k in reversed(range(NL)):
            xu = us_o[lt, k, ro, :] + (jnp.where(lu > k + 1, VISC_IN[k] * xu, ZERO) if k < NL - 1 else ZERO)
            xv = vs_o[lt, k, ro, :] + (jnp.where(lv > k + 1, VISC_IN[k] * xv, ZERO) if k < NL - 1 else ZERO)
            outu = (ONE / VISC_R) * xu
            outv = (ONE / VISC_R) * xv
            us_o[lt, k, ro, :] = outu
            vs_o[lt, k, ro, :] = outv
            mu = mu + jnp.where(lu > k, outu, ZERO)
            mv = mv + jnp.where(lv > k, outv, ZERO)
        iu = ONE / jnp.maximum(lu, ONE)
        iv = ONE / jnp.maximum(lv, ONE)
        mu_s[lt, ro, :] = mu * iu
        mv_s[lt, ro, :] = mv * iv
        scale = dtb * dtb / TIME_STEP
        rw = pl.ds(WO + SUB * j, SUB)
        abuf[0, lt, rw, :] = jnp.where(lu > ZERO, scale * hu * ((mu - su) * iu), ZERO)
        abuf[1, lt, rw, :] = jnp.where(lv > ZERO, scale * hv * ((mv - sv) * iv), ZERO)

    def momentum_inner(i, _):
        momentum(lax.rem(i, 4), 1 + i // 4)
        return 0
    lax.fori_loop(0, SUB, momentum_inner, 0)

    @pl.when(has_s)
    def _():
        for cp in (to_n[0], to_n[1], to_n[2], to_n[3]):
            cp.wait_recv()

    @pl.when(has_n)
    def _():
        for cp in (to_s[0], to_s[1], to_s[2], to_s[3], to_s[4], to_s[5]):
            cp.wait_recv()

    def pressure_north(i, _):
        pressure(1 + i, RO + NR)
        return 0
    lax.fori_loop(0, 4, pressure_north, 0)

    def momentum_outer(i, _):
        momentum(lax.rem(i, 4), 3 * (i // 4))
        return 0
    lax.fori_loop(0, SUB, momentum_outer, 0)

    for f in range(2):
        for j in range(4):
            rows = pl.ds(WO + SUB * j, SUB)
            asend[f, pl.ds(SUB * j, SUB), :] = jnp.where(half, abuf[f, 0, rows, :], abuf[f, 3, rows, :])

    def arows(b):
        return abuf.at[:, own4, pl.ds(WO, NR), :], abuf.at[:, own4, pl.ds(b, NR), :]

    force_z = remote(20, asend, abuf.at[:, 4, pl.ds(WO, NR), :], dev(0, ocol))
    force_n = [remote(21, *arows(WO - NR), dev(1, col)), remote(23, asend, abuf.at[:, 4, pl.ds(WO - NR, NR), :], dev(1, ocol))]
    force_s = [remote(22, *arows(WO + NR), dev(-1, col)), remote(24, asend, abuf.at[:, 4, pl.ds(WO + NR, NR), :], dev(-1, ocol))]
    force_z.start()

    @pl.when(has_n)
    def _():
        for cp in force_n:
            cp.start()

    @pl.when(has_s)
    def _():
        for cp in force_s:
            cp.start()

    @pl.when(has_s)
    def _():
        for cp in (to_n[4], to_n[5]):
            cp.wait_recv()

    def tracers(lt, j):
        rc, rn, rs = pl.ds(RO + SUB * j, SUB), pl.ds(RO + 1 + SUB * j, SUB), pl.ds(RO - 1 + SUB * j, SUB)
        ro = pl.ds(SUB * j, SUB)
        t = lt + 1
        rw = pl.ds(WO + SUB * j, SUB)
        c0 = wide[4, lt, rw, :]
        left = lax.rem(lt + 4, 5)
        luw = jnp.minimum(c0, west_of(c0, wide[4, left, rw, :]))
        lvs = jnp.minimum(c0, wide[4, lt, pl.ds(WO - 1 + SUB * j, SUB), :])
        lu = lu_o[lt, ro, :]
        lv = lv_o[lt, ro, :]
        half_dt = 0.5 * TIME_STEP
        yt, ys = zero8, zero8
        for k in range(NL):
            u = ub[t, k, rc, :]
            me = jnp.where(lu > k, half_dt * u, ZERO)
            mw = jnp.where(luw > k, half_dt * west_of(u, ub[t - 1, k, rc, :]), ZERO)
            mn = jnp.where(lv > k, half_dt * vb[t, k, rc, :], ZERO)
            ms = jnp.where(lvs > k, half_dt * vb[t, k, rs, :], ZERO)

            def advect(buf):
                q = buf[t, k, rc, :]
                qe = east_of(q, buf[t + 1, k, rc, :])
                qw = west_of(q, buf[t - 1, k, rc, :])
                qn = buf[t, k, rn, :]
                qs = buf[t, k, rs, :]
                return q - ((me * (q + qe) - mw * (qw + q)) + (mn * (q + qn) - ms * (qs + q)))

            qt = advect(tb)
            qs_ = advect(sb)
            fac = jnp.where(c0 > k + 1, DIFF_IN[k], DIFF_END[k]) if k < NL - 1 else DIFF_END[k]
            yt = jnp.where(c0 > k, (qt + yt) * fac, DIFF_R * qt)
            ys = jnp.where(c0 > k, (qs_ + ys) * fac, DIFF_R * qs_)
            tn_o[lt, k, ro, :] = yt
            sn_o[lt, k, ro, :] = ys
        xt, xs_ = zero8, zero8
        for k in reversed(range(NL)):
            xt = tn_o[lt, k, ro, :] + (jnp.where(c0 > k + 1, DIFF_IN[k] * xt, ZERO) if k < NL - 1 else ZERO)
            xs_ = sn_o[lt, k, ro, :] + (jnp.where(c0 > k + 1, DIFF_IN[k] * xs_, ZERO) if k < NL - 1 else ZERO)
            tn_o[lt, k, ro, :] = (ONE / DIFF_R) * xt
            sn_o[lt, k, ro, :] = (ONE / DIFF_R) * xs_

    def tracers_all(i, _):
        tracers(lax.rem(i, 4), i // 4)
        return 0
    lax.fori_loop(0, 16, tracers_all, 0)

    @pl.when(has_s)
    def _():
        for cp in (to_n[6], to_n[7], to_n[SUB]):
            cp.wait_recv()

    @pl.when(has_n)
    def _():
        for cp in (to_s[6], to_s[7], to_s[SUB]):
            cp.wait_recv()

    force_z.wait_recv()

    @pl.when(has_s)
    def _():
        for cp in force_n:
            cp.wait_recv()

    @pl.when(has_n)
    def _():
        for cp in force_s:
            cp.wait_recv()

    for cp in east_w + [force_z]:
        cp.wait_send()

    @pl.when(has_n)
    def _():
        for cp in to_n + force_n:
            cp.wait_send()

    @pl.when(has_s)
    def _():
        for cp in to_s + force_s:
            cp.wait_send()


def finish_kernel(n_row, n_sub, w_ref,
                  us, vs, tn, sn, wide, abuf, lu, lv, hu_s, hv_s, mu_s, mv_s,
                  eta_o, tu_o, tv_o, u_o, v_o, t_o, s_o,
                  bu, bv, cfu, cfv, mku, mkv, tu, tv, xs, acu, acv, cu, cv, flat_b, ubuf, vbuf, sem):
    row = lax.axis_index('row')
    dtb = TIME_STEP / n_sub
    total_rows = float(n_row * NR)
    zero8 = jnp.zeros((SUB, LANE), F32)
    copies = []

    def put(src, dst):
        cp = pltpu.make_async_copy(src, dst, sem.at[len(copies)])
        cp.start()
        copies.append(cp)

    for src, dst in ((tn, t_o), (sn, s_o)):
        for t in range(NT):
            put(src.at[t], dst.at[:, :, pl.ds(LANE * t, LANE)])

    def setup(i, _):
        base = SUB + SUB * i
        rows = pl.ds(base, SUB)
        rown = pl.ds(base + 1, SUB)
        fu, fv = corio(row * NR + SUB * i - NR, total_rows)
        for t in range(5):
            right = (t + 1) % 5
            c0 = wide[4, t, rows, :]
            wet_u = (jnp.minimum(c0, east_of(c0, wide[4, right, rows, :])) > ZERO).astype(F32)
            wet_v = (jnp.minimum(c0, wide[4, t, rown, :]) > ZERO).astype(F32)
            d0 = wide[3, t, rows, :]
            scale = dtb * dtb * GRAVITY * 0.5
            bu[t, rows, :] = wet_u * (scale * (d0 + east_of(d0, wide[3, right, rows, :])))
            bv[t, rows, :] = wet_v * (scale * (d0 + wide[3, t, rown, :]))
            cfu[t, rows, :] = wet_u * ((0.25 * dtb) * fu)
            cfv[t, rows, :] = wet_v * ((0.25 * dtb) * fv)
            mku[t, rows, :] = wet_u
            mkv[t, rows, :] = wet_v
            tu[0, t, rows, :] = dtb * wide[1, t, rows, :]
            tv[0, t, rows, :] = dtb * wide[2, t, rows, :]
        return 0
    lax.fori_loop(0, 12, setup, 0)
    for t in range(5):
        for a in (0, 1):
            for start in (0, 104):
                tu[a, t, pl.ds(start, SUB), :] = zero8
                tv[a, t, pl.ds(start, SUB), :] = zero8
        for i in range(2):
            xs[t, pl.ds(104 * i, SUB), :] = zero8
    for i in range(13):
        for t in range(5):
            tu[1, t, pl.ds(SUB * i + SUB, SUB), :] = zero8
            tv[1, t, pl.ds(SUB * i + SUB, SUB), :] = zero8
            xs[t, pl.ds(SUB * i + SUB, SUB), :] = zero8
    for t in range(NT):
        for j in range(4):
            acu[t, pl.ds(SUB * j, SUB), :] = zero8
            acv[t, pl.ds(SUB * j, SUB), :] = zero8

    def subcycle(n, cur, lo, hi, first=False):
        nxt = 1 - cur
        weight = w_ref[n] * (ONE / dtb)
        for i in range(lo, hi):
            rows = pl.ds(SUB + SUB * i, SUB)
            rows_s = pl.ds(7 + SUB * i, SUB)
            us = [tu[cur, t, rows, :] for t in range(5)]
            for t in range(5):
                uw = west_of(us[t], us[(t + 4) % 5])
                xs[t, rows, :] = us[t] + uw
                wide[0, t, rows, :] = wide[0, t, rows, :] - ((us[t] - uw) + (tv[cur, t, rows, :] - tv[cur, t, rows_s, :]))
        for i in range(lo, hi):
            rows = pl.ds(SUB + SUB * i, SUB)
            rows_s = pl.ds(7 + SUB * i, SUB)
            rows_n = pl.ds(9 + SUB * i, SUB)
            es = [wide[0, t, rows, :] for t in range(5)]
            v0 = [tv[cur, t, rows, :] for t in range(5)]
            v2 = [v0[t] + tv[cur, t, rows_s, :] for t in range(5)]
            for t in range(5):
                right = (t + 1) % 5
                v4 = v2[t] + east_of(v2[t], v2[right])
                slope_u = east_of(es[t], es[right]) - es[t]
                slope_v = wide[0, t, rows_n, :] - es[t]
                u4 = xs[t, rows, :] + xs[t, rows_n, :]
                u_old = tu[cur, t, rows, :]
                v_old = v0[t]
                if first:
                    u_old = mku[t, rows, :] * u_old
                    v_old = mkv[t, rows, :] * v_old
                u_new = (u_old + abuf[0, t, rows, :]) + (cfu[t, rows, :] * v4 - bu[t, rows, :] * slope_u)
                v_new = (v_old + abuf[1, t, rows, :]) - (cfv[t, rows, :] * u4 + bv[t, rows, :] * slope_v)
                tu[nxt, t, rows, :] = u_new
                tv[nxt, t, rows, :] = v_new
                if 4 <= i < SUB and t < NT:
                    ro = pl.ds(SUB * (i - 4), SUB)
                    acu[t, ro, :] += weight * u_new
                    acv[t, ro, :] += weight * v_new

    def pairs(first_n, count, lo, hi):
        def body(i, _):
            n = first_n + 2 * i
            subcycle(n, 0, lo, hi)
            subcycle(n + 1, 1, lo, hi)
            return 0
        lax.fori_loop(0, count, body, 0)

    subcycle(0, 0, 0, 12, first=True)
    subcycle(1, 1, 0, 12)
    pairs(2, 2, 0, 12)
    pairs(6, 4, 1, 11)
    pairs(14, 4, 2, 10)
    pairs(22, 4, 3, 9)

    for t in range(NT):
        for j in range(4):
            rw = pl.ds(WO + SUB * j, SUB)
            ro = pl.ds(SUB * j, SUB)
            flat_b[0, t, ro, :] = wide[0, t, rw, :]
            flat_b[1, t, ro, :] = (ONE / dtb) * tu[0, t, rw, :]
            flat_b[2, t, ro, :] = (ONE / dtb) * tv[0, t, rw, :]
            cu[t, ro, :] = acu[t, ro, :] / hu_s[t, ro, :] - mu_s[t, ro, :]
            hv = hv_s[t, ro, :]
            cv[t, ro, :] = acv[t, ro, :] / hv - mv_s[t, ro, :]

    for f, dst in enumerate((eta_o, tu_o, tv_o)):
        for t in range(NT):
            put(flat_b.at[f, t], dst.at[:, pl.ds(LANE * t, LANE)])
    for lev, cor, src, buf, dst in ((lu, cu, us, ubuf, u_o), (lv, cv, vs, vbuf, v_o)):
        for t in range(NT):
            for j in range(4):
                ro = pl.ds(SUB * j, SUB)
                count = lev[t, ro, :]
                shift = cor[t, ro, :]
                for k in range(NL):
                    buf[t, k, ro, :] = jnp.where(count > k, src[t, k, ro, :] + shift, ZERO)
            put(buf.at[t], dst.at[:, :, pl.ds(LANE * t, LANE)])
    for cp in copies:
        cp.wait()


def solution(mesh):
    n_row = mesh.shape['row']

    def step(vel_u, vel_v, temperature, salinity, surf_eta, trans_u, trans_v, bottom_depth, level_count, avg_weights):
        n_sub = avg_weights.shape[0]
        hbm = pl.BlockSpec(memory_space=pltpu.HBM)
        vmem = pl.BlockSpec(memory_space=pltpu.VMEM)
        smem = pl.BlockSpec(memory_space=pltpu.SMEM)
        cube_v = pltpu.VMEM((NT, NL, NR, LANE), F32)
        flat_v = pltpu.VMEM((NT, NR, LANE), F32)
        pad3 = pltpu.VMEM((6, NL, 48, LANE), F32)
        wide1 = pltpu.VMEM((5, WR, LANE), F32)
        wide_v = pltpu.VMEM((5, 5, WR, LANE), F32)
        force_v = pltpu.VMEM((2, 5, WR, LANE), F32)
        sems = pltpu.SemaphoreType.DMA
        outs = [cube_v] * 4 + [wide_v, force_v] + [flat_v] * 6
        mids = pl.pallas_call(
            functools.partial(ocean_kernel, n_row, n_sub),
            out_shape=outs,
            in_specs=[hbm] * 9,
            out_specs=[vmem] * len(outs),
            scratch_shapes=[pad3] * 5 + [
                pltpu.VMEM((5, NR, LANE), F32),
                pltpu.VMEM((NT, NR, LANE), jnp.int32),
                pltpu.VMEM((SUB, SUB, LANE), F32),
                pltpu.VMEM((SUB, SUB, LANE), F32),
                pltpu.VMEM((2, NR, LANE), F32),
                sems((16,)), sems((20,)), sems((N_COPY,)), sems((N_COPY,)),
            ],
            compiler_params=pltpu.CompilerParams(collective_id=0, has_side_effects=True, vmem_limit_bytes=VMEM_MAIN),
            name='ocean',
        )(*[pltpu.with_memory_space_constraint(x, pltpu.HBM) for x in (vel_u, vel_v, temperature, salinity, surf_eta, trans_u, trans_v, bottom_depth, level_count)])
        cube = jax.ShapeDtypeStruct((NL, NR, NT * LANE), F32)
        flat = jax.ShapeDtypeStruct((NR, NT * LANE), F32)
        return pl.pallas_call(
            functools.partial(finish_kernel, n_row, n_sub),
            out_shape=[flat] * 3 + [cube] * 4,
            in_specs=[smem] + [vmem] * len(outs),
            out_specs=[hbm] * 7,
            scratch_shapes=[wide1] * 6 + [force_v, force_v, wide1] + [flat_v] * 4 + [pltpu.VMEM((3, NT, NR, LANE), F32), cube_v, cube_v, sems((28,))],
            compiler_params=pltpu.CompilerParams(vmem_limit_bytes=VMEM_FINISH),
            name='finish',
        )(avg_weights, *mids)

    cube = P(None, 'row', 'col')
    flat = P('row', 'col')
    return jax.shard_map(step, mesh=mesh, in_specs=(cube, cube, cube, cube, flat, flat, flat, flat, flat, P()), out_specs=(flat, flat, flat, cube, cube, cube, cube), check_vma=False)
```

```python
import functools

import jax
import jax.numpy as jnp
from jax import lax
from jax.experimental import pallas as pl
from jax.experimental.pallas import tpu as pltpu
from jax.sharding import PartitionSpec as P

TIME_STEP = 1.0
GRAVITY = 16.0
BC_GRAVITY = 4.0
EXPAND_T = 0.2
CONTRACT_S = 0.6
CORIO_F0 = 0.4
CORIO_BETA = 0.4
VISC_R = 2.0
DIFF_R = 0.5

MESH = pl.DeviceIdType.MESH
F32 = jnp.float32

SUB = 8
LANE = 128
ZERO = 0.0
ONE = 1.0
NL = 31
NR = 32
NT = 4
RO = 8
WO = 40
WR = 112
N_COPY = 32
NH = 30
VMEM_MAIN = 40 * 1024 * 1024
VMEM_FINISH = 12 * 1024 * 1024


def factors(strength):
    inner, last = [], []
    before = ZERO
    for level in range(NL):
        low = ZERO if level == 0 else strength
        inner.append(strength / (ONE + low + strength - low * before))
        last.append(strength / (ONE + low - low * before))
        before = inner[-1]
    return inner, last


VISC_IN, VISC_END = factors(VISC_R)
DIFF_IN, DIFF_END = factors(DIFF_R)


def lanes():
    return lax.broadcasted_iota(jnp.int32, (SUB, LANE), 1)


def west_of(own, left):
    return pltpu.roll(jnp.where(lanes() == 127, left, own), 1, 1)


def east_of(own, right):
    return pltpu.roll(jnp.where(lanes() == 0, right, own), 127, 1)


def corio(first, total_rows):
    pos = (first + lax.broadcasted_iota(jnp.int32, (SUB, LANE), 0)).astype(F32)
    fu = CORIO_F0 + CORIO_BETA * ((pos + 0.5) / total_rows - 0.5)
    fv = CORIO_F0 + CORIO_BETA * ((pos + ONE) / total_rows - 0.5)
    return fu, fv


def ocean_kernel(n_row, n_sub,
                 u_in, v_in, t_in, s_in, eta_in, tu_in, tv_in, dep_in, cnt_in,
                 us_o, vs_o, tn_o, sn_o, wide, abuf, lu_o, lv_o, hu_s, hv_s, mu_s, mv_s,
                 fb, pb, cnt, wsend, cnt_i, pk_s, pk_r, asend,
                 in_sem, w_sem, send, recv):
    row = lax.axis_index('row')
    col = lax.axis_index('col')
    ocol = 1 - col
    has_s = row > 0
    has_n = row < n_row - 1
    dtb = TIME_STEP / n_sub
    total_rows = float(n_row * NR)
    used = []
    ub, vb, tb, sb = (fb.at[f] for f in range(4))
    zero8 = jnp.zeros((SUB, LANE), F32)

    def dev(step, c):
        return {'row': row + step, 'col': c}

    def remote(src, dst, device):
        used.append(0)
        idx = len(used) - 1
        return pltpu.make_async_remote_copy(src, dst, send.at[idx], recv.at[idx], device_id=device, device_id_type=MESH)

    def start(copies):
        for cp in copies:
            cp.start()

    def both(south, north, action):
        @pl.when(has_s)
        def _():
            for cp in south:
                action(cp)

        @pl.when(has_n)
        def _():
            for cp in north:
                action(cp)

    def arrived(south_from, north_from):
        both(south_from, north_from, lambda cp: cp.wait_recv())

    wloads, loads = {}, {}
    for f, src in enumerate((eta_in, tv_in, tu_in, dep_in, cnt_in)):
        for t in range(NT):
            dst = wide.at[f, t, pl.ds(WO, NR), :] if f < 4 else cnt_i.at[t]
            wloads[f, t] = pltpu.make_async_copy(src.at[:, pl.ds(LANE * t, LANE)], dst, w_sem.at[f * NT + t])
    for f, src in enumerate((u_in, v_in, t_in, s_in)):
        for t in range(NT):
            loads[f, t] = pltpu.make_async_copy(src.at[:, :, pl.ds(LANE * t, LANE)], fb.at[f, t + 1, :, pl.ds(RO, NR), :], in_sem.at[f * NT + t])
    start(wloads.values())
    order = [(f, t) for f in range(4) for t in (0, 3)] + [(f, t) for f in (0, 1, 2, 3) for t in (1, 2)]
    start([loads[key] for key in order])

    for i in range(5):
        for rr in (0, SUB, WR - 2 * SUB, WR - SUB):
            for f in range(4):
                wide[f, i, pl.ds(rr, SUB), :] = zero8
            for f in range(2):
                abuf[f, i, pl.ds(rr, SUB), :] = zero8

    barrier = pltpu.get_barrier_semaphore()
    pl.semaphore_signal(barrier, inc=1, device_id=dev(0, ocol), device_id_type=MESH)

    @pl.when(has_n)
    def _():
        for c in (col, ocol):
            pl.semaphore_signal(barrier, inc=1, device_id=dev(1, c), device_id_type=MESH)

    @pl.when(has_s)
    def _():
        for c in (col, ocol):
            pl.semaphore_signal(barrier, inc=1, device_id=dev(-1, c), device_id_type=MESH)

    def fill(first3, first2):
        def body(i, _):
            for f in range(4):
                fb[f, i, :, pl.ds(first3, SUB), :] = jnp.zeros((NL, SUB, LANE), F32)
            return 0
        lax.fori_loop(0, 6, body, 0)
        for i in range(5):
            for f in range(4):
                wide[f, i, pl.ds(first2, NR), :] = jnp.zeros((NR, LANE), F32)
            for f in range(2):
                abuf[f, i, pl.ds(first2, NR), :] = jnp.zeros((NR, LANE), F32)
            cnt[i, pl.ds(first3, SUB), :] = zero8

    @pl.when(jnp.logical_not(has_s))
    def _():
        fill(0, WO - NR)

    @pl.when(jnp.logical_not(has_n))
    def _():
        fill(RO + NR, WO + NR)

    for cp in wloads.values():
        cp.wait()
    for t in range(NT):
        cnt[t, pl.ds(RO, NR), :] = cnt_i[t].astype(F32)
    lane = lanes()
    outer = lane < LANE // 2
    middle = jnp.logical_and(lane >= NR, lane < LANE - NR)

    def edges(buf, f, first):
        rows = pl.ds(first, SUB)
        return jnp.where(outer, buf[f, 0, rows, :], buf[f, 3, rows, :])

    def paired(buf, f, g, first):
        return jnp.where(middle, pltpu.roll(edges(buf, g, first), LANE // 2, 1), edges(buf, f, first))

    for j in range(4):
        mine = pl.ds(SUB * j, SUB)
        first = WO + SUB * j
        for f in range(2):
            wsend[f, mine, :] = paired(wide, f, f + 2, first)
        own = pl.ds(RO + SUB * j, SUB)
        wsend[2, mine, :] = jnp.where(outer, cnt[0, own, :], cnt[3, own, :])

    barrier_count = 1 + 2 * has_n.astype(jnp.int32) + 2 * has_s.astype(jnp.int32)
    pl.semaphore_wait(barrier, barrier_count)

    own4 = pl.ds(0, NT)
    mid4 = pl.ds(1, NT)
    two = pl.ds(0, 2)
    top, low, north, south = RO + NR - 1, RO, RO + NR, RO - 1
    n_src, n_dst, s_src, s_dst = WO + NR - NH, WO - NH, WO, WO + NR

    def rows3(f, a, b, d):
        return remote(fb.at[f, mid4, :, pl.ds(a, 1), :], fb.at[f, mid4, :, pl.ds(b, 1), :], dev(d, col))

    def rows2(buf, f, nf, a, b, d):
        return remote(buf.at[pl.ds(f, nf), own4, pl.ds(a, NH), :], buf.at[pl.ds(f, nf), own4, pl.ds(b, NH), :], dev(d, col))

    def row1(a, b, d):
        return remote(cnt.at[own4, pl.ds(a, 1), :], cnt.at[own4, pl.ds(b, 1), :], dev(d, col))

    def corner(a, b, d):
        return remote(wsend.at[two, pl.ds(a - WO, NH), :], wide.at[two, 4, pl.ds(b, NH), :], dev(d, ocol))

    z_wide = [
        remote(wsend.at[2], cnt.at[4, pl.ds(RO, NR), :], dev(0, ocol)),
        remote(wsend.at[two], wide.at[two, 4, pl.ds(WO, NR), :], dev(0, ocol)),
    ]
    n_first = [row1(top, south, 1), rows2(wide, 3, 1, n_src, n_dst, 1)]
    s_first = [row1(low, north, -1), rows2(wide, 3, 1, s_src, s_dst, -1)]
    start(z_wide)
    both(s_first, n_first, lambda cp: cp.start())

    for f in (0, 1):
        for t in (0, 3, 1, 2):
            loads[f, t].wait()
    n_vel = [rows3(0, top, south, 1), rows3(1, top, south, 1),
             remote(fb.at[1, 1, :, pl.ds(top, 1), :], fb.at[1, 5, :, pl.ds(south, 1), :], dev(1, ocol))]
    s_vel = [rows3(0, low, north, -1), rows3(1, low, north, -1),
             remote(fb.at[0, 4, :, pl.ds(low, 1), :], fb.at[0, 0, :, pl.ds(north, 1), :], dev(-1, ocol))]
    both(s_vel, n_vel, lambda cp: cp.start())
    for f in (2, 3):
        for t in (0, 3, 1, 2):
            loads[f, t].wait()
    n_tra = [rows3(2, top, south, 1), rows3(3, top, south, 1)]
    s_tra = [rows3(2, low, north, -1), rows3(3, low, north, -1)]
    n_far = [rows2(wide, 0, 3, n_src, n_dst, 1), corner(n_src, n_dst, 1)]
    s_far = [rows2(wide, 0, 3, s_src, s_dst, -1), corner(s_src, s_dst, -1)]
    both(s_tra + s_far, n_tra + n_far, lambda cp: cp.start())

    def pack(f, _):
        here = lanes()
        east, west = zero8, zero8
        for k in range(NL):
            for j in range(4):
                slot = 4 * k + j
                rows = pl.ds(RO + SUB * j, SUB)
                east = jnp.where(here == slot, pltpu.roll(fb[f, 1, k, rows, :], slot, 1) if slot else fb[f, 1, k, rows, :], east)
                west = jnp.where(here == slot, pltpu.roll(fb[f, 4, k, rows, :], slot + 1, 1), west)
        pk_s[f, 0] = east
        pk_s[f, 1] = west
        return 0
    lax.fori_loop(0, 4, pack, 0)
    z_col = remote(pk_s, pk_r, dev(0, ocol))
    z_col.start()

    p_unit = 0.5 * BC_GRAVITY / NL

    def pressure(t, start):
        rows = pl.ds(start, SUB)
        total = zero8
        for k in range(NL):
            part = (p_unit * CONTRACT_S) * sb[t, k, rows, :] - (p_unit * EXPAND_T) * tb[t, k, rows, :]
            here = total + part
            pb[t, k, rows, :] = here
            total = here + part

    def pressure_own(i, _):
        pressure(1 + i // 4, pl.multiple_of(RO + SUB * lax.rem(i, 4), SUB))
        return 0
    lax.fori_loop(0, 16, pressure_own, 0)

    def near2d(buf, first, t):
        c = buf[t, pl.ds(first, SUB), :]
        return c, east_of(c, buf[t + 1, pl.ds(first, SUB), :]), buf[t, pl.ds(first + 1, SUB), :]

    depth = wide.at[3]

    def momentum(lt, j):
        rc, rn, rs = pl.ds(RO + SUB * j, SUB), pl.ds(RO + 1 + SUB * j, SUB), pl.ds(RO - 1 + SUB * j, SUB)
        ro = pl.ds(SUB * j, SUB)
        t = lt + 1
        fu, fv = corio(row * NR + SUB * j, total_rows)
        fu4 = 0.25 * fu
        fv4 = 0.25 * fv
        c0, ce, cn = near2d(cnt, RO + SUB * j, lt)
        lu = jnp.minimum(c0, ce)
        lv = jnp.minimum(c0, cn)
        d0, de, dn = near2d(depth, WO + SUB * j, lt)
        hu = 0.5 * (d0 + de)
        hv = 0.5 * (d0 + dn)
        lu_o[lt, ro, :] = lu
        lv_o[lt, ro, :] = lv
        hu_s[lt, ro, :] = hu
        hv_s[lt, ro, :] = hv
        yu, yv = zero8, zero8
        su, sv = zero8, zero8
        for k in range(NL):
            u = ub[t, k, rc, :]
            v = vb[t, k, rc, :]
            uw = west_of(u, ub[t - 1, k, rc, :])
            ue = east_of(u, ub[t + 1, k, rc, :])
            un = ub[t, k, rn, :]
            us = ub[t, k, rs, :]
            unw = west_of(un, ub[t - 1, k, rn, :])
            vw = west_of(v, vb[t - 1, k, rc, :])
            vright = vb[t + 1, k, rc, :]
            ve = east_of(v, vright)
            vn = vb[t, k, rn, :]
            vs = vb[t, k, rs, :]
            v2 = v + vs
            v4 = v2 + east_of(v2, vright + vb[t + 1, k, rs, :])
            u4 = (u + uw) + (un + unw)
            p = pb[t, k, rc, :]
            pe = east_of(p, pb[t + 1, k, rc, :])
            pn = pb[t, k, rn, :]
            ustar = u + (v4 * (fu4 - 0.125 * (un - us)) - 0.5 * u * (ue - uw) - (pe - p))
            vstar = v - (u4 * (fv4 + 0.125 * (ve - vw)) + 0.5 * v * (vn - vs) + (pn - p))
            yu = (ustar + yu) * (jnp.where(lu > k + 1, VISC_IN[k], VISC_END[k]) if k < NL - 1 else VISC_END[k])
            yv = (vstar + yv) * (jnp.where(lv > k + 1, VISC_IN[k], VISC_END[k]) if k < NL - 1 else VISC_END[k])
            us_o[lt, k, ro, :] = yu
            vs_o[lt, k, ro, :] = yv
            su = su + jnp.where(lu > k, u, ZERO)
            sv = sv + jnp.where(lv > k, v, ZERO)
        mu, mv = zero8, zero8
        xu, xv = zero8, zero8
        for k in reversed(range(NL)):
            xu = us_o[lt, k, ro, :] + (jnp.where(lu > k + 1, VISC_IN[k] * xu, ZERO) if k < NL - 1 else ZERO)
            xv = vs_o[lt, k, ro, :] + (jnp.where(lv > k + 1, VISC_IN[k] * xv, ZERO) if k < NL - 1 else ZERO)
            outu = (ONE / VISC_R) * xu
            outv = (ONE / VISC_R) * xv
            us_o[lt, k, ro, :] = outu
            vs_o[lt, k, ro, :] = outv
            mu = mu + jnp.where(lu > k, outu, ZERO)
            mv = mv + jnp.where(lv > k, outv, ZERO)
        iu = ONE / jnp.maximum(lu, ONE)
        iv = ONE / jnp.maximum(lv, ONE)
        mu_s[lt, ro, :] = mu * iu
        mv_s[lt, ro, :] = mv * iv
        scale = dtb * dtb / TIME_STEP
        rw = pl.ds(WO + SUB * j, SUB)
        abuf[0, lt, rw, :] = jnp.where(lu > ZERO, scale * hu * ((mu - su) * iu), ZERO)
        abuf[1, lt, rw, :] = jnp.where(lv > ZERO, scale * hv * ((mv - sv) * iv), ZERO)

    def momentum_free(i, _):
        momentum(1 + lax.rem(i, 2), 1 + i // 2)
        return 0

    def momentum_side(i, _):
        momentum(3 * lax.rem(i, 2), 1 + i // 2)
        return 0

    def momentum_ends(i, _):
        momentum(lax.rem(i, 4), 3 * (i // 4))
        return 0

    lax.fori_loop(0, 4, momentum_free, 0)

    for cp in z_wide + [z_col]:
        cp.wait_recv()

    def unpack(f, _):
        east, west = pk_r[f, 0], pk_r[f, 1]
        for k in range(NL):
            for j in range(4):
                slot = 4 * k + j
                rows = pl.ds(RO + SUB * j, SUB)
                fb[f, 5, k, rows, :] = pltpu.roll(east, LANE - slot, 1) if slot else east
                fb[f, 0, k, rows, :] = pltpu.roll(west, LANE - 1 - slot, 1)
        return 0
    lax.fori_loop(0, 4, unpack, 0)
    for j in range(4):
        rows = pl.ds(WO + SUB * j, SUB)
        wide[3, 4, rows, :] = pltpu.roll(wide[1, 4, rows, :], LANE // 2, 1)

    def pressure_east(i, _):
        pressure(5, pl.multiple_of(RO + SUB * i, SUB))
        return 0
    lax.fori_loop(0, 4, pressure_east, 0)
    lax.fori_loop(0, 4, momentum_side, 0)

    arrived(n_first + n_vel, s_first + s_vel + s_tra)

    def pressure_north(i, _):
        pressure(1 + i, RO + NR)
        return 0
    lax.fori_loop(0, 4, pressure_north, 0)
    lax.fori_loop(0, SUB, momentum_ends, 0)

    for j in range(4):
        asend[pl.ds(SUB * j, SUB), :] = paired(abuf, 0, 1, WO + SUB * j)

    def force_corner(a, b, d):
        return remote(asend.at[pl.ds(a - WO, NH), :], abuf.at[0, 4, pl.ds(b, NH), :], dev(d, ocol))

    z_force = remote(asend, abuf.at[0, 4, pl.ds(WO, NR), :], dev(0, ocol))
    n_force = [rows2(abuf, 0, 2, n_src, n_dst, 1), force_corner(n_src, n_dst, 1)]
    s_force = [rows2(abuf, 0, 2, s_src, s_dst, -1), force_corner(s_src, s_dst, -1)]
    z_force.start()
    both(s_force, n_force, lambda cp: cp.start())

    arrived(n_tra, [])

    def tracers(lt, j):
        rc, rn, rs = pl.ds(RO + SUB * j, SUB), pl.ds(RO + 1 + SUB * j, SUB), pl.ds(RO - 1 + SUB * j, SUB)
        ro = pl.ds(SUB * j, SUB)
        t = lt + 1
        c0 = cnt[lt, rc, :]
        left = lax.rem(lt + 4, 5)
        luw = jnp.minimum(c0, west_of(c0, cnt[left, rc, :]))
        lvs = jnp.minimum(c0, cnt[lt, rs, :])
        lu = lu_o[lt, ro, :]
        lv = lv_o[lt, ro, :]
        half_dt = 0.5 * TIME_STEP
        yt, ys = zero8, zero8
        for k in range(NL):
            u = ub[t, k, rc, :]
            me = jnp.where(lu > k, half_dt * u, ZERO)
            mw = jnp.where(luw > k, half_dt * west_of(u, ub[t - 1, k, rc, :]), ZERO)
            mn = jnp.where(lv > k, half_dt * vb[t, k, rc, :], ZERO)
            ms = jnp.where(lvs > k, half_dt * vb[t, k, rs, :], ZERO)

            def advect(buf):
                q = buf[t, k, rc, :]
                qe = east_of(q, buf[t + 1, k, rc, :])
                qw = west_of(q, buf[t - 1, k, rc, :])
                qn = buf[t, k, rn, :]
                qs = buf[t, k, rs, :]
                return q - ((me * (q + qe) - mw * (qw + q)) + (mn * (q + qn) - ms * (qs + q)))

            qt = advect(tb)
            qs_ = advect(sb)
            fac = jnp.where(c0 > k + 1, DIFF_IN[k], DIFF_END[k]) if k < NL - 1 else DIFF_END[k]
            yt = jnp.where(c0 > k, (qt + yt) * fac, DIFF_R * qt)
            ys = jnp.where(c0 > k, (qs_ + ys) * fac, DIFF_R * qs_)
            tn_o[lt, k, ro, :] = yt
            sn_o[lt, k, ro, :] = ys
        xt, xs_ = zero8, zero8
        for k in reversed(range(NL)):
            xt = tn_o[lt, k, ro, :] + (jnp.where(c0 > k + 1, DIFF_IN[k] * xt, ZERO) if k < NL - 1 else ZERO)
            xs_ = sn_o[lt, k, ro, :] + (jnp.where(c0 > k + 1, DIFF_IN[k] * xs_, ZERO) if k < NL - 1 else ZERO)
            tn_o[lt, k, ro, :] = (ONE / DIFF_R) * xt
            sn_o[lt, k, ro, :] = (ONE / DIFF_R) * xs_

    def tracers_all(i, _):
        tracers(lax.rem(i, 4), i // 4)
        return 0
    lax.fori_loop(0, 16, tracers_all, 0)

    z_force.wait_recv()
    arrived(n_far + n_force, s_far + s_force)

    for cp in z_wide + [z_col, z_force]:
        cp.wait_send()
    both(s_first + s_vel + s_tra + s_far + s_force, n_first + n_vel + n_tra + n_far + n_force, lambda cp: cp.wait_send())


def finish_kernel(n_row, n_sub, w_ref,
                  us, vs, tn, sn, wide, abuf, lu, lv, hu_s, hv_s, mu_s, mv_s,
                  eta_o, tu_o, tv_o, u_o, v_o, t_o, s_o,
                  bu, bv, cfu, cfv, mku, mkv, tu, tv, xs, acu, acv, cu, cv, flat_b, ubuf, vbuf, sem):
    row = lax.axis_index('row')
    dtb = TIME_STEP / n_sub
    total_rows = float(n_row * NR)
    zero8 = jnp.zeros((SUB, LANE), F32)
    copies = []

    def put(src, dst):
        cp = pltpu.make_async_copy(src, dst, sem.at[len(copies)])
        cp.start()
        copies.append(cp)

    for src, dst in ((tn, t_o), (sn, s_o)):
        for t in range(NT):
            put(src.at[t], dst.at[:, :, pl.ds(LANE * t, LANE)])

    def setup(i, _):
        base = SUB + SUB * i
        rows = pl.ds(base, SUB)
        rown = pl.ds(base + 1, SUB)
        first = row * NR + SUB * i - NR
        fu, fv = corio(first, total_rows)
        place = first + lax.broadcasted_iota(jnp.int32, (SUB, LANE), 0)
        inside = place >= 0
        wet_u = jnp.logical_and(inside, place < n_row * NR).astype(F32)
        wet_v = jnp.logical_and(inside, place < n_row * NR - 1).astype(F32)
        for t in range(5):
            right = (t + 1) % 5
            d0 = wide[3, t, rows, :]
            scale = 0.5 * dtb * dtb * GRAVITY
            bu[t, rows, :] = wet_u * (scale * (d0 + east_of(d0, wide[3, right, rows, :])))
            bv[t, rows, :] = wet_v * (scale * (d0 + wide[3, t, rown, :]))
            cfu[t, rows, :] = wet_u * ((0.25 * dtb) * fu)
            cfv[t, rows, :] = wet_v * ((0.25 * dtb) * fv)
            mku[t, rows, :] = wet_u
            mkv[t, rows, :] = wet_v
            tu[0, t, rows, :] = dtb * wide[2, t, rows, :]
            tv[0, t, rows, :] = dtb * wide[1, t, rows, :]
        return 0

    for i in range(12):
        rows = pl.ds(SUB + SUB * i, SUB)
        for f in range(2):
            wide[f + 2, 4, rows, :] = pltpu.roll(wide[f, 4, rows, :], LANE // 2, 1)
        abuf[1, 4, rows, :] = pltpu.roll(abuf[0, 4, rows, :], LANE // 2, 1)
    lax.fori_loop(0, 12, setup, 0)
    for t in range(NT):
        acu[t] = jnp.zeros((NR, LANE), F32)
        acv[t] = jnp.zeros((NR, LANE), F32)

    def subcycle(n, cur, lo, hi, first=False):
        nxt = 1 - cur
        weight = w_ref[n] * (ONE / dtb)
        for i in range(lo, hi):
            rows = pl.ds(SUB + SUB * i, SUB)
            rows_s = pl.ds(7 + SUB * i, SUB)
            us = [tu[cur, t, rows, :] for t in range(5)]
            for t in range(5):
                uw = west_of(us[t], us[(t + 4) % 5])
                xs[t, rows, :] = us[t] + uw
                wide[0, t, rows, :] = wide[0, t, rows, :] - ((us[t] - uw) + (tv[cur, t, rows, :] - tv[cur, t, rows_s, :]))
        for i in range(lo, hi):
            rows = pl.ds(SUB + SUB * i, SUB)
            rows_s = pl.ds(7 + SUB * i, SUB)
            rows_n = pl.ds(9 + SUB * i, SUB)
            es = [wide[0, t, rows, :] for t in range(5)]
            v0 = [tv[cur, t, rows, :] for t in range(5)]
            v2 = [v0[t] + tv[cur, t, rows_s, :] for t in range(5)]
            for t in range(5):
                right = (t + 1) % 5
                v4 = v2[t] + east_of(v2[t], v2[right])
                slope_u = east_of(es[t], es[right]) - es[t]
                slope_v = wide[0, t, rows_n, :] - es[t]
                u4 = xs[t, rows, :] + xs[t, rows_n, :]
                u_old = tu[cur, t, rows, :]
                v_old = v0[t]
                if first:
                    u_old = mku[t, rows, :] * u_old
                    v_old = mkv[t, rows, :] * v_old
                u_new = (u_old + abuf[0, t, rows, :]) + (cfu[t, rows, :] * v4 - bu[t, rows, :] * slope_u)
                v_new = (v_old + abuf[1, t, rows, :]) - (cfv[t, rows, :] * u4 + bv[t, rows, :] * slope_v)
                tu[nxt, t, rows, :] = u_new
                tv[nxt, t, rows, :] = v_new
                if 4 <= i < SUB and t < NT:
                    ro = pl.ds(SUB * (i - 4), SUB)
                    acu[t, ro, :] += weight * u_new
                    acv[t, ro, :] += weight * v_new

    def pairs(first_n, count, lo, hi):
        def body(i, _):
            n = first_n + 2 * i
            subcycle(n, 0, lo, hi)
            subcycle(n + 1, 1, lo, hi)
            return 0
        lax.fori_loop(0, count, body, 0)

    subcycle(0, 0, 0, 12, first=True)
    subcycle(1, 1, 0, 12)
    pairs(2, 2, 0, 12)
    pairs(6, 4, 1, 11)
    pairs(14, 4, 2, 10)
    pairs(22, 4, 3, 9)

    for t in range(NT):
        for j in range(4):
            rw = pl.ds(WO + SUB * j, SUB)
            ro = pl.ds(SUB * j, SUB)
            flat_b[0, t, ro, :] = wide[0, t, rw, :]
            flat_b[1, t, ro, :] = (ONE / dtb) * tu[0, t, rw, :]
            flat_b[2, t, ro, :] = (ONE / dtb) * tv[0, t, rw, :]
            cu[t, ro, :] = acu[t, ro, :] / hu_s[t, ro, :] - mu_s[t, ro, :]
            hv = hv_s[t, ro, :]
            cv[t, ro, :] = acv[t, ro, :] / hv - mv_s[t, ro, :]

    for f, dst in enumerate((eta_o, tu_o, tv_o)):
        for t in range(NT):
            put(flat_b.at[f, t], dst.at[:, pl.ds(LANE * t, LANE)])
    for lev, cor, src, buf, dst in ((lu, cu, us, ubuf, u_o), (lv, cv, vs, vbuf, v_o)):
        for t in range(NT):
            for j in range(4):
                ro = pl.ds(SUB * j, SUB)
                count = lev[t, ro, :]
                shift = cor[t, ro, :]
                for k in range(NL):
                    buf[t, k, ro, :] = jnp.where(count > k, src[t, k, ro, :] + shift, ZERO)
            put(buf.at[t], dst.at[:, :, pl.ds(LANE * t, LANE)])
    for cp in copies:
        cp.wait()


def solution(mesh):
    n_row = mesh.shape['row']

    def step(vel_u, vel_v, temperature, salinity, surf_eta, trans_u, trans_v, bottom_depth, level_count, avg_weights):
        n_sub = avg_weights.shape[0]
        hbm = pl.BlockSpec(memory_space=pltpu.HBM)
        vmem = pl.BlockSpec(memory_space=pltpu.VMEM)
        smem = pl.BlockSpec(memory_space=pltpu.SMEM)
        cube_v = pltpu.VMEM((NT, NL, NR, LANE), F32)
        flat_v = pltpu.VMEM((NT, NR, LANE), F32)
        wide1 = pltpu.VMEM((5, WR, LANE), F32)
        wide_v = pltpu.VMEM((4, 5, WR, LANE), F32)
        force_v = pltpu.VMEM((2, 5, WR, LANE), F32)
        sems = pltpu.SemaphoreType.DMA
        outs = [cube_v] * 4 + [wide_v, force_v] + [flat_v] * 6
        mids = pl.pallas_call(
            functools.partial(ocean_kernel, n_row, n_sub),
            out_shape=outs,
            in_specs=[hbm] * 9,
            out_specs=[vmem] * len(outs),
            scratch_shapes=[
                pltpu.VMEM((4, 6, NL, RO + NR + SUB, LANE), F32),
                pltpu.VMEM((6, NL, RO + NR + SUB, LANE), F32),
                pltpu.VMEM((5, RO + NR + SUB, LANE), F32),
                pltpu.VMEM((3, NR, LANE), F32),
                pltpu.VMEM((NT, NR, LANE), jnp.int32),
                pltpu.VMEM((4, 2, SUB, LANE), F32),
                pltpu.VMEM((4, 2, SUB, LANE), F32),
                pltpu.VMEM((NR, LANE), F32),
                sems((16,)), sems((20,)), sems((N_COPY,)), sems((N_COPY,)),
            ],
            compiler_params=pltpu.CompilerParams(collective_id=0, has_side_effects=True, vmem_limit_bytes=VMEM_MAIN),
            name='ocean',
        )(*[pltpu.with_memory_space_constraint(x, pltpu.HBM) for x in (vel_u, vel_v, temperature, salinity, surf_eta, trans_u, trans_v, bottom_depth, level_count)])
        cube = jax.ShapeDtypeStruct((NL, NR, NT * LANE), F32)
        flat = jax.ShapeDtypeStruct((NR, NT * LANE), F32)
        return pl.pallas_call(
            functools.partial(finish_kernel, n_row, n_sub),
            out_shape=[flat] * 3 + [cube] * 4,
            in_specs=[smem] + [vmem] * len(outs),
            out_specs=[hbm] * 7,
            scratch_shapes=[wide1] * 6 + [force_v, force_v, wide1] + [flat_v] * 4 + [pltpu.VMEM((3, NT, NR, LANE), F32), cube_v, cube_v, sems((28,))],
            compiler_params=pltpu.CompilerParams(vmem_limit_bytes=VMEM_FINISH),
            name='finish',
        )(avg_weights, *mids)

    cube = P(None, 'row', 'col')
    flat = P('row', 'col')
    return jax.shard_map(step, mesh=mesh, in_specs=(cube, cube, cube, cube, flat, flat, flat, flat, flat, P()), out_specs=(flat, flat, flat, cube, cube, cube, cube), check_vma=False)
```

```python
import functools

import jax
import jax.numpy as jnp
from jax import lax
from jax.experimental import pallas as pl
from jax.experimental.pallas import tpu as pltpu
from jax.sharding import PartitionSpec as P

TIME_STEP = 1.0
GRAVITY = 16.0
BC_GRAVITY = 4.0
EXPAND_T = 0.2
CONTRACT_S = 0.6
CORIO_F0 = 0.4
CORIO_BETA = 0.4
VISC_R = 2.0
DIFF_R = 0.5

MESH = pl.DeviceIdType.MESH
F32 = jnp.float32

SUB = 8
LANE = 128
ZERO = 0.0
ONE = 1.0
NL = 31
NR = 32
NT = 4
RO = 8
WO = 40
WR = 112
N_COPY = 40
NH = 30
VMEM_MAIN = 40 * 1024 * 1024
VMEM_FINISH = 12 * 1024 * 1024


def factors(strength):
    inner, last = [], []
    before = ZERO
    for level in range(NL):
        low = ZERO if level == 0 else strength
        inner.append(strength / (ONE + low + strength - low * before))
        last.append(strength / (ONE + low - low * before))
        before = inner[-1]
    return inner, last


VISC_IN, VISC_END = factors(VISC_R)
DIFF_IN, DIFF_END = factors(DIFF_R)


def lanes():
    return lax.broadcasted_iota(jnp.int32, (SUB, LANE), 1)


def movers(height=SUB):
    here = lax.broadcasted_iota(jnp.int32, (height, LANE), 1)
    first, last = here == 0, here == LANE - 1

    def west_of(own, left):
        return pltpu.roll(lax.select(last, left, own), 1, 1)

    def east_of(own, right):
        return pltpu.roll(lax.select(first, right, own), LANE - 1, 1)

    return west_of, east_of


def corio(first, total_rows):
    pos = (first + lax.broadcasted_iota(jnp.int32, (SUB, LANE), 0)).astype(F32)
    fu = CORIO_F0 + CORIO_BETA * ((pos + 0.5) / total_rows - 0.5)
    fv = CORIO_F0 + CORIO_BETA * ((pos + ONE) / total_rows - 0.5)
    return fu, fv


def ocean_kernel(n_row, n_sub,
                 u_in, v_in, t_in, s_in, eta_in, tu_in, tv_in, dep_in, cnt_in,
                 us_o, vs_o, tn_o, sn_o, wide, abuf, lu_o, lv_o, hu_s, hv_s, mu_s, mv_s,
                 fb, pb, uw_b, ve_b, near, relay, wsend, cnt_i, pk_s, pk_r, asend,
                 in_sem, w_sem, send, recv):
    row = lax.axis_index('row')
    col = lax.axis_index('col')
    ocol = 1 - col
    has_s = row > 0
    has_n = row < n_row - 1
    dtb = TIME_STEP / n_sub
    total_rows = float(n_row * NR)
    used = []
    ub, vb, tb, sb = (fb.at[f] for f in range(4))
    zero8 = jnp.zeros((SUB, LANE), F32)
    west_of, east_of = movers()
    west_all, east_all = movers(NR)
    all_rows = pl.ds(RO, NR)
    cnt, depth = near.at[0], near.at[1]
    half_row = n_row // 2
    up, down = row == half_row - 1, row == half_row
    first_row, last_row = row == 0, row == n_row - 1

    def dev(step, c):
        return {'row': row + step, 'col': c}

    def remote(src, dst, device):
        used.append(0)
        idx = len(used) - 1
        return pltpu.make_async_remote_copy(src, dst, send.at[idx], recv.at[idx], device_id=device, device_id_type=MESH)

    def start(copies):
        for cp in copies:
            cp.start()

    def both(south, north, action):
        @pl.when(has_s)
        def _():
            for cp in south:
                action(cp)

        @pl.when(has_n)
        def _():
            for cp in north:
                action(cp)

    def arrived(south_from, north_from):
        both(south_from, north_from, lambda cp: cp.wait_recv())

    wloads, loads = {}, {}
    for f, src in enumerate((eta_in, tv_in, tu_in, dep_in, cnt_in)):
        for t in range(NT):
            dst = wide.at[f, t, pl.ds(WO, NR), :] if f < 4 else cnt_i.at[t]
            wloads[f, t] = pltpu.make_async_copy(src.at[:, pl.ds(LANE * t, LANE)], dst, w_sem.at[f * NT + t])
    for f, src in enumerate((u_in, v_in, t_in, s_in)):
        for t in range(NT):
            loads[f, t] = pltpu.make_async_copy(src.at[:, :, pl.ds(LANE * t, LANE)], fb.at[f, t, :, pl.ds(RO, NR), :], in_sem.at[f * NT + t])
    for t in range(NT):
        wloads[5, t] = pltpu.make_async_copy(dep_in.at[:, pl.ds(LANE * t, LANE)], near.at[1, t, pl.ds(RO, NR), :], w_sem.at[5 * NT + t])
    start(wloads.values())
    order = [(f, t) for g in (0, 2) for tiles in ((0, 3), (1, 2)) for f in (g, g + 1) for t in tiles]
    start([loads[key] for key in order])

    for i in range(5):
        for rr in (0, SUB, WR - 2 * SUB, WR - SUB):
            for f in range(4):
                wide[f, i, pl.ds(rr, SUB), :] = zero8
            for f in range(2):
                abuf[f, i, pl.ds(rr, SUB), :] = zero8

    barrier = pltpu.get_barrier_semaphore()
    pl.semaphore_signal(barrier, inc=1, device_id=dev(0, ocol), device_id_type=MESH)

    @pl.when(has_n)
    def _():
        for c in (col, ocol):
            pl.semaphore_signal(barrier, inc=1, device_id=dev(1, c), device_id_type=MESH)

    @pl.when(has_s)
    def _():
        for c in (col, ocol):
            pl.semaphore_signal(barrier, inc=1, device_id=dev(-1, c), device_id_type=MESH)

    def greet(rows_of):
        for d in rows_of:
            pl.semaphore_signal(barrier, inc=1, device_id=dev(d, col), device_id_type=MESH)

    pl.when(up)(lambda: greet((half_row, 1 - half_row)))
    pl.when(down)(lambda: greet((half_row - 1, -half_row)))
    pl.when(first_row)(lambda: greet((half_row - 1, half_row)))
    pl.when(last_row)(lambda: greet((-half_row, 1 - half_row)))

    def fill(first3, first2):
        def body(i, _):
            for f in range(4):
                fb[f, i, :, pl.ds(first3, SUB), :] = jnp.zeros((NL, SUB, LANE), F32)
            return 0
        lax.fori_loop(0, 5, body, 0)
        for i in range(5):
            for f in range(4):
                wide[f, i, pl.ds(first2, NR), :] = jnp.zeros((NR, LANE), F32)
            for f in range(2):
                abuf[f, i, pl.ds(first2, NR), :] = jnp.zeros((NR, LANE), F32)
            for f in range(2):
                near[f, i, pl.ds(first3, SUB), :] = zero8

    @pl.when(jnp.logical_not(has_s))
    def _():
        fill(0, WO - NR)

    @pl.when(jnp.logical_not(has_n))
    def _():
        fill(RO + NR, WO + NR)

    for cp in wloads.values():
        cp.wait()
    for t in range(NT):
        cnt[t, pl.ds(RO, NR), :] = cnt_i[t].astype(F32)
    lane = lanes()
    outer = lane < LANE // 2
    middle = jnp.logical_and(lane >= NR, lane < LANE - NR)

    def edges(buf, f, first):
        rows = pl.ds(first, SUB)
        return jnp.where(outer, buf[f, 0, rows, :], buf[f, 3, rows, :])

    def paired(buf, f, g, first):
        return jnp.where(middle, pltpu.roll(edges(buf, g, first), LANE // 2, 1), edges(buf, f, first))

    for j in range(4):
        mine = pl.ds(SUB * j, SUB)
        first = WO + SUB * j
        for f in range(2):
            wsend[f, mine, :] = paired(wide, f, f + 2, first)
        own = pl.ds(RO + SUB * j, SUB)
        for f in range(2):
            wsend[2 + f, mine, :] = jnp.where(outer, near[f, 0, own, :], near[f, 3, own, :])

    round_about = jnp.logical_or(jnp.logical_or(up, down), jnp.logical_or(first_row, last_row))
    barrier_count = 1 + 2 * has_n.astype(jnp.int32) + 2 * has_s.astype(jnp.int32) + 2 * round_about.astype(jnp.int32)
    pl.semaphore_wait(barrier, barrier_count)

    own4 = pl.ds(0, NT)
    two = pl.ds(0, 2)
    top, low, north, south = RO + NR - 1, RO, RO + NR, RO - 1
    n_src, n_dst, s_src, s_dst = WO + NR - NH, WO - NH, WO, WO + NR

    def rows3(f, a, b, d):
        return remote(fb.at[f, own4, :, pl.ds(a, 1), :], fb.at[f, own4, :, pl.ds(b, 1), :], dev(d, col))

    def rows2(buf, f, nf, a, b, d):
        return remote(buf.at[pl.ds(f, nf), own4, pl.ds(a, NH), :], buf.at[pl.ds(f, nf), own4, pl.ds(b, NH), :], dev(d, col))

    def row1(a, b, d):
        return remote(near.at[:, own4, pl.ds(a, 1), :], near.at[:, own4, pl.ds(b, 1), :], dev(d, col))

    def corner(a, b, d):
        return remote(wsend.at[two, pl.ds(a - WO, NH), :], wide.at[two, 4, pl.ds(b, NH), :], dev(d, ocol))

    z_wide = [
        remote(wsend.at[pl.ds(2, 2)], near.at[:, 4, pl.ds(RO, NR), :], dev(0, ocol)),
        remote(wsend.at[two], wide.at[two, 4, pl.ds(WO, NR), :], dev(0, ocol)),
    ]
    n_first = [row1(top, south, 1)]
    s_first = [row1(low, north, -1)]

    def via(src_row, dst_row, there, onward):
        leg1 = remote(wide.at[:, own4, pl.ds(src_row, NH), :], relay, dev(there, col))
        leg2 = remote(relay, wide.at[:, own4, pl.ds(dst_row, NH), :], dev(onward, col))
        return leg1, leg2

    n_leg1, n_leg2 = via(n_src, n_dst, half_row, 1 - half_row)
    s_leg1, s_leg2 = via(s_src, s_dst, -half_row, half_row - 1)
    pl.when(up)(n_leg1.start)
    pl.when(down)(s_leg1.start)
    start(z_wide)
    both(s_first, n_first, lambda cp: cp.start())

    def slot(k, j):
        return (4 * k + j) // 64, 2 * ((4 * k + j) % 64)

    def pack(half_of, _):
        here = lanes()
        first = lax.broadcasted_iota(jnp.int32, (NR, LANE), 1) == 0
        acc = {}
        for k in range(NL):
            for f in range(2):
                field = 2 * half_of + f
                both_edges = lax.select(first, fb[field, 0, k, all_rows, :], fb[field, 3, k, all_rows, :])
                for j in range(4):
                    word, at = slot(k, j)
                    pair = both_edges[SUB * j:SUB * (j + 1)]
                    if at:
                        mine = jnp.logical_or(here == at, here == at - 1)
                        acc[f, word] = lax.select(mine, pltpu.roll(pair, at, 1), acc[f, word])
                    else:
                        acc[f, word] = pair
        for f, word in acc:
            pk_s[2 * half_of + f, word] = acc[f, word]
        return 0

    def unpack(half_of, _):
        for f in range(2):
            field = 2 * half_of + f
            got = [pk_r[field, word] for word in range(2)]
            for k in range(NL):
                parts = []
                for j in range(4):
                    word, at = slot(k, j)
                    parts.append(pltpu.roll(got[word], LANE - at, 1) if at else got[word])
                fb[field, 4, k, all_rows, :] = jnp.concatenate(parts, axis=0)
        return 0

    def shift_u(t):
        for k in range(NL):
            uw_b[t, k, all_rows, :] = west_all(ub[t, k, all_rows, :], ub[lax.rem(t + 4, 5), k, all_rows, :])

    def shift_v(t):
        for k in range(NL):
            ve_b[t, k, all_rows, :] = east_all(vb[t, k, all_rows, :], vb[t + 1, k, all_rows, :])

    for t in (0, 3, 1, 2):
        for f in (0, 1):
            loads[f, t].wait()
    n_vel = [rows3(0, top, south, 1), rows3(1, top, south, 1),
             remote(fb.at[1, 0, :, pl.ds(top, 1), :], fb.at[1, 4, :, pl.ds(south, 1), :], dev(1, ocol))]
    s_vel = [rows3(0, low, north, -1), rows3(1, low, north, -1),
             remote(fb.at[0, 3, :, pl.ds(low, 1), :], fb.at[0, 4, :, pl.ds(north, 1), :], dev(-1, ocol))]
    both(s_vel, n_vel, lambda cp: cp.start())

    def shift_own(t, _):
        shift_u(t + 1)
        shift_v(t)
        return 0
    lax.fori_loop(0, 3, shift_own, 0)

    for t in (0, 3, 1, 2):
        for f in (2, 3):
            loads[f, t].wait()
    n_tra = [rows3(2, top, south, 1), rows3(3, top, south, 1)]
    s_tra = [rows3(2, low, north, -1), rows3(3, low, north, -1)]
    n_far, s_far = rows2(wide, 0, 4, n_src, n_dst, 1), rows2(wide, 0, 4, s_src, s_dst, -1)
    n_cor, s_cor = corner(n_src, n_dst, 1), corner(s_src, s_dst, -1)
    both(s_tra, n_tra, lambda cp: cp.start())
    far_n, far_s = jnp.logical_and(has_n, jnp.logical_not(up)), jnp.logical_and(has_s, jnp.logical_not(down))
    pl.when(far_n)(n_far.start)
    pl.when(far_s)(s_far.start)
    both([s_cor], [n_cor], lambda cp: cp.start())
    lax.fori_loop(0, 2, pack, 0)
    z_col = remote(pk_s, pk_r, dev(0, ocol))
    z_col.start()

    p_unit = 0.5 * BC_GRAVITY / NL

    def pressure(t, rows, height):
        total = jnp.zeros((height, LANE), F32)
        for k in range(NL):
            part = (p_unit * CONTRACT_S) * sb[t, k, rows, :] - (p_unit * EXPAND_T) * tb[t, k, rows, :]
            here = total + part
            pb[t, k, rows, :] = here
            total = here + part

    def pressure_own(t, _):
        pressure(t, all_rows, NR)
        return 0
    lax.fori_loop(0, NT, pressure_own, 0)

    def near2d(buf, first, t):
        c = buf[t, pl.ds(first, SUB), :]
        return c, east_of(c, buf[t + 1, pl.ds(first, SUB), :]), buf[t, pl.ds(first + 1, SUB), :]

    def pick(mask, inner, last):
        return lax.select(mask, jnp.full((SUB, LANE), inner, F32), jnp.full((SUB, LANE), last, F32))

    def keep(mask, value):
        return lax.select(mask, value, zero8)

    def momentum(lt, j, at_south=False, at_north=False):
        rc, rn, rs = pl.ds(RO + SUB * j, SUB), pl.ds(RO + 1 + SUB * j, SUB), pl.ds(RO - 1 + SUB * j, SUB)
        ro = pl.ds(SUB * j, SUB)
        t, right, left = lt, lax.rem(lt + 1, 5), lax.rem(lt + 4, 5)
        fu, fv = corio(row * NR + SUB * j, total_rows)
        fu4 = 0.25 * fu
        fv4 = 0.25 * fv
        c0, ce, cn = near2d(cnt, RO + SUB * j, lt)
        lu = jnp.minimum(c0, ce)
        lv = jnp.minimum(c0, cn)
        d0, de, dn = near2d(depth, RO + SUB * j, lt)
        hu = 0.5 * (d0 + de)
        hv = 0.5 * (d0 + dn)
        lu_o[lt, ro, :] = lu
        lv_o[lt, ro, :] = lv
        hu_s[lt, ro, :] = hu
        hv_s[lt, ro, :] = hv
        yu, yv = zero8, zero8
        su, sv = zero8, zero8
        for k in range(NL):
            u = ub[t, k, rc, :]
            v = vb[t, k, rc, :]
            uw = uw_b[t, k, rc, :]
            ue = east_of(u, ub[right, k, rc, :])
            un = ub[t, k, rn, :]
            us = ub[t, k, rs, :]
            unw = west_of(un, ub[left, k, rn, :]) if at_north else uw_b[t, k, rn, :]
            vw = west_of(v, vb[left, k, rc, :])
            ve = ve_b[t, k, rc, :]
            vn = vb[t, k, rn, :]
            vs = vb[t, k, rs, :]
            vse = east_of(vs, vb[right, k, rs, :]) if at_south else ve_b[t, k, rs, :]
            v4 = (v + ve) + (vs + vse)
            u4 = (u + uw) + (un + unw)
            p = pb[t, k, rc, :]
            pe = east_of(p, pb[right, k, rc, :])
            pn = pb[t, k, rn, :]
            ustar = u + (v4 * (fu4 - 0.125 * (un - us)) - 0.5 * u * (ue - uw) - (pe - p))
            vstar = v - (u4 * (fv4 + 0.125 * (ve - vw)) + 0.5 * v * (vn - vs) + (pn - p))
            yu = (ustar + yu) * (pick(lu > k + 1, VISC_IN[k], VISC_END[k]) if k < NL - 1 else VISC_END[k])
            yv = (vstar + yv) * (pick(lv > k + 1, VISC_IN[k], VISC_END[k]) if k < NL - 1 else VISC_END[k])
            us_o[lt, k, ro, :] = yu
            vs_o[lt, k, ro, :] = yv
            su = su + keep(lu > k, u)
            sv = sv + keep(lv > k, v)
        mu, mv = zero8, zero8
        xu, xv = zero8, zero8
        for k in reversed(range(NL)):
            xu = us_o[lt, k, ro, :] + (keep(lu > k + 1, VISC_IN[k] * xu) if k < NL - 1 else ZERO)
            xv = vs_o[lt, k, ro, :] + (keep(lv > k + 1, VISC_IN[k] * xv) if k < NL - 1 else ZERO)
            outu = (ONE / VISC_R) * xu
            outv = (ONE / VISC_R) * xv
            us_o[lt, k, ro, :] = outu
            vs_o[lt, k, ro, :] = outv
            mu = mu + keep(lu > k, outu)
            mv = mv + keep(lv > k, outv)
        iu = ONE / jnp.maximum(lu, ONE)
        iv = ONE / jnp.maximum(lv, ONE)
        mu_s[lt, ro, :] = mu * iu
        mv_s[lt, ro, :] = mv * iv
        scale = dtb * dtb / TIME_STEP
        rw = pl.ds(WO + SUB * j, SUB)
        abuf[0, lt, rw, :] = jnp.where(lu > ZERO, scale * hu * ((mu - su) * iu), ZERO)
        abuf[1, lt, rw, :] = jnp.where(lv > ZERO, scale * hv * ((mv - sv) * iv), ZERO)

    def middle_rows(i, _):
        odd, later = lax.rem(i, 2), i // 4

        @pl.when(jnp.logical_and(i == 6, last_row))
        def _():
            n_leg1.wait_recv()
            n_leg2.start()

        @pl.when(jnp.logical_and(i == 6, first_row))
        def _():
            s_leg1.wait_recv()
            s_leg2.start()

        @pl.when(i == 4)
        def _():
            for cp in (z_wide[0], z_col):
                cp.wait_recv()
            lax.fori_loop(0, 2, unpack, 0)
            shift_u(0)
            shift_v(3)
            pressure(4, all_rows, NR)

        momentum(1 + odd + later * (2 * odd - 1), 1 + lax.rem(i, 4) // 2)
        return 0

    lax.fori_loop(0, SUB, middle_rows, 0)

    arrived(n_first + n_vel, s_first + s_vel + s_tra)

    def pressure_north(i, _):
        for odd in range(2):
            pressure(2 * i + odd, pl.ds(RO + NR, SUB), SUB)
        return 0
    lax.fori_loop(0, 2, pressure_north, 0)

    def force_corner(a, b, d):
        return remote(asend.at[pl.ds(a - WO, NH), :], abuf.at[0, 4, pl.ds(b, NH), :], dev(d, ocol))

    def force_rows(t, a, b, d):
        return remote(abuf.at[:, t, pl.ds(a, NH), :], abuf.at[:, t, pl.ds(b, NH), :], dev(d, col))

    def force_pair(t):
        return force_rows(t, n_src, n_dst, 1), force_rows(t, s_src, s_dst, -1)

    z_force = remote(asend, abuf.at[0, 4, pl.ds(WO, NR), :], dev(0, ocol))
    n_fcor, s_fcor = force_corner(n_src, n_dst, 1), force_corner(s_src, s_dst, -1)

    force = [force_pair(t) for t in range(NT)]
    n_force = [p[0] for p in force] + [n_fcor]
    s_force = [p[1] for p in force] + [s_fcor]

    def send_force(which):
        both([s_force[i] for i in which], [n_force[i] for i in which], lambda cp: cp.start())

    def ends(i, _):
        t = lax.rem(3 * i, 4)
        momentum(t, 0, at_south=True)
        momentum(t, 3, at_north=True)

        @pl.when(i == 1)
        def _():
            for j in range(4):
                asend[pl.ds(SUB * j, SUB), :] = paired(abuf, 0, 1, WO + SUB * j)
            z_force.start()
            send_force((0, 3, 4))

        @pl.when(i == 2)
        def _():
            send_force((2,))
        return 0

    lax.fori_loop(0, NT, ends, 0)
    send_force((1,))

    arrived(n_tra, [])

    def tracers(lt, j):
        rc, rn, rs = pl.ds(RO + SUB * j, SUB), pl.ds(RO + 1 + SUB * j, SUB), pl.ds(RO - 1 + SUB * j, SUB)
        ro = pl.ds(SUB * j, SUB)
        t, right, left = lt, lax.rem(lt + 1, 5), lax.rem(lt + 4, 5)
        c0 = cnt[lt, rc, :]
        luw = jnp.minimum(c0, west_of(c0, cnt[left, rc, :]))
        lvs = jnp.minimum(c0, cnt[lt, rs, :])
        lu = lu_o[lt, ro, :]
        lv = lv_o[lt, ro, :]
        half_dt = 0.5 * TIME_STEP
        yt, ys = zero8, zero8
        for k in range(NL):
            u = ub[t, k, rc, :]
            me = keep(lu > k, half_dt * u)
            mw = keep(luw > k, half_dt * uw_b[t, k, rc, :])
            mn = keep(lv > k, half_dt * vb[t, k, rc, :])
            ms = keep(lvs > k, half_dt * vb[t, k, rs, :])

            def advect(buf):
                q = buf[t, k, rc, :]
                qe = east_of(q, buf[right, k, rc, :])
                qw = west_of(q, buf[left, k, rc, :])
                qn = buf[t, k, rn, :]
                qs = buf[t, k, rs, :]
                return q - ((me * (q + qe) - mw * (qw + q)) + (mn * (q + qn) - ms * (qs + q)))

            qt = advect(tb)
            qs_ = advect(sb)
            fac = pick(c0 > k + 1, DIFF_IN[k], DIFF_END[k]) if k < NL - 1 else DIFF_END[k]
            yt = jnp.where(c0 > k, (qt + yt) * fac, DIFF_R * qt)
            ys = jnp.where(c0 > k, (qs_ + ys) * fac, DIFF_R * qs_)
            tn_o[lt, k, ro, :] = yt
            sn_o[lt, k, ro, :] = ys
        xt, xs_ = zero8, zero8
        for k in reversed(range(NL)):
            xt = tn_o[lt, k, ro, :] + (keep(c0 > k + 1, DIFF_IN[k] * xt) if k < NL - 1 else ZERO)
            xs_ = sn_o[lt, k, ro, :] + (keep(c0 > k + 1, DIFF_IN[k] * xs_) if k < NL - 1 else ZERO)
            tn_o[lt, k, ro, :] = (ONE / DIFF_R) * xt
            sn_o[lt, k, ro, :] = (ONE / DIFF_R) * xs_

    def tracers_all(i, _):
        tracers(lax.rem(i, 4), i // 4)
        return 0
    lax.fori_loop(0, 16, tracers_all, 0)

    z_wide[1].wait_recv()
    z_force.wait_recv()
    pl.when(far_s)(n_far.wait_recv)
    pl.when(far_n)(s_far.wait_recv)
    pl.when(down)(n_leg2.wait_recv)
    pl.when(up)(s_leg2.wait_recv)
    arrived([n_cor] + n_force, [s_cor] + s_force)

    for cp in z_wide + [z_col, z_force]:
        cp.wait_send()
    both(s_first + s_vel + s_tra + [s_cor] + s_force, n_first + n_vel + n_tra + [n_cor] + n_force, lambda cp: cp.wait_send())
    pl.when(far_n)(n_far.wait_send)
    pl.when(far_s)(s_far.wait_send)
    pl.when(up)(n_leg1.wait_send)
    pl.when(down)(s_leg1.wait_send)
    pl.when(last_row)(n_leg2.wait_send)
    pl.when(first_row)(s_leg2.wait_send)


def finish_kernel(n_row, n_sub, w_ref,
                  us, vs, tn, sn, wide, abuf, lu, lv, hu_s, hv_s, mu_s, mv_s,
                  eta_o, tu_o, tv_o, u_o, v_o, t_o, s_o,
                  bu, bv, cfu, cfv, mku, mkv, tu, tv, xs, acu, acv, cu, cv, flat_b, ubuf, vbuf, sem):
    row = lax.axis_index('row')
    dtb = TIME_STEP / n_sub
    total_rows = float(n_row * NR)
    zero8 = jnp.zeros((SUB, LANE), F32)
    west_of, east_of = movers()
    copies = []

    def put(src, dst):
        cp = pltpu.make_async_copy(src, dst, sem.at[len(copies)])
        cp.start()
        copies.append(cp)

    for src, dst in ((tn, t_o), (sn, s_o)):
        for t in range(NT):
            put(src.at[t], dst.at[:, :, pl.ds(LANE * t, LANE)])

    def setup(i, _):
        base = SUB + SUB * i
        rows = pl.ds(base, SUB)
        rown = pl.ds(base + 1, SUB)
        first = row * NR + SUB * i - NR
        fu, fv = corio(first, total_rows)
        place = first + lax.broadcasted_iota(jnp.int32, (SUB, LANE), 0)
        inside = place >= 0
        wet_u = jnp.logical_and(inside, place < n_row * NR).astype(F32)
        wet_v = jnp.logical_and(inside, place < n_row * NR - 1).astype(F32)
        for t in range(5):
            right = (t + 1) % 5
            d0 = wide[3, t, rows, :]
            scale = 0.5 * dtb * dtb * GRAVITY
            bu[t, rows, :] = wet_u * (scale * (d0 + east_of(d0, wide[3, right, rows, :])))
            bv[t, rows, :] = wet_v * (scale * (d0 + wide[3, t, rown, :]))
            cfu[t, rows, :] = wet_u * ((0.25 * dtb) * fu)
            cfv[t, rows, :] = wet_v * ((0.25 * dtb) * fv)
            mku[t, rows, :] = wet_u
            mkv[t, rows, :] = wet_v
            tu[0, t, rows, :] = dtb * wide[2, t, rows, :]
            tv[0, t, rows, :] = dtb * wide[1, t, rows, :]
        return 0

    for i in range(12):
        rows = pl.ds(SUB + SUB * i, SUB)
        for f in range(2):
            wide[f + 2, 4, rows, :] = pltpu.roll(wide[f, 4, rows, :], LANE // 2, 1)
        abuf[1, 4, rows, :] = pltpu.roll(abuf[0, 4, rows, :], LANE // 2, 1)
    lax.fori_loop(0, 12, setup, 0)
    for t in range(NT):
        acu[t] = jnp.zeros((NR, LANE), F32)
        acv[t] = jnp.zeros((NR, LANE), F32)

    def subcycle(n, cur, lo, hi, first=False):
        nxt = 1 - cur
        weight = w_ref[n] * (ONE / dtb)
        for i in range(lo, hi):
            rows = pl.ds(SUB + SUB * i, SUB)
            rows_s = pl.ds(7 + SUB * i, SUB)
            us = [tu[cur, t, rows, :] for t in range(5)]
            for t in range(5):
                uw = west_of(us[t], us[(t + 4) % 5])
                xs[t, rows, :] = us[t] + uw
                wide[0, t, rows, :] = wide[0, t, rows, :] - ((us[t] - uw) + (tv[cur, t, rows, :] - tv[cur, t, rows_s, :]))
        for i in range(lo, hi):
            rows = pl.ds(SUB + SUB * i, SUB)
            rows_s = pl.ds(7 + SUB * i, SUB)
            rows_n = pl.ds(9 + SUB * i, SUB)
            es = [wide[0, t, rows, :] for t in range(5)]
            v0 = [tv[cur, t, rows, :] for t in range(5)]
            v2 = [v0[t] + tv[cur, t, rows_s, :] for t in range(5)]
            for t in range(5):
                right = (t + 1) % 5
                v4 = v2[t] + east_of(v2[t], v2[right])
                slope_u = east_of(es[t], es[right]) - es[t]
                slope_v = wide[0, t, rows_n, :] - es[t]
                u4 = xs[t, rows, :] + xs[t, rows_n, :]
                u_old = tu[cur, t, rows, :]
                v_old = v0[t]
                if first:
                    u_old = mku[t, rows, :] * u_old
                    v_old = mkv[t, rows, :] * v_old
                u_new = (u_old + abuf[0, t, rows, :]) + (cfu[t, rows, :] * v4 - bu[t, rows, :] * slope_u)
                v_new = (v_old + abuf[1, t, rows, :]) - (cfv[t, rows, :] * u4 + bv[t, rows, :] * slope_v)
                tu[nxt, t, rows, :] = u_new
                tv[nxt, t, rows, :] = v_new
                if 4 <= i < SUB and t < NT:
                    ro = pl.ds(SUB * (i - 4), SUB)
                    acu[t, ro, :] += weight * u_new
                    acv[t, ro, :] += weight * v_new

    def pairs(first_n, count, lo, hi):
        def body(i, _):
            n = first_n + 2 * i
            subcycle(n, 0, lo, hi)
            subcycle(n + 1, 1, lo, hi)
            return 0
        lax.fori_loop(0, count, body, 0)

    subcycle(0, 0, 0, 12, first=True)
    subcycle(1, 1, 0, 12)
    pairs(2, 2, 0, 12)
    pairs(6, 4, 1, 11)
    pairs(14, 4, 2, 10)
    pairs(22, 4, 3, 9)

    for t in range(NT):
        for j in range(4):
            rw = pl.ds(WO + SUB * j, SUB)
            ro = pl.ds(SUB * j, SUB)
            flat_b[0, t, ro, :] = wide[0, t, rw, :]
            flat_b[1, t, ro, :] = (ONE / dtb) * tu[0, t, rw, :]
            flat_b[2, t, ro, :] = (ONE / dtb) * tv[0, t, rw, :]
            cu[t, ro, :] = acu[t, ro, :] / hu_s[t, ro, :] - mu_s[t, ro, :]
            hv = hv_s[t, ro, :]
            cv[t, ro, :] = acv[t, ro, :] / hv - mv_s[t, ro, :]

    for f, dst in enumerate((eta_o, tu_o, tv_o)):
        for t in range(NT):
            put(flat_b.at[f, t], dst.at[:, pl.ds(LANE * t, LANE)])
    for lev, cor, src, buf, dst in ((lu, cu, us, ubuf, u_o), (lv, cv, vs, vbuf, v_o)):
        for t in range(NT):
            for j in range(4):
                ro = pl.ds(SUB * j, SUB)
                count = lev[t, ro, :]
                shift = cor[t, ro, :]
                for k in range(NL):
                    buf[t, k, ro, :] = jnp.where(count > k, src[t, k, ro, :] + shift, ZERO)
            put(buf.at[t], dst.at[:, :, pl.ds(LANE * t, LANE)])
    for cp in copies:
        cp.wait()


def solution(mesh):
    n_row = mesh.shape['row']

    def step(vel_u, vel_v, temperature, salinity, surf_eta, trans_u, trans_v, bottom_depth, level_count, avg_weights):
        n_sub = avg_weights.shape[0]
        hbm = pl.BlockSpec(memory_space=pltpu.HBM)
        vmem = pl.BlockSpec(memory_space=pltpu.VMEM)
        smem = pl.BlockSpec(memory_space=pltpu.SMEM)
        cube_v = pltpu.VMEM((NT, NL, NR, LANE), F32)
        flat_v = pltpu.VMEM((NT, NR, LANE), F32)
        wide1 = pltpu.VMEM((5, WR, LANE), F32)
        wide_v = pltpu.VMEM((4, 5, WR, LANE), F32)
        force_v = pltpu.VMEM((2, 5, WR, LANE), F32)
        sems = pltpu.SemaphoreType.DMA
        outs = [cube_v] * 4 + [wide_v, force_v] + [flat_v] * 6
        mids = pl.pallas_call(
            functools.partial(ocean_kernel, n_row, n_sub),
            out_shape=outs,
            in_specs=[hbm] * 9,
            out_specs=[vmem] * len(outs),
            scratch_shapes=[
                pltpu.VMEM((4, 5, NL, RO + NR + SUB, LANE), F32),
                pltpu.VMEM((5, NL, RO + NR + SUB, LANE), F32),
                pltpu.VMEM((NT, NL, RO + NR + SUB, LANE), F32),
                pltpu.VMEM((NT, NL, RO + NR + SUB, LANE), F32),
                pltpu.VMEM((2, 5, RO + NR + SUB, LANE), F32),
                pltpu.VMEM((4, NT, NH, LANE), F32),
                pltpu.VMEM((4, NR, LANE), F32),
                pltpu.VMEM((NT, NR, LANE), jnp.int32),
                pltpu.VMEM((4, 2, SUB, LANE), F32),
                pltpu.VMEM((4, 2, SUB, LANE), F32),
                pltpu.VMEM((NR, LANE), F32),
                sems((16,)), sems((24,)), sems((N_COPY,)), sems((N_COPY,)),
            ],
            compiler_params=pltpu.CompilerParams(collective_id=0, has_side_effects=True, vmem_limit_bytes=VMEM_MAIN),
            name='ocean',
        )(*[pltpu.with_memory_space_constraint(x, pltpu.HBM) for x in (vel_u, vel_v, temperature, salinity, surf_eta, trans_u, trans_v, bottom_depth, level_count)])
        cube = jax.ShapeDtypeStruct((NL, NR, NT * LANE), F32)
        flat = jax.ShapeDtypeStruct((NR, NT * LANE), F32)
        return pl.pallas_call(
            functools.partial(finish_kernel, n_row, n_sub),
            out_shape=[flat] * 3 + [cube] * 4,
            in_specs=[smem] + [vmem] * len(outs),
            out_specs=[hbm] * 7,
            scratch_shapes=[wide1] * 6 + [force_v, force_v, wide1] + [flat_v] * 4 + [pltpu.VMEM((3, NT, NR, LANE), F32), cube_v, cube_v, sems((28,))],
            compiler_params=pltpu.CompilerParams(vmem_limit_bytes=VMEM_FINISH),
            name='finish',
        )(avg_weights, *mids)

    cube = P(None, 'row', 'col')
    flat = P('row', 'col')
    return jax.shard_map(step, mesh=mesh, in_specs=(cube, cube, cube, cube, flat, flat, flat, flat, flat, P()), out_specs=(flat, flat, flat, cube, cube, cube, cube), check_vma=False)
```

```python
import functools

import jax
import jax.numpy as jnp
from jax import lax
from jax.experimental import pallas as pl
from jax.experimental.pallas import tpu as pltpu
from jax.sharding import PartitionSpec as P

TIME_STEP = 1.0
GRAVITY = 16.0
BC_GRAVITY = 4.0
EXPAND_T = 0.2
CONTRACT_S = 0.6
CORIO_F0 = 0.4
CORIO_BETA = 0.4
VISC_R = 2.0
DIFF_R = 0.5

MESH = pl.DeviceIdType.MESH
F32 = jnp.float32

SUB = 8
LANE = 128
ZERO = 0.0
ONE = 1.0
NL = 31
NR = 32
NT = 4
RO = 8
WO = 40
WR = 112
N_COPY = 40
LATE = 2
T_TILES = 4
NH = 30
VMEM_MAIN = 40 * 1024 * 1024
VMEM_FINISH = 12 * 1024 * 1024


def factors(strength):
    inner, last = [], []
    before = ZERO
    for level in range(NL):
        low = ZERO if level == 0 else strength
        inner.append(strength / (ONE + low + strength - low * before))
        last.append(strength / (ONE + low - low * before))
        before = inner[-1]
    return inner, last


VISC_IN, VISC_END = factors(VISC_R)
DIFF_IN, DIFF_END = factors(DIFF_R)


def lanes():
    return lax.broadcasted_iota(jnp.int32, (SUB, LANE), 1)


def movers(height=SUB):
    here = lax.broadcasted_iota(jnp.int32, (height, LANE), 1)
    first, last = here == 0, here == LANE - 1

    def west_of(own, left):
        return pltpu.roll(lax.select(last, left, own), 1, 1)

    def east_of(own, right):
        return pltpu.roll(lax.select(first, right, own), LANE - 1, 1)

    return west_of, east_of


def corio(first, total_rows, height=SUB):
    pos = (first + lax.broadcasted_iota(jnp.int32, (height, LANE), 0)).astype(F32)
    fu = CORIO_F0 + CORIO_BETA * ((pos + 0.5) / total_rows - 0.5)
    fv = CORIO_F0 + CORIO_BETA * ((pos + ONE) / total_rows - 0.5)
    return fu, fv


def ocean_kernel(n_row, n_sub,
                 u_in, v_in, t_in, s_in, eta_in, tu_in, tv_in, dep_in, cnt_in,
                 us_o, vs_o, tn_o, sn_o, wide, abuf, lu_o, lv_o, hu_s, hv_s, mu_s, mv_s,
                 fb, pb, uw_b, ve_b, near, relay, wsend, cnt_i, pk_s, pk_r, asend,
                 in_sem, w_sem, send, recv):
    row = lax.axis_index('row')
    col = lax.axis_index('col')
    ocol = 1 - col
    has_s = row > 0
    has_n = row < n_row - 1
    dtb = TIME_STEP / n_sub
    total_rows = float(n_row * NR)
    used = []
    ub, vb, tb, sb = (fb.at[f] for f in range(4))
    zero8 = jnp.zeros((SUB, LANE), F32)
    west_of, east_of = movers()
    west_all, east_all = movers(NR)
    all_rows = pl.ds(RO, NR)
    cnt, depth = near.at[0], near.at[1]
    half_row = n_row // 2
    up, down = row == half_row - 1, row == half_row
    first_row, last_row = row == 0, row == n_row - 1

    def dev(step, c):
        return {'row': row + step, 'col': c}

    def remote(src, dst, device):
        used.append(0)
        idx = len(used) - 1
        return pltpu.make_async_remote_copy(src, dst, send.at[idx], recv.at[idx], device_id=device, device_id_type=MESH)

    def start(copies):
        for cp in copies:
            cp.start()

    def both(south, north, action):
        @pl.when(has_s)
        def _():
            for cp in south:
                action(cp)

        @pl.when(has_n)
        def _():
            for cp in north:
                action(cp)

    def arrived(south_from, north_from):
        both(south_from, north_from, lambda cp: cp.wait_recv())

    wloads, loads = {}, {}
    for f, src in enumerate((eta_in, tv_in, tu_in, dep_in, cnt_in)):
        for t in range(NT):
            dst = wide.at[f, t, pl.ds(WO, NR), :] if f < 4 else cnt_i.at[t]
            wloads[f, t] = pltpu.make_async_copy(src.at[:, pl.ds(LANE * t, LANE)], dst, w_sem.at[f * NT + t])
    for f, src in enumerate((u_in, v_in, t_in, s_in)):
        for t in range(NT):
            loads[f, t] = pltpu.make_async_copy(src.at[:, :, pl.ds(LANE * t, LANE)], fb.at[f, t, :, pl.ds(RO, NR), :], in_sem.at[f * NT + t])
    for t in range(NT):
        wloads[5, t] = pltpu.make_async_copy(dep_in.at[:, pl.ds(LANE * t, LANE)], near.at[1, t, pl.ds(RO, NR), :], w_sem.at[5 * NT + t])
    start(wloads.values())
    order = [(f, t) for g in (0, 2) for tiles in ((0, 3), (1, 2)) for f in (g, g + 1) for t in tiles]
    start([loads[key] for key in order])

    for i in range(5):
        for rr in (0, SUB, WR - 2 * SUB, WR - SUB):
            for f in range(4):
                wide[f, i, pl.ds(rr, SUB), :] = zero8
            for f in range(2):
                abuf[f, i, pl.ds(rr, SUB), :] = zero8

    barrier = pltpu.get_barrier_semaphore()
    pl.semaphore_signal(barrier, inc=1, device_id=dev(0, ocol), device_id_type=MESH)

    @pl.when(has_n)
    def _():
        for c in (col, ocol):
            pl.semaphore_signal(barrier, inc=1, device_id=dev(1, c), device_id_type=MESH)

    @pl.when(has_s)
    def _():
        for c in (col, ocol):
            pl.semaphore_signal(barrier, inc=1, device_id=dev(-1, c), device_id_type=MESH)

    def greet(rows_of):
        for d in rows_of:
            pl.semaphore_signal(barrier, inc=1, device_id=dev(d, col), device_id_type=MESH)

    pl.when(up)(lambda: greet((half_row, 1 - half_row)))
    pl.when(down)(lambda: greet((half_row - 1, -half_row)))
    pl.when(first_row)(lambda: greet((half_row - 1, half_row)))
    pl.when(last_row)(lambda: greet((-half_row, 1 - half_row)))

    def fill(first3, first2):
        def body(i, _):
            for f in range(4):
                fb[f, i, :, pl.ds(first3, SUB), :] = jnp.zeros((NL, SUB, LANE), F32)
            return 0
        lax.fori_loop(0, 5, body, 0)
        for i in range(5):
            for f in range(4):
                wide[f, i, pl.ds(first2, NR), :] = jnp.zeros((NR, LANE), F32)
            for f in range(2):
                abuf[f, i, pl.ds(first2, NR), :] = jnp.zeros((NR, LANE), F32)
            for f in range(2):
                near[f, i, pl.ds(first3, SUB), :] = zero8

    @pl.when(jnp.logical_not(has_s))
    def _():
        fill(0, WO - NR)

    @pl.when(jnp.logical_not(has_n))
    def _():
        fill(RO + NR, WO + NR)

    for cp in wloads.values():
        cp.wait()
    for t in range(NT):
        cnt[t, pl.ds(RO, NR), :] = cnt_i[t].astype(F32)
    lane = lanes()
    outer = lane < LANE // 2
    middle = jnp.logical_and(lane >= NR, lane < LANE - NR)

    def edges(buf, f, first):
        rows = pl.ds(first, SUB)
        return jnp.where(outer, buf[f, 0, rows, :], buf[f, 3, rows, :])

    def paired(buf, f, g, first):
        return jnp.where(middle, pltpu.roll(edges(buf, g, first), LANE // 2, 1), edges(buf, f, first))

    for j in range(4):
        mine = pl.ds(SUB * j, SUB)
        first = WO + SUB * j
        for f in range(2):
            wsend[f, mine, :] = paired(wide, f, f + 2, first)
        own = pl.ds(RO + SUB * j, SUB)
        for f in range(2):
            wsend[2 + f, mine, :] = jnp.where(outer, near[f, 0, own, :], near[f, 3, own, :])

    round_about = jnp.logical_or(jnp.logical_or(up, down), jnp.logical_or(first_row, last_row))
    barrier_count = 1 + 2 * has_n.astype(jnp.int32) + 2 * has_s.astype(jnp.int32) + 2 * round_about.astype(jnp.int32)
    pl.semaphore_wait(barrier, barrier_count)

    own4 = pl.ds(0, NT)
    two = pl.ds(0, 2)
    top, low, north, south = RO + NR - 1, RO, RO + NR, RO - 1
    n_src, n_dst, s_src, s_dst = WO + NR - NH, WO - NH, WO, WO + NR

    def rows3(f, a, b, d):
        return remote(fb.at[f, own4, :, pl.ds(a, 1), :], fb.at[f, own4, :, pl.ds(b, 1), :], dev(d, col))

    def rows2(buf, f, nf, a, b, d):
        return remote(buf.at[pl.ds(f, nf), own4, pl.ds(a, NH), :], buf.at[pl.ds(f, nf), own4, pl.ds(b, NH), :], dev(d, col))

    def row1(a, b, d):
        return remote(near.at[:, own4, pl.ds(a, 1), :], near.at[:, own4, pl.ds(b, 1), :], dev(d, col))

    def corner(a, b, d):
        return remote(wsend.at[two, pl.ds(a - WO, NH), :], wide.at[two, 4, pl.ds(b, NH), :], dev(d, ocol))

    z_wide = [
        remote(wsend.at[pl.ds(2, 2)], near.at[:, 4, pl.ds(RO, NR), :], dev(0, ocol)),
        remote(wsend.at[two], wide.at[two, 4, pl.ds(WO, NR), :], dev(0, ocol)),
    ]
    n_first = [row1(top, south, 1)]
    s_first = [row1(low, north, -1)]

    def via(src_row, dst_row, there, onward):
        leg1 = remote(wide.at[:, own4, pl.ds(src_row, NH), :], relay, dev(there, col))
        leg2 = remote(relay, wide.at[:, own4, pl.ds(dst_row, NH), :], dev(onward, col))
        return leg1, leg2

    n_leg1, n_leg2 = via(n_src, n_dst, half_row, 1 - half_row)
    s_leg1, s_leg2 = via(s_src, s_dst, -half_row, half_row - 1)
    pl.when(up)(n_leg1.start)
    pl.when(down)(s_leg1.start)
    start(z_wide)
    both(s_first, n_first, lambda cp: cp.start())

    def slot(k, j):
        return (4 * k + j) // 64, 2 * ((4 * k + j) % 64)

    def pack(half_of, _):
        here = lanes()
        first = lax.broadcasted_iota(jnp.int32, (NR, LANE), 1) == 0
        acc = {}
        for k in range(NL):
            for f in range(2):
                field = 2 * half_of + f
                both_edges = lax.select(first, fb[field, 0, k, all_rows, :], fb[field, 3, k, all_rows, :])
                for j in range(4):
                    word, at = slot(k, j)
                    pair = both_edges[SUB * j:SUB * (j + 1)]
                    if at:
                        mine = jnp.logical_or(here == at, here == at - 1)
                        acc[f, word] = lax.select(mine, pltpu.roll(pair, at, 1), acc[f, word])
                    else:
                        acc[f, word] = pair
        for f, word in acc:
            pk_s[2 * half_of + f, word] = acc[f, word]
        return 0

    def unpack(half_of, _):
        for f in range(2):
            field = 2 * half_of + f
            got = [pk_r[field, word] for word in range(2)]
            for k in range(NL):
                parts = []
                for j in range(4):
                    word, at = slot(k, j)
                    parts.append(pltpu.roll(got[word], LANE - at, 1) if at else got[word])
                fb[field, 4, k, all_rows, :] = jnp.concatenate(parts, axis=0)
        return 0

    def shift_u(t):
        for k in range(NL):
            uw_b[t, k, all_rows, :] = west_all(ub[t, k, all_rows, :], ub[lax.rem(t + 4, 5), k, all_rows, :])

    def shift_v(t):
        for k in range(NL):
            ve_b[t, k, all_rows, :] = east_all(vb[t, k, all_rows, :], vb[t + 1, k, all_rows, :])

    for t in (0, 3, 1, 2):
        for f in (0, 1):
            loads[f, t].wait()
    n_vel = [rows3(0, top, south, 1), rows3(1, top, south, 1),
             remote(fb.at[1, 0, :, pl.ds(top, 1), :], fb.at[1, 4, :, pl.ds(south, 1), :], dev(1, ocol))]
    s_vel = [rows3(0, low, north, -1), rows3(1, low, north, -1),
             remote(fb.at[0, 3, :, pl.ds(low, 1), :], fb.at[0, 4, :, pl.ds(north, 1), :], dev(-1, ocol))]
    both(s_vel, n_vel, lambda cp: cp.start())

    def shift_own(t, _):
        shift_u(t + 1)
        shift_v(t)
        return 0
    lax.fori_loop(0, 3, shift_own, 0)

    for t in (0, 3, 1, 2):
        for f in (2, 3):
            loads[f, t].wait()
    n_tra = [rows3(2, top, south, 1), rows3(3, top, south, 1)]
    s_tra = [rows3(2, low, north, -1), rows3(3, low, north, -1)]
    n_far, s_far = rows2(wide, 0, 4, n_src, n_dst, 1), rows2(wide, 0, 4, s_src, s_dst, -1)
    n_cor, s_cor = corner(n_src, n_dst, 1), corner(s_src, s_dst, -1)
    both(s_tra, [], lambda cp: cp.start())
    far_n, far_s = jnp.logical_and(has_n, jnp.logical_not(up)), jnp.logical_and(has_s, jnp.logical_not(down))
    lax.fori_loop(0, 2, pack, 0)
    z_col = remote(pk_s, pk_r, dev(0, ocol))
    z_col.start()

    p_unit = 0.5 * BC_GRAVITY / NL

    def pressure(t, rows, height):
        total = jnp.zeros((height, LANE), F32)
        for k in range(NL):
            part = (p_unit * CONTRACT_S) * sb[t, k, rows, :] - (p_unit * EXPAND_T) * tb[t, k, rows, :]
            here = total + part
            pb[t, k, rows, :] = here
            total = here + part

    def pressure_own(t, _):
        pressure(t, all_rows, NR)
        return 0
    lax.fori_loop(0, NT, pressure_own, 0)

    def chooser(height):
        nothing = jnp.zeros((height, LANE), F32)

        def pick(mask, inner, last):
            return lax.select(mask, jnp.full((height, LANE), inner, F32), jnp.full((height, LANE), last, F32))

        def keep(mask, value):
            return lax.select(mask, value, nothing)

        return nothing, pick, keep

    def momentum(lt, j, height=SUB, at_south=False, at_north=False):
        west_of, east_of = movers(height)
        zero8, pick, keep = chooser(height)

        def near2d(buf):
            c = buf[lt, rc, :]
            return c, east_of(c, buf[lt + 1, rc, :]), buf[lt, rn, :]

        rc, rn, rs = pl.ds(RO + SUB * j, height), pl.ds(RO + 1 + SUB * j, height), pl.ds(RO - 1 + SUB * j, height)
        ro = pl.ds(SUB * j, height)
        t, right, left = lt, lax.rem(lt + 1, 5), lax.rem(lt + 4, 5)
        fu, fv = corio(row * NR + SUB * j, total_rows, height)
        fu4 = 0.25 * fu
        fv4 = 0.25 * fv
        c0, ce, cn = near2d(cnt)
        lu = jnp.minimum(c0, ce)
        lv = jnp.minimum(c0, cn)
        d0, de, dn = near2d(depth)
        hu = 0.5 * (d0 + de)
        hv = 0.5 * (d0 + dn)
        lu_o[lt, ro, :] = lu
        lv_o[lt, ro, :] = lv
        hu_s[lt, ro, :] = hu
        hv_s[lt, ro, :] = hv
        yu, yv = zero8, zero8
        su, sv = zero8, zero8
        for k in range(NL):
            u = ub[t, k, rc, :]
            v = vb[t, k, rc, :]
            uw = uw_b[t, k, rc, :]
            ue = east_of(u, ub[right, k, rc, :])
            un = ub[t, k, rn, :]
            us = ub[t, k, rs, :]
            unw = west_of(un, ub[left, k, rn, :]) if at_north else uw_b[t, k, rn, :]
            vw = west_of(v, vb[left, k, rc, :])
            ve = ve_b[t, k, rc, :]
            vn = vb[t, k, rn, :]
            vs = vb[t, k, rs, :]
            vse = east_of(vs, vb[right, k, rs, :]) if at_south else ve_b[t, k, rs, :]
            v4 = (v + ve) + (vs + vse)
            u4 = (u + uw) + (un + unw)
            p = pb[t, k, rc, :]
            pe = east_of(p, pb[right, k, rc, :])
            pn = pb[t, k, rn, :]
            ustar = u + (v4 * (fu4 - 0.125 * (un - us)) - 0.5 * u * (ue - uw) - (pe - p))
            vstar = v - (u4 * (fv4 + 0.125 * (ve - vw)) + 0.5 * v * (vn - vs) + (pn - p))
            yu = (ustar + yu) * (pick(lu > k + 1, VISC_IN[k], VISC_END[k]) if k < NL - 1 else VISC_END[k])
            yv = (vstar + yv) * (pick(lv > k + 1, VISC_IN[k], VISC_END[k]) if k < NL - 1 else VISC_END[k])
            if k < NL - 1:
                us_o[lt, k, ro, :] = yu
                vs_o[lt, k, ro, :] = yv
            su = su + keep(lu > k, u)
            sv = sv + keep(lv > k, v)
        mu, mv = zero8, zero8
        xu, xv = zero8, zero8
        for k in reversed(range(NL)):
            xu = yu if k == NL - 1 else us_o[lt, k, ro, :] + (keep(lu > k + 1, VISC_IN[k] * xu))
            xv = yv if k == NL - 1 else vs_o[lt, k, ro, :] + (keep(lv > k + 1, VISC_IN[k] * xv))
            outu = (ONE / VISC_R) * xu
            outv = (ONE / VISC_R) * xv
            us_o[lt, k, ro, :] = outu
            vs_o[lt, k, ro, :] = outv
            mu = mu + keep(lu > k, outu)
            mv = mv + keep(lv > k, outv)
        iu = ONE / jnp.maximum(lu, ONE)
        iv = ONE / jnp.maximum(lv, ONE)
        mu_s[lt, ro, :] = mu * iu
        mv_s[lt, ro, :] = mv * iv
        scale = dtb * dtb / TIME_STEP
        rw = pl.ds(WO + SUB * j, height)
        abuf[0, lt, rw, :] = jnp.where(lu > ZERO, scale * hu * ((mu - su) * iu), ZERO)
        abuf[1, lt, rw, :] = jnp.where(lv > ZERO, scale * hv * ((mv - sv) * iv), ZERO)

    def middle_rows(i, _):
        odd, later = lax.rem(i, 2), i // 2

        @pl.when(jnp.logical_and(i == 3, last_row))
        def _():
            n_leg1.wait_recv()
            n_leg2.start()

        @pl.when(jnp.logical_and(i == 3, first_row))
        def _():
            s_leg1.wait_recv()
            s_leg2.start()

        @pl.when(i == LATE)
        def _():
            both([], n_tra, lambda cp: cp.start())
            pl.when(far_n)(n_far.start)
            pl.when(far_s)(s_far.start)
            both([s_cor], [n_cor], lambda cp: cp.start())

        @pl.when(i == 2)
        def _():
            for cp in (z_wide[0], z_col):
                cp.wait_recv()
            lax.fori_loop(0, 2, unpack, 0)
            shift_u(0)
            shift_v(3)
            pressure(4, all_rows, NR)

        momentum(1 + odd + later * (2 * odd - 1), 1, 2 * SUB)
        return 0

    lax.fori_loop(0, NT, middle_rows, 0)

    arrived(n_first + n_vel, s_first + s_vel + s_tra)

    def pressure_north(i, _):
        for odd in range(2):
            pressure(2 * i + odd, pl.ds(RO + NR, SUB), SUB)
        return 0
    lax.fori_loop(0, 2, pressure_north, 0)

    def force_corner(a, b, d):
        return remote(asend.at[pl.ds(a - WO, NH), :], abuf.at[0, 4, pl.ds(b, NH), :], dev(d, ocol))

    def force_rows(t, a, b, d):
        return remote(abuf.at[:, t, pl.ds(a, NH), :], abuf.at[:, t, pl.ds(b, NH), :], dev(d, col))

    def force_pair(t):
        return force_rows(t, n_src, n_dst, 1), force_rows(t, s_src, s_dst, -1)

    z_force = remote(asend, abuf.at[0, 4, pl.ds(WO, NR), :], dev(0, ocol))
    n_fcor, s_fcor = force_corner(n_src, n_dst, 1), force_corner(s_src, s_dst, -1)

    force = [force_pair(t) for t in range(NT)]
    n_force = [p[0] for p in force] + [n_fcor]
    s_force = [p[1] for p in force] + [s_fcor]

    def send_force(which):
        both([s_force[i] for i in which], [n_force[i] for i in which], lambda cp: cp.start())

    def ends(i, _):
        t = lax.rem(3 * i, 4)
        momentum(t, 0, at_south=True)
        momentum(t, 3, at_north=True)

        @pl.when(i == 1)
        def _():
            for j in range(4):
                asend[pl.ds(SUB * j, SUB), :] = paired(abuf, 0, 1, WO + SUB * j)
            z_force.start()
            send_force((0, 3, 4))

        @pl.when(i == 2)
        def _():
            send_force((2,))
        return 0

    lax.fori_loop(0, NT, ends, 0)
    send_force((1,))

    arrived(n_tra, [])

    def tracers(lt, j, height):
        west_of, east_of = movers(height)
        zero8, pick, keep = chooser(height)
        rc, rn, rs = pl.ds(RO + SUB * j, height), pl.ds(RO + 1 + SUB * j, height), pl.ds(RO - 1 + SUB * j, height)
        ro = pl.ds(SUB * j, height)
        t, right, left = lt, lax.rem(lt + 1, 5), lax.rem(lt + 4, 5)
        c0 = cnt[lt, rc, :]
        luw = jnp.minimum(c0, west_of(c0, cnt[left, rc, :]))
        lvs = jnp.minimum(c0, cnt[lt, rs, :])
        lu = lu_o[lt, ro, :]
        lv = lv_o[lt, ro, :]
        half_dt = 0.5 * TIME_STEP
        yt, ys = zero8, zero8
        for k in range(NL):
            u = ub[t, k, rc, :]
            me = keep(lu > k, u)
            mw = keep(luw > k, uw_b[t, k, rc, :])
            mn = keep(lv > k, vb[t, k, rc, :])
            ms = keep(lvs > k, vb[t, k, rs, :])

            def advect(buf):
                q = buf[t, k, rc, :]
                qe = east_of(q, buf[right, k, rc, :])
                qw = west_of(q, buf[left, k, rc, :])
                qn = buf[t, k, rn, :]
                qs = buf[t, k, rs, :]
                return q - half_dt * ((me * (q + qe) - mw * (qw + q)) + (mn * (q + qn) - ms * (qs + q)))

            qt = advect(tb)
            qs_ = advect(sb)
            fac = pick(c0 > k + 1, DIFF_IN[k], DIFF_END[k]) if k < NL - 1 else DIFF_END[k]
            yt = jnp.where(c0 > k, (qt + yt) * fac, DIFF_R * qt)
            ys = jnp.where(c0 > k, (qs_ + ys) * fac, DIFF_R * qs_)
            if k < NL - 1:
                tn_o[lt, k, ro, :] = yt
                sn_o[lt, k, ro, :] = ys
        xt, xs_ = zero8, zero8
        for k in reversed(range(NL)):
            xt = yt if k == NL - 1 else tn_o[lt, k, ro, :] + (keep(c0 > k + 1, DIFF_IN[k] * xt))
            xs_ = ys if k == NL - 1 else sn_o[lt, k, ro, :] + (keep(c0 > k + 1, DIFF_IN[k] * xs_))
            tn_o[lt, k, ro, :] = (ONE / DIFF_R) * xt
            sn_o[lt, k, ro, :] = (ONE / DIFF_R) * xs_

    def tracers_all(i, _):
        tracers(lax.rem(i, NT), T_TILES * (i // NT), T_TILES * SUB)
        return 0
    lax.fori_loop(0, 16 // T_TILES, tracers_all, 0)

    z_wide[1].wait_recv()
    z_force.wait_recv()
    pl.when(far_s)(n_far.wait_recv)
    pl.when(far_n)(s_far.wait_recv)
    pl.when(down)(n_leg2.wait_recv)
    pl.when(up)(s_leg2.wait_recv)
    arrived([n_cor] + n_force, [s_cor] + s_force)

    for cp in z_wide + [z_col, z_force]:
        cp.wait_send()
    both(s_first + s_vel + s_tra + [s_cor] + s_force, n_first + n_vel + n_tra + [n_cor] + n_force, lambda cp: cp.wait_send())
    pl.when(far_n)(n_far.wait_send)
    pl.when(far_s)(s_far.wait_send)
    pl.when(up)(n_leg1.wait_send)
    pl.when(down)(s_leg1.wait_send)
    pl.when(last_row)(n_leg2.wait_send)
    pl.when(first_row)(s_leg2.wait_send)


def finish_kernel(n_row, n_sub, w_ref,
                  us, vs, tn, sn, wide, abuf, lu, lv, hu_s, hv_s, mu_s, mv_s,
                  eta_o, tu_o, tv_o, u_o, v_o, t_o, s_o,
                  bu, bv, cfu, cfv, mku, mkv, tu, tv, xs, acu, acv, cu, cv, flat_b, ubuf, vbuf, sem):
    row = lax.axis_index('row')
    dtb = TIME_STEP / n_sub
    total_rows = float(n_row * NR)
    zero8 = jnp.zeros((SUB, LANE), F32)
    west_of, east_of = movers()
    copies = []

    def put(src, dst):
        cp = pltpu.make_async_copy(src, dst, sem.at[len(copies)])
        cp.start()
        copies.append(cp)

    for src, dst in ((tn, t_o), (sn, s_o)):
        for t in range(NT):
            put(src.at[t], dst.at[:, :, pl.ds(LANE * t, LANE)])

    def setup(i, _):
        base = SUB + SUB * i
        rows = pl.ds(base, SUB)
        rown = pl.ds(base + 1, SUB)
        first = row * NR + SUB * i - NR
        fu, fv = corio(first, total_rows)
        place = first + lax.broadcasted_iota(jnp.int32, (SUB, LANE), 0)
        inside = place >= 0
        wet_u = jnp.logical_and(inside, place < n_row * NR).astype(F32)
        wet_v = jnp.logical_and(inside, place < n_row * NR - 1).astype(F32)
        cfu[rows, :] = wet_u * ((0.25 * dtb) * fu)
        cfv[rows, :] = wet_v * ((0.25 * dtb) * fv)
        mku[rows, :] = wet_u
        mkv[rows, :] = wet_v
        for t in range(5):
            right = (t + 1) % 5
            d0 = wide[3, t, rows, :]
            scale = 0.5 * dtb * dtb * GRAVITY
            bu[t, rows, :] = wet_u * (scale * (d0 + east_of(d0, wide[3, right, rows, :])))
            bv[t, rows, :] = wet_v * (scale * (d0 + wide[3, t, rown, :]))
            tu[0, t, rows, :] = dtb * wide[2, t, rows, :]
            tv[0, t, rows, :] = dtb * wide[1, t, rows, :]
        return 0

    for i in range(12):
        rows = pl.ds(SUB + SUB * i, SUB)
        for f in range(2):
            wide[f + 2, 4, rows, :] = pltpu.roll(wide[f, 4, rows, :], LANE // 2, 1)
        abuf[1, 4, rows, :] = pltpu.roll(abuf[0, 4, rows, :], LANE // 2, 1)
    lax.fori_loop(0, 12, setup, 0)
    for t in range(NT):
        acu[t] = jnp.zeros((NR, LANE), F32)
        acv[t] = jnp.zeros((NR, LANE), F32)

    def subcycle(n, cur, lo, hi, first=False):
        nxt = 1 - cur
        weight = w_ref[n] * (ONE / dtb)
        def eta_part(i):
            rows, rows_s = pl.ds(SUB + SUB * i, SUB), pl.ds(7 + SUB * i, SUB)
            u0 = [tu[cur, t, rows, :] for t in range(5)]
            v0 = [tv[cur, t, rows, :] for t in range(5)]
            vs = [tv[cur, t, rows_s, :] for t in range(5)]
            uw = [west_of(u0[t], u0[(t + 4) % 5]) for t in range(5)]
            u2 = [u0[t] + uw[t] for t in range(5)]
            es = [wide[0, t, rows, :] - ((u0[t] - uw[t]) + (v0[t] - vs[t])) for t in range(5)]
            for t in range(5):
                wide[0, t, rows, :] = es[t]
                xs[t, rows, :] = u2[t]

        def flow_part(i):
            rows, rows_n = pl.ds(SUB + SUB * i, SUB), pl.ds(9 + SUB * i, SUB)
            f_u, f_v = cfu[rows, :], cfv[rows, :]
            rows_s = pl.ds(7 + SUB * i, SUB)
            v0 = [tv[cur, t, rows, :] for t in range(5)]
            v2 = [v0[t] + tv[cur, t, rows_s, :] for t in range(5)]
            v4 = [v2[t] + east_of(v2[t], v2[(t + 1) % 5]) for t in range(5)]
            es = [wide[0, t, rows, :] for t in range(5)]
            for t in range(5):
                slope_u = east_of(es[t], es[(t + 1) % 5]) - es[t]
                slope_v = wide[0, t, rows_n, :] - es[t]
                u4 = xs[t, rows, :] + xs[t, rows_n, :]
                u_old, v_old = tu[cur, t, rows, :], tv[cur, t, rows, :]
                if first:
                    u_old = mku[rows, :] * u_old
                    v_old = mkv[rows, :] * v_old
                u_new = (u_old + abuf[0, t, rows, :]) + (f_u * v4[t] - bu[t, rows, :] * slope_u)
                v_new = (v_old + abuf[1, t, rows, :]) - (f_v * u4 + bv[t, rows, :] * slope_v)
                tu[nxt, t, rows, :] = u_new
                tv[nxt, t, rows, :] = v_new
                if 4 <= i < SUB and t < NT:
                    ro = pl.ds(SUB * (i - 4), SUB)
                    acu[t, ro, :] += weight * u_new
                    acv[t, ro, :] += weight * v_new

        for part in (eta_part, flow_part):
            for i in reversed(range(lo, hi)):
                part(i)

    def pairs(first_n, count, lo, hi):
        def body(i, _):
            n = first_n + 2 * i
            subcycle(n, 0, lo, hi)
            subcycle(n + 1, 1, lo, hi)
            return 0
        lax.fori_loop(0, count, body, 0)

    subcycle(0, 0, 0, 12, first=True)
    subcycle(1, 1, 0, 12)
    pairs(2, 2, 0, 12)
    pairs(6, 4, 1, 11)
    pairs(14, 4, 2, 10)
    pairs(22, 4, 3, 9)

    for t in range(NT):
        for j in range(4):
            rw = pl.ds(WO + SUB * j, SUB)
            ro = pl.ds(SUB * j, SUB)
            flat_b[0, t, ro, :] = wide[0, t, rw, :]
            flat_b[1, t, ro, :] = (ONE / dtb) * tu[0, t, rw, :]
            flat_b[2, t, ro, :] = (ONE / dtb) * tv[0, t, rw, :]
            cu[t, ro, :] = acu[t, ro, :] / hu_s[t, ro, :] - mu_s[t, ro, :]
            hv = hv_s[t, ro, :]
            cv[t, ro, :] = acv[t, ro, :] / hv - mv_s[t, ro, :]

    for f, dst in enumerate((eta_o, tu_o, tv_o)):
        for t in range(NT):
            put(flat_b.at[f, t], dst.at[:, pl.ds(LANE * t, LANE)])
    for lev, cor, src, buf, dst in ((lu, cu, us, ubuf, u_o), (lv, cv, vs, vbuf, v_o)):
        for t in range(NT):
            for j in range(4):
                ro = pl.ds(SUB * j, SUB)
                count = lev[t, ro, :]
                shift = cor[t, ro, :]
                for k in range(NL):
                    buf[t, k, ro, :] = jnp.where(count > k, src[t, k, ro, :] + shift, ZERO)
            put(buf.at[t], dst.at[:, :, pl.ds(LANE * t, LANE)])
    for cp in copies:
        cp.wait()


def solution(mesh):
    n_row = mesh.shape['row']

    def step(vel_u, vel_v, temperature, salinity, surf_eta, trans_u, trans_v, bottom_depth, level_count, avg_weights):
        n_sub = avg_weights.shape[0]
        hbm = pl.BlockSpec(memory_space=pltpu.HBM)
        vmem = pl.BlockSpec(memory_space=pltpu.VMEM)
        smem = pl.BlockSpec(memory_space=pltpu.SMEM)
        cube_v = pltpu.VMEM((NT, NL, NR, LANE), F32)
        flat_v = pltpu.VMEM((NT, NR, LANE), F32)
        wide1 = pltpu.VMEM((5, WR, LANE), F32)
        wide_v = pltpu.VMEM((4, 5, WR, LANE), F32)
        force_v = pltpu.VMEM((2, 5, WR, LANE), F32)
        sems = pltpu.SemaphoreType.DMA
        outs = [cube_v] * 4 + [wide_v, force_v] + [flat_v] * 6
        mids = pl.pallas_call(
            functools.partial(ocean_kernel, n_row, n_sub),
            out_shape=outs,
            in_specs=[hbm] * 9,
            out_specs=[vmem] * len(outs),
            scratch_shapes=[
                pltpu.VMEM((4, 5, NL, RO + NR + SUB, LANE), F32),
                pltpu.VMEM((5, NL, RO + NR + SUB, LANE), F32),
                pltpu.VMEM((NT, NL, RO + NR + SUB, LANE), F32),
                pltpu.VMEM((NT, NL, RO + NR + SUB, LANE), F32),
                pltpu.VMEM((2, 5, RO + NR + SUB, LANE), F32),
                pltpu.VMEM((4, NT, NH, LANE), F32),
                pltpu.VMEM((4, NR, LANE), F32),
                pltpu.VMEM((NT, NR, LANE), jnp.int32),
                pltpu.VMEM((4, 2, SUB, LANE), F32),
                pltpu.VMEM((4, 2, SUB, LANE), F32),
                pltpu.VMEM((NR, LANE), F32),
                sems((16,)), sems((24,)), sems((N_COPY,)), sems((N_COPY,)),
            ],
            compiler_params=pltpu.CompilerParams(collective_id=0, has_side_effects=True, vmem_limit_bytes=VMEM_MAIN),
            name='ocean',
        )(*[pltpu.with_memory_space_constraint(x, pltpu.HBM) for x in (vel_u, vel_v, temperature, salinity, surf_eta, trans_u, trans_v, bottom_depth, level_count)])
        cube = jax.ShapeDtypeStruct((NL, NR, NT * LANE), F32)
        flat = jax.ShapeDtypeStruct((NR, NT * LANE), F32)
        return pl.pallas_call(
            functools.partial(finish_kernel, n_row, n_sub),
            out_shape=[flat] * 3 + [cube] * 4,
            in_specs=[smem] + [vmem] * len(outs),
            out_specs=[hbm] * 7,
            scratch_shapes=[wide1] * 2 + [pltpu.VMEM((WR, LANE), F32)] * 4 + [force_v, force_v, wide1] + [flat_v] * 4 + [pltpu.VMEM((3, NT, NR, LANE), F32), cube_v, cube_v, sems((28,))],
            compiler_params=pltpu.CompilerParams(vmem_limit_bytes=VMEM_FINISH),
            name='finish',
        )(avg_weights, *mids)

    cube = P(None, 'row', 'col')
    flat = P('row', 'col')
    return jax.shard_map(step, mesh=mesh, in_specs=(cube, cube, cube, cube, flat, flat, flat, flat, flat, P()), out_specs=(flat, flat, flat, cube, cube, cube, cube), check_vma=False)
```

```python
import functools

import jax
import jax.numpy as jnp
from jax import lax
from jax.experimental import pallas as pl
from jax.experimental.pallas import tpu as pltpu
from jax.sharding import PartitionSpec as P

TIME_STEP = 1.0
GRAVITY = 16.0
BC_GRAVITY = 4.0
EXPAND_T = 0.2
CONTRACT_S = 0.6
CORIO_F0 = 0.4
CORIO_BETA = 0.4
VISC_R = 2.0
DIFF_R = 0.5

MESH = pl.DeviceIdType.MESH
F32 = jnp.float32

SUB = 8
LANE = 128
ZERO = 0.0
ONE = 1.0
NL = 31
NR = 32
NT = 4
RO = 8
WO = 40
WR = 112
N_COPY = 40
LATE = 2
T_TILES = 4
NH = 30
VMEM_MAIN = 40 * 1024 * 1024
VMEM_FINISH = 12 * 1024 * 1024


def factors(strength):
    inner, last = [], []
    before = ZERO
    for level in range(NL):
        low = ZERO if level == 0 else strength
        inner.append(strength / (ONE + low + strength - low * before))
        last.append(strength / (ONE + low - low * before))
        before = inner[-1]
    return inner, last


VISC_IN, VISC_END = factors(VISC_R)
DIFF_IN, DIFF_END = factors(DIFF_R)


def lanes():
    return lax.broadcasted_iota(jnp.int32, (SUB, LANE), 1)


def movers(height=SUB):
    here = lax.broadcasted_iota(jnp.int32, (height, LANE), 1)
    first, last = here == 0, here == LANE - 1

    def west_of(own, left):
        return pltpu.roll(lax.select(last, left, own), 1, 1)

    def east_of(own, right):
        return pltpu.roll(lax.select(first, right, own), LANE - 1, 1)

    return west_of, east_of


def corio(first, total_rows, height=SUB):
    pos = (first + lax.broadcasted_iota(jnp.int32, (height, LANE), 0)).astype(F32)
    fu = CORIO_F0 + CORIO_BETA * ((pos + 0.5) / total_rows - 0.5)
    fv = CORIO_F0 + CORIO_BETA * ((pos + ONE) / total_rows - 0.5)
    return fu, fv


def ocean_kernel(n_row, n_sub,
                 u_in, v_in, t_in, s_in, eta_in, tu_in, tv_in, dep_in, cnt_in,
                 us_o, vs_o, tn_o, sn_o, wide, abuf, lu_o, lv_o, hu_s, hv_s, mu_s, mv_s,
                 fb, pb, uw_b, ve_b, near, relay, wsend, cnt_i, pk_s, pk_r, asend,
                 in_sem, w_sem, send, recv):
    row = lax.axis_index('row')
    col = lax.axis_index('col')
    ocol = 1 - col
    has_s = row > 0
    has_n = row < n_row - 1
    dtb = TIME_STEP / n_sub
    total_rows = float(n_row * NR)
    used = []
    ub, vb, tb, sb = (fb.at[f] for f in range(4))
    zero8 = jnp.zeros((SUB, LANE), F32)
    west_of, east_of = movers()
    west_all, east_all = movers(NR)
    all_rows = pl.ds(RO, NR)
    cnt, depth = near.at[0], near.at[1]
    half_row = n_row // 2
    up, down = row == half_row - 1, row == half_row
    first_row, last_row = row == 0, row == n_row - 1

    def dev(step, c):
        return {'row': row + step, 'col': c}

    def remote(src, dst, device):
        used.append(0)
        idx = len(used) - 1
        return pltpu.make_async_remote_copy(src, dst, send.at[idx], recv.at[idx], device_id=device, device_id_type=MESH)

    def start(copies):
        for cp in copies:
            cp.start()

    def both(south, north, action):
        @pl.when(has_s)
        def _():
            for cp in south:
                action(cp)

        @pl.when(has_n)
        def _():
            for cp in north:
                action(cp)

    def arrived(south_from, north_from):
        both(south_from, north_from, lambda cp: cp.wait_recv())

    wloads, loads = {}, {}
    for f, src in enumerate((eta_in, tv_in, tu_in, dep_in, cnt_in)):
        for t in range(NT):
            dst = wide.at[f, t, pl.ds(WO, NR), :] if f < 4 else cnt_i.at[t]
            wloads[f, t] = pltpu.make_async_copy(src.at[:, pl.ds(LANE * t, LANE)], dst, w_sem.at[f * NT + t])
    for f, src in enumerate((u_in, v_in, t_in, s_in)):
        for t in range(NT):
            loads[f, t] = pltpu.make_async_copy(src.at[:, :, pl.ds(LANE * t, LANE)], fb.at[f, t, :, pl.ds(RO, NR), :], in_sem.at[f * NT + t])
    for t in range(NT):
        wloads[5, t] = pltpu.make_async_copy(dep_in.at[:, pl.ds(LANE * t, LANE)], near.at[1, t, pl.ds(RO, NR), :], w_sem.at[5 * NT + t])
    start(wloads.values())
    order = [(f, t) for g in (0, 2) for tiles in ((0, 3), (1, 2)) for f in (g, g + 1) for t in tiles]
    start([loads[key] for key in order])

    for i in range(5):
        for rr in (0, SUB, WR - 2 * SUB, WR - SUB):
            for f in range(4):
                wide[f, i, pl.ds(rr, SUB), :] = zero8
            for f in range(2):
                abuf[f, i, pl.ds(rr, SUB), :] = zero8

    barrier = pltpu.get_barrier_semaphore()
    pl.semaphore_signal(barrier, inc=1, device_id=dev(0, ocol), device_id_type=MESH)

    @pl.when(has_n)
    def _():
        for c in (col, ocol):
            pl.semaphore_signal(barrier, inc=1, device_id=dev(1, c), device_id_type=MESH)

    @pl.when(has_s)
    def _():
        for c in (col, ocol):
            pl.semaphore_signal(barrier, inc=1, device_id=dev(-1, c), device_id_type=MESH)

    def greet(rows_of):
        for d in rows_of:
            pl.semaphore_signal(barrier, inc=1, device_id=dev(d, col), device_id_type=MESH)

    pl.when(up)(lambda: greet((half_row, 1 - half_row)))
    pl.when(down)(lambda: greet((half_row - 1, -half_row)))
    pl.when(first_row)(lambda: greet((half_row - 1, half_row)))
    pl.when(last_row)(lambda: greet((-half_row, 1 - half_row)))

    def fill(first3, first2):
        def body(i, _):
            for f in range(4):
                fb[f, i, :, pl.ds(first3, SUB), :] = jnp.zeros((NL, SUB, LANE), F32)
            return 0
        lax.fori_loop(0, 5, body, 0)
        for i in range(5):
            for f in range(4):
                wide[f, i, pl.ds(first2, NR), :] = jnp.zeros((NR, LANE), F32)
            for f in range(2):
                abuf[f, i, pl.ds(first2, NR), :] = jnp.zeros((NR, LANE), F32)
            for f in range(2):
                near[f, i, pl.ds(first3, SUB), :] = zero8

    @pl.when(jnp.logical_not(has_s))
    def _():
        fill(0, WO - NR)

    @pl.when(jnp.logical_not(has_n))
    def _():
        fill(RO + NR, WO + NR)

    for cp in wloads.values():
        cp.wait()
    for t in range(NT):
        cnt[t, pl.ds(RO, NR), :] = cnt_i[t].astype(F32)
    lane = lanes()
    outer = lane < LANE // 2
    middle = jnp.logical_and(lane >= NR, lane < LANE - NR)

    def edges(buf, f, first):
        rows = pl.ds(first, SUB)
        return jnp.where(outer, buf[f, 0, rows, :], buf[f, 3, rows, :])

    def paired(buf, f, g, first):
        return jnp.where(middle, pltpu.roll(edges(buf, g, first), LANE // 2, 1), edges(buf, f, first))

    for j in range(4):
        mine = pl.ds(SUB * j, SUB)
        first = WO + SUB * j
        for f in range(2):
            wsend[f, mine, :] = paired(wide, f, f + 2, first)
        own = pl.ds(RO + SUB * j, SUB)
        for f in range(2):
            wsend[2 + f, mine, :] = jnp.where(outer, near[f, 0, own, :], near[f, 3, own, :])

    round_about = jnp.logical_or(jnp.logical_or(up, down), jnp.logical_or(first_row, last_row))
    barrier_count = 1 + 2 * has_n.astype(jnp.int32) + 2 * has_s.astype(jnp.int32) + 2 * round_about.astype(jnp.int32)
    pl.semaphore_wait(barrier, barrier_count)

    own4 = pl.ds(0, NT)
    two = pl.ds(0, 2)
    top, low, north, south = RO + NR - 1, RO, RO + NR, RO - 1
    n_src, n_dst, s_src, s_dst = WO + NR - NH, WO - NH, WO, WO + NR

    def rows3(f, a, b, d):
        return remote(fb.at[f, own4, :, pl.ds(a, 1), :], fb.at[f, own4, :, pl.ds(b, 1), :], dev(d, col))

    def rows2(buf, f, nf, a, b, d):
        return remote(buf.at[pl.ds(f, nf), own4, pl.ds(a, NH), :], buf.at[pl.ds(f, nf), own4, pl.ds(b, NH), :], dev(d, col))

    def row1(a, b, d):
        return remote(near.at[:, own4, pl.ds(a, 1), :], near.at[:, own4, pl.ds(b, 1), :], dev(d, col))

    def corner(a, b, d):
        return remote(wsend.at[two, pl.ds(a - WO, NH), :], wide.at[two, 4, pl.ds(b, NH), :], dev(d, ocol))

    z_wide = [
        remote(wsend.at[pl.ds(2, 2)], near.at[:, 4, pl.ds(RO, NR), :], dev(0, ocol)),
        remote(wsend.at[two], wide.at[two, 4, pl.ds(WO, NR), :], dev(0, ocol)),
    ]
    n_first = [row1(top, south, 1)]
    s_first = [row1(low, north, -1)]

    def via(src_row, dst_row, there, onward):
        leg1 = remote(wide.at[:, own4, pl.ds(src_row, NH), :], relay, dev(there, col))
        leg2 = remote(relay, wide.at[:, own4, pl.ds(dst_row, NH), :], dev(onward, col))
        return leg1, leg2

    n_leg1, n_leg2 = via(n_src, n_dst, half_row, 1 - half_row)
    s_leg1, s_leg2 = via(s_src, s_dst, -half_row, half_row - 1)
    pl.when(up)(n_leg1.start)
    pl.when(down)(s_leg1.start)
    start(z_wide)
    both(s_first, n_first, lambda cp: cp.start())

    def slot(k, j):
        return (4 * k + j) // 64, 2 * ((4 * k + j) % 64)

    def pack(half_of, _):
        here = lanes()
        first = lax.broadcasted_iota(jnp.int32, (NR, LANE), 1) == 0
        acc = {}
        for k in range(NL):
            for f in range(2):
                field = 2 * half_of + f
                both_edges = lax.select(first, fb[field, 0, k, all_rows, :], fb[field, 3, k, all_rows, :])
                for j in range(4):
                    word, at = slot(k, j)
                    pair = both_edges[SUB * j:SUB * (j + 1)]
                    if at:
                        mine = jnp.logical_or(here == at, here == at - 1)
                        acc[f, word] = lax.select(mine, pltpu.roll(pair, at, 1), acc[f, word])
                    else:
                        acc[f, word] = pair
        for f, word in acc:
            pk_s[2 * half_of + f, word] = acc[f, word]
        return 0

    def unpack(half_of, _):
        for f in range(2):
            field = 2 * half_of + f
            got = [pk_r[field, word] for word in range(2)]
            for k in range(NL):
                parts = []
                for j in range(4):
                    word, at = slot(k, j)
                    parts.append(pltpu.roll(got[word], LANE - at, 1) if at else got[word])
                fb[field, 4, k, all_rows, :] = jnp.concatenate(parts, axis=0)
        return 0

    def shift_u(t):
        for k in range(NL):
            uw_b[t, k, all_rows, :] = west_all(ub[t, k, all_rows, :], ub[lax.rem(t + 4, 5), k, all_rows, :])

    def shift_v(t):
        for k in range(NL):
            ve_b[t, k, all_rows, :] = east_all(vb[t, k, all_rows, :], vb[t + 1, k, all_rows, :])

    for t in (0, 3, 1, 2):
        for f in (0, 1):
            loads[f, t].wait()
    n_vel = [rows3(0, top, south, 1), rows3(1, top, south, 1),
             remote(fb.at[1, 0, :, pl.ds(top, 1), :], fb.at[1, 4, :, pl.ds(south, 1), :], dev(1, ocol))]
    s_vel = [rows3(0, low, north, -1), rows3(1, low, north, -1),
             remote(fb.at[0, 3, :, pl.ds(low, 1), :], fb.at[0, 4, :, pl.ds(north, 1), :], dev(-1, ocol))]
    both(s_vel, n_vel, lambda cp: cp.start())

    def shift_own(t, _):
        shift_u(t + 1)
        shift_v(t)
        return 0
    lax.fori_loop(0, 3, shift_own, 0)

    for t in (0, 3, 1, 2):
        for f in (2, 3):
            loads[f, t].wait()
    n_tra = [rows3(2, top, south, 1), rows3(3, top, south, 1)]
    s_tra = [rows3(2, low, north, -1), rows3(3, low, north, -1)]
    n_far, s_far = rows2(wide, 0, 4, n_src, n_dst, 1), rows2(wide, 0, 4, s_src, s_dst, -1)
    n_cor, s_cor = corner(n_src, n_dst, 1), corner(s_src, s_dst, -1)
    both(s_tra, [], lambda cp: cp.start())
    far_n, far_s = jnp.logical_and(has_n, jnp.logical_not(up)), jnp.logical_and(has_s, jnp.logical_not(down))
    lax.fori_loop(0, 2, pack, 0)
    z_col = remote(pk_s, pk_r, dev(0, ocol))
    z_col.start()

    p_unit = 0.5 * BC_GRAVITY / NL

    def pressure(t, rows, height):
        total = jnp.zeros((height, LANE), F32)
        for k in range(NL):
            part = (p_unit * CONTRACT_S) * sb[t, k, rows, :] - (p_unit * EXPAND_T) * tb[t, k, rows, :]
            here = total + part
            pb[t, k, rows, :] = here
            total = here + part

    def pressure_own(t, _):
        pressure(t, all_rows, NR)
        return 0
    lax.fori_loop(0, NT, pressure_own, 0)

    def chooser(height):
        nothing = jnp.zeros((height, LANE), F32)

        def pick(mask, inner, last):
            return lax.select(mask, jnp.full((height, LANE), inner, F32), jnp.full((height, LANE), last, F32))

        def keep(mask, value):
            return lax.select(mask, value, nothing)

        return nothing, pick, keep

    def momentum(lt, j, height=SUB, at_south=False, at_north=False):
        west_of, east_of = movers(height)
        zero8, pick, keep = chooser(height)

        def near2d(buf):
            c = buf[lt, rc, :]
            return c, east_of(c, buf[lt + 1, rc, :]), buf[lt, rn, :]

        rc, rn, rs = pl.ds(RO + SUB * j, height), pl.ds(RO + 1 + SUB * j, height), pl.ds(RO - 1 + SUB * j, height)
        ro = pl.ds(SUB * j, height)
        t, right, left = lt, lax.rem(lt + 1, 5), lax.rem(lt + 4, 5)
        fu, fv = corio(row * NR + SUB * j, total_rows, height)
        fu4 = 0.25 * fu
        fv4 = 0.25 * fv
        c0, ce, cn = near2d(cnt)
        lu = jnp.minimum(c0, ce)
        lv = jnp.minimum(c0, cn)
        d0, de, dn = near2d(depth)
        hu = 0.5 * (d0 + de)
        hv = 0.5 * (d0 + dn)
        lu_o[lt, ro, :] = lu
        lv_o[lt, ro, :] = lv
        hu_s[lt, ro, :] = hu
        hv_s[lt, ro, :] = hv
        yu, yv = zero8, zero8
        su, sv = zero8, zero8
        for k in range(NL):
            u = ub[t, k, rc, :]
            v = vb[t, k, rc, :]
            uw = uw_b[t, k, rc, :]
            ue = east_of(u, ub[right, k, rc, :])
            un = ub[t, k, rn, :]
            us = ub[t, k, rs, :]
            unw = west_of(un, ub[left, k, rn, :]) if at_north else uw_b[t, k, rn, :]
            vw = west_of(v, vb[left, k, rc, :])
            ve = ve_b[t, k, rc, :]
            vn = vb[t, k, rn, :]
            vs = vb[t, k, rs, :]
            vse = east_of(vs, vb[right, k, rs, :]) if at_south else ve_b[t, k, rs, :]
            v4 = (v + ve) + (vs + vse)
            u4 = (u + uw) + (un + unw)
            p = pb[t, k, rc, :]
            pe = east_of(p, pb[right, k, rc, :])
            pn = pb[t, k, rn, :]
            ustar = u + (v4 * (fu4 - 0.125 * (un - us)) - 0.5 * u * (ue - uw) - (pe - p))
            vstar = v - (u4 * (fv4 + 0.125 * (ve - vw)) + 0.5 * v * (vn - vs) + (pn - p))
            yu = (ustar + yu) * (pick(lu > k + 1, VISC_IN[k], VISC_END[k]) if k < NL - 1 else VISC_END[k])
            yv = (vstar + yv) * (pick(lv > k + 1, VISC_IN[k], VISC_END[k]) if k < NL - 1 else VISC_END[k])
            if k < NL - 1:
                us_o[lt, k, ro, :] = yu
                vs_o[lt, k, ro, :] = yv
            su = su + keep(lu > k, u)
            sv = sv + keep(lv > k, v)
        mu, mv = zero8, zero8
        xu, xv = zero8, zero8
        for k in reversed(range(NL)):
            xu = yu if k == NL - 1 else us_o[lt, k, ro, :] + (keep(lu > k + 1, VISC_IN[k] * xu))
            xv = yv if k == NL - 1 else vs_o[lt, k, ro, :] + (keep(lv > k + 1, VISC_IN[k] * xv))
            us_o[lt, k, ro, :] = xu
            vs_o[lt, k, ro, :] = xv
            mu = mu + keep(lu > k, xu)
            mv = mv + keep(lv > k, xv)
        mu, mv = (ONE / VISC_R) * mu, (ONE / VISC_R) * mv
        iu = ONE / jnp.maximum(lu, ONE)
        iv = ONE / jnp.maximum(lv, ONE)
        mu_s[lt, ro, :] = mu * iu
        mv_s[lt, ro, :] = mv * iv
        scale = dtb * dtb / TIME_STEP
        rw = pl.ds(WO + SUB * j, height)
        abuf[0, lt, rw, :] = jnp.where(lu > ZERO, scale * hu * ((mu - su) * iu), ZERO)
        abuf[1, lt, rw, :] = jnp.where(lv > ZERO, scale * hv * ((mv - sv) * iv), ZERO)

    def middle_rows(i, _):
        odd, later = lax.rem(i, 2), i // 2

        @pl.when(jnp.logical_and(i == 3, last_row))
        def _():
            n_leg1.wait_recv()
            n_leg2.start()

        @pl.when(jnp.logical_and(i == 3, first_row))
        def _():
            s_leg1.wait_recv()
            s_leg2.start()

        @pl.when(i == LATE)
        def _():
            both([], n_tra, lambda cp: cp.start())
            pl.when(far_n)(n_far.start)
            pl.when(far_s)(s_far.start)
            both([s_cor], [n_cor], lambda cp: cp.start())

        @pl.when(i == 2)
        def _():
            for cp in (z_wide[0], z_col):
                cp.wait_recv()
            lax.fori_loop(0, 2, unpack, 0)
            shift_u(0)
            shift_v(3)
            pressure(4, all_rows, NR)

        momentum(1 + odd + later * (2 * odd - 1), 1, 2 * SUB)
        return 0

    lax.fori_loop(0, NT, middle_rows, 0)

    arrived(n_first + n_vel, s_first + s_vel + s_tra)

    def pressure_north(i, _):
        for odd in range(2):
            pressure(2 * i + odd, pl.ds(RO + NR, SUB), SUB)
        return 0
    lax.fori_loop(0, 2, pressure_north, 0)

    def force_corner(a, b, d):
        return remote(asend.at[pl.ds(a - WO, NH), :], abuf.at[0, 4, pl.ds(b, NH), :], dev(d, ocol))

    def force_rows(t, a, b, d):
        return remote(abuf.at[:, t, pl.ds(a, NH), :], abuf.at[:, t, pl.ds(b, NH), :], dev(d, col))

    def force_pair(t):
        return force_rows(t, n_src, n_dst, 1), force_rows(t, s_src, s_dst, -1)

    z_force = remote(asend, abuf.at[0, 4, pl.ds(WO, NR), :], dev(0, ocol))
    n_fcor, s_fcor = force_corner(n_src, n_dst, 1), force_corner(s_src, s_dst, -1)

    force = [force_pair(t) for t in range(NT)]
    n_force = [p[0] for p in force] + [n_fcor]
    s_force = [p[1] for p in force] + [s_fcor]

    def send_force(which):
        both([s_force[i] for i in which], [n_force[i] for i in which], lambda cp: cp.start())

    def ends(i, _):
        t = lax.rem(3 * i, 4)
        momentum(t, 0, at_south=True)
        momentum(t, 3, at_north=True)

        @pl.when(i == 1)
        def _():
            for j in range(4):
                asend[pl.ds(SUB * j, SUB), :] = paired(abuf, 0, 1, WO + SUB * j)
            z_force.start()
            send_force((0, 3, 4))

        @pl.when(i == 2)
        def _():
            send_force((2,))
        return 0

    lax.fori_loop(0, NT, ends, 0)
    send_force((1,))

    arrived(n_tra, [])

    def tracers(lt, j, height):
        west_of, east_of = movers(height)
        zero8, pick, keep = chooser(height)
        rc, rn, rs = pl.ds(RO + SUB * j, height), pl.ds(RO + 1 + SUB * j, height), pl.ds(RO - 1 + SUB * j, height)
        ro = pl.ds(SUB * j, height)
        t, right, left = lt, lax.rem(lt + 1, 5), lax.rem(lt + 4, 5)
        c0 = cnt[lt, rc, :]
        luw = jnp.minimum(c0, west_of(c0, cnt[left, rc, :]))
        lvs = jnp.minimum(c0, cnt[lt, rs, :])
        lu = lu_o[lt, ro, :]
        lv = lv_o[lt, ro, :]
        yt, ys = zero8, zero8
        for k in range(NL):
            here = c0 > k
            me = keep(lu > k, ub[t, k, rc, :])
            mw = keep(luw > k, uw_b[t, k, rc, :])
            mn = keep(lv > k, vb[t, k, rc, :])
            ms = keep(lvs > k, vb[t, k, rs, :])
            own = 2.0 - ((me - mw) + (mn - ms))

            def advect(buf):
                q = buf[t, k, rc, :]
                qe = east_of(q, buf[right, k, rc, :])
                qw = west_of(q, buf[left, k, rc, :])
                return (own * q + (mw * qw - me * qe)) + (ms * buf[t, k, rs, :] - mn * buf[t, k, rn, :])

            end = pick(here, DIFF_END[k], 0.5)
            fac = lax.select(c0 > k + 1, jnp.full_like(end, DIFF_IN[k]), end) if k < NL - 1 else end
            yt = (advect(tb) + keep(here, yt)) * fac
            ys = (advect(sb) + keep(here, ys)) * fac
            if k < NL - 1:
                tn_o[lt, k, ro, :] = yt
                sn_o[lt, k, ro, :] = ys
        xt, xs_ = zero8, zero8
        for k in reversed(range(NL)):
            xt = yt if k == NL - 1 else tn_o[lt, k, ro, :] + keep(c0 > k + 1, DIFF_IN[k] * xt)
            xs_ = ys if k == NL - 1 else sn_o[lt, k, ro, :] + keep(c0 > k + 1, DIFF_IN[k] * xs_)
            tn_o[lt, k, ro, :] = xt
            sn_o[lt, k, ro, :] = xs_

    def tracers_all(i, _):
        tracers(lax.rem(i, NT), T_TILES * (i // NT), T_TILES * SUB)
        return 0
    lax.fori_loop(0, 16 // T_TILES, tracers_all, 0)

    z_wide[1].wait_recv()
    z_force.wait_recv()
    pl.when(far_s)(n_far.wait_recv)
    pl.when(far_n)(s_far.wait_recv)
    pl.when(down)(n_leg2.wait_recv)
    pl.when(up)(s_leg2.wait_recv)
    arrived([n_cor] + n_force, [s_cor] + s_force)

    for cp in z_wide + [z_col, z_force]:
        cp.wait_send()
    both(s_first + s_vel + s_tra + [s_cor] + s_force, n_first + n_vel + n_tra + [n_cor] + n_force, lambda cp: cp.wait_send())
    pl.when(far_n)(n_far.wait_send)
    pl.when(far_s)(s_far.wait_send)
    pl.when(up)(n_leg1.wait_send)
    pl.when(down)(s_leg1.wait_send)
    pl.when(last_row)(n_leg2.wait_send)
    pl.when(first_row)(s_leg2.wait_send)


def finish_kernel(n_row, n_sub, w_ref,
                  us, vs, tn, sn, wide, abuf, lu, lv, hu_s, hv_s, mu_s, mv_s,
                  eta_o, tu_o, tv_o, u_o, v_o, t_o, s_o,
                  bu, bv, cfu, cfv, mku, mkv, tu, tv, xs, acu, acv, cu, cv, flat_b, ubuf, vbuf, sem):
    row = lax.axis_index('row')
    dtb = TIME_STEP / n_sub
    total_rows = float(n_row * NR)
    zero8 = jnp.zeros((SUB, LANE), F32)
    west_of, east_of = movers()
    copies = []

    def put(src, dst):
        cp = pltpu.make_async_copy(src, dst, sem.at[len(copies)])
        cp.start()
        copies.append(cp)

    for src, dst in ((tn, t_o), (sn, s_o)):
        for t in range(NT):
            put(src.at[t], dst.at[:, :, pl.ds(LANE * t, LANE)])

    def setup(i):
        base = SUB + SUB * i
        rows = pl.ds(base, SUB)
        rown = pl.ds(base + 1, SUB)
        first = row * NR + SUB * i - NR
        fu, fv = corio(first, total_rows)
        place = first + lax.broadcasted_iota(jnp.int32, (SUB, LANE), 0)
        inside = place >= 0
        wet_u = jnp.logical_and(inside, place < n_row * NR).astype(F32)
        wet_v = jnp.logical_and(inside, place < n_row * NR - 1).astype(F32)
        cfu[rows, :] = wet_u * ((0.25 * dtb) * fu)
        cfv[rows, :] = wet_v * ((0.25 * dtb) * fv)
        mku[rows, :] = wet_u
        mkv[rows, :] = wet_v
        for t in range(5):
            right = (t + 1) % 5
            d0 = wide[3, t, rows, :]
            scale = 0.5 * dtb * dtb * GRAVITY
            bu[t, rows, :] = wet_u * (scale * (d0 + east_of(d0, wide[3, right, rows, :])))
            bv[t, rows, :] = wet_v * (scale * (d0 + wide[3, t, rown, :]))
            tu[0, t, rows, :] = dtb * wide[2, t, rows, :]
            tv[0, t, rows, :] = dtb * wide[1, t, rows, :]

    for i in range(12):
        rows = pl.ds(SUB + SUB * i, SUB)
        for f in range(2):
            wide[f + 2, 4, rows, :] = pltpu.roll(wide[f, 4, rows, :], LANE // 2, 1)
        abuf[1, 4, rows, :] = pltpu.roll(abuf[0, 4, rows, :], LANE // 2, 1)
    for i in range(12):
        setup(i)
    for t in range(NT):
        acu[t] = jnp.zeros((NR, LANE), F32)
        acv[t] = jnp.zeros((NR, LANE), F32)

    def subcycle(n, cur, lo, hi, first=False):
        nxt = 1 - cur
        weight = w_ref[n] * (ONE / dtb)
        def eta_part(i):
            rows, rows_s = pl.ds(SUB + SUB * i, SUB), pl.ds(7 + SUB * i, SUB)
            u0 = [tu[cur, t, rows, :] for t in range(5)]
            v0 = [tv[cur, t, rows, :] for t in range(5)]
            vs = [tv[cur, t, rows_s, :] for t in range(5)]
            uw = [west_of(u0[t], u0[(t + 4) % 5]) for t in range(5)]
            u2 = [u0[t] + uw[t] for t in range(5)]
            es = [wide[0, t, rows, :] - ((u0[t] - uw[t]) + (v0[t] - vs[t])) for t in range(5)]
            for t in range(5):
                wide[0, t, rows, :] = es[t]
                xs[t, rows, :] = u2[t]

        def flow_part(i):
            rows, rows_n = pl.ds(SUB + SUB * i, SUB), pl.ds(9 + SUB * i, SUB)
            f_u, f_v = cfu[rows, :], cfv[rows, :]
            rows_s = pl.ds(7 + SUB * i, SUB)
            v0 = [tv[cur, t, rows, :] for t in range(5)]
            v2 = [v0[t] + tv[cur, t, rows_s, :] for t in range(5)]
            v4 = [v2[t] + east_of(v2[t], v2[(t + 1) % 5]) for t in range(5)]
            es = [wide[0, t, rows, :] for t in range(5)]
            for t in range(5):
                slope_u = east_of(es[t], es[(t + 1) % 5]) - es[t]
                slope_v = wide[0, t, rows_n, :] - es[t]
                u4 = xs[t, rows, :] + xs[t, rows_n, :]
                u_old, v_old = tu[cur, t, rows, :], tv[cur, t, rows, :]
                if first:
                    u_old = mku[rows, :] * u_old
                    v_old = mkv[rows, :] * v_old
                u_new = (u_old + abuf[0, t, rows, :]) + (f_u * v4[t] - bu[t, rows, :] * slope_u)
                v_new = (v_old + abuf[1, t, rows, :]) - (f_v * u4 + bv[t, rows, :] * slope_v)
                tu[nxt, t, rows, :] = u_new
                tv[nxt, t, rows, :] = v_new
                if 4 <= i < SUB and t < NT:
                    ro = pl.ds(SUB * (i - 4), SUB)
                    acu[t, ro, :] += weight * u_new
                    acv[t, ro, :] += weight * v_new

        for part in (eta_part, flow_part):
            for i in reversed(range(lo, hi)):
                part(i)

    def pairs(first_n, count, lo, hi):
        def body(i, _):
            n = first_n + 2 * i
            subcycle(n, 0, lo, hi)
            subcycle(n + 1, 1, lo, hi)
            return 0
        lax.fori_loop(0, count, body, 0)

    subcycle(0, 0, 0, 12, first=True)
    subcycle(1, 1, 0, 12)
    pairs(2, 2, 0, 12)
    pairs(6, 4, 1, 11)
    pairs(14, 4, 2, 10)
    pairs(22, 4, 3, 9)

    for t in range(NT):
        for j in range(4):
            rw = pl.ds(WO + SUB * j, SUB)
            ro = pl.ds(SUB * j, SUB)
            flat_b[0, t, ro, :] = wide[0, t, rw, :]
            flat_b[1, t, ro, :] = (ONE / dtb) * tu[0, t, rw, :]
            flat_b[2, t, ro, :] = (ONE / dtb) * tv[0, t, rw, :]
            cu[t, ro, :] = acu[t, ro, :] / hu_s[t, ro, :] - mu_s[t, ro, :]
            hv = hv_s[t, ro, :]
            cv[t, ro, :] = acv[t, ro, :] / hv - mv_s[t, ro, :]

    for f, dst in enumerate((eta_o, tu_o, tv_o)):
        for t in range(NT):
            put(flat_b.at[f, t], dst.at[:, pl.ds(LANE * t, LANE)])
    for lev, cor, src, buf, dst in ((lu, cu, us, ubuf, u_o), (lv, cv, vs, vbuf, v_o)):
        for t in range(NT):
            for j in range(4):
                ro = pl.ds(SUB * j, SUB)
                count = lev[t, ro, :]
                shift = cor[t, ro, :]
                for k in range(NL):
                    buf[t, k, ro, :] = jnp.where(count > k, (ONE / VISC_R) * src[t, k, ro, :] + shift, ZERO)
            put(buf.at[t], dst.at[:, :, pl.ds(LANE * t, LANE)])
    for cp in copies:
        cp.wait()


def solution(mesh):
    n_row = mesh.shape['row']

    def step(vel_u, vel_v, temperature, salinity, surf_eta, trans_u, trans_v, bottom_depth, level_count, avg_weights):
        n_sub = avg_weights.shape[0]
        hbm = pl.BlockSpec(memory_space=pltpu.HBM)
        vmem = pl.BlockSpec(memory_space=pltpu.VMEM)
        smem = pl.BlockSpec(memory_space=pltpu.SMEM)
        cube_v = pltpu.VMEM((NT, NL, NR, LANE), F32)
        flat_v = pltpu.VMEM((NT, NR, LANE), F32)
        wide1 = pltpu.VMEM((5, WR, LANE), F32)
        wide_v = pltpu.VMEM((4, 5, WR, LANE), F32)
        force_v = pltpu.VMEM((2, 5, WR, LANE), F32)
        sems = pltpu.SemaphoreType.DMA
        outs = [cube_v] * 4 + [wide_v, force_v] + [flat_v] * 6
        mids = pl.pallas_call(
            functools.partial(ocean_kernel, n_row, n_sub),
            out_shape=outs,
            in_specs=[hbm] * 9,
            out_specs=[vmem] * len(outs),
            scratch_shapes=[
                pltpu.VMEM((4, 5, NL, RO + NR + SUB, LANE), F32),
                pltpu.VMEM((5, NL, RO + NR + SUB, LANE), F32),
                pltpu.VMEM((NT, NL, RO + NR + SUB, LANE), F32),
                pltpu.VMEM((NT, NL, RO + NR + SUB, LANE), F32),
                pltpu.VMEM((2, 5, RO + NR + SUB, LANE), F32),
                pltpu.VMEM((4, NT, NH, LANE), F32),
                pltpu.VMEM((4, NR, LANE), F32),
                pltpu.VMEM((NT, NR, LANE), jnp.int32),
                pltpu.VMEM((4, 2, SUB, LANE), F32),
                pltpu.VMEM((4, 2, SUB, LANE), F32),
                pltpu.VMEM((NR, LANE), F32),
                sems((16,)), sems((24,)), sems((N_COPY,)), sems((N_COPY,)),
            ],
            compiler_params=pltpu.CompilerParams(collective_id=0, has_side_effects=True, vmem_limit_bytes=VMEM_MAIN),
            name='ocean',
        )(*[pltpu.with_memory_space_constraint(x, pltpu.HBM) for x in (vel_u, vel_v, temperature, salinity, surf_eta, trans_u, trans_v, bottom_depth, level_count)])
        cube = jax.ShapeDtypeStruct((NL, NR, NT * LANE), F32)
        flat = jax.ShapeDtypeStruct((NR, NT * LANE), F32)
        return pl.pallas_call(
            functools.partial(finish_kernel, n_row, n_sub),
            out_shape=[flat] * 3 + [cube] * 4,
            in_specs=[smem] + [vmem] * len(outs),
            out_specs=[hbm] * 7,
            scratch_shapes=[wide1] * 2 + [pltpu.VMEM((WR, LANE), F32)] * 4 + [force_v, force_v, wide1] + [flat_v] * 4 + [pltpu.VMEM((3, NT, NR, LANE), F32), cube_v, cube_v, sems((28,))],
            compiler_params=pltpu.CompilerParams(vmem_limit_bytes=VMEM_FINISH),
            name='finish',
        )(avg_weights, *mids)

    cube = P(None, 'row', 'col')
    flat = P('row', 'col')
    return jax.shard_map(step, mesh=mesh, in_specs=(cube, cube, cube, cube, flat, flat, flat, flat, flat, P()), out_specs=(flat, flat, flat, cube, cube, cube, cube), check_vma=False)
```

```python
import functools

import jax
import jax.numpy as jnp
from jax import lax
from jax.experimental import pallas as pl
from jax.experimental.pallas import tpu as pltpu
from jax.sharding import PartitionSpec as P

TIME_STEP = 1.0
GRAVITY = 16.0
BC_GRAVITY = 4.0
EXPAND_T = 0.2
CONTRACT_S = 0.6
CORIO_F0 = 0.4
CORIO_BETA = 0.4
VISC_R = 2.0
DIFF_R = 0.5

MESH = pl.DeviceIdType.MESH
F32 = jnp.float32

SUB = 8
LANE = 128
ZERO = 0.0
ONE = 1.0
NL = 31
NR = 32
NT = 4
RO = 8
WO = 40
WR = 112
N_COPY = 40
LATE = 2
T_TILES = 4
NH = 30
VMEM_MAIN = 40 * 1024 * 1024
VMEM_FINISH = 12 * 1024 * 1024


def factors(strength):
    inner, last = [], []
    before = ZERO
    for level in range(NL):
        low = ZERO if level == 0 else strength
        inner.append(strength / (ONE + low + strength - low * before))
        last.append(strength / (ONE + low - low * before))
        before = inner[-1]
    return inner, last


VISC_IN, VISC_END = factors(VISC_R)
DIFF_IN, DIFF_END = factors(DIFF_R)


def lanes():
    return lax.broadcasted_iota(jnp.int32, (SUB, LANE), 1)


def movers(height=SUB):
    here = lax.broadcasted_iota(jnp.int32, (height, LANE), 1)
    first, last = here == 0, here == LANE - 1

    def west_of(own, left):
        return pltpu.roll(lax.select(last, left, own), 1, 1)

    def east_of(own, right):
        return pltpu.roll(lax.select(first, right, own), LANE - 1, 1)

    return west_of, east_of


def corio(first, total_rows, height=SUB):
    pos = (first + lax.broadcasted_iota(jnp.int32, (height, LANE), 0)).astype(F32)
    fu = CORIO_F0 + CORIO_BETA * ((pos + 0.5) / total_rows - 0.5)
    fv = CORIO_F0 + CORIO_BETA * ((pos + ONE) / total_rows - 0.5)
    return fu, fv


def ocean_kernel(n_row, n_sub,
                 u_in, v_in, t_in, s_in, eta_in, tu_in, tv_in, dep_in, cnt_in,
                 us_o, vs_o, tn_o, sn_o, wide, abuf, lu_o, lv_o, hu_s, hv_s, mu_s, mv_s,
                 fb, pb, uw_b, ve_b, near, relay, wsend, cnt_i, pk_s, pk_r, asend,
                 in_sem, w_sem, send, recv):
    row = lax.axis_index('row')
    col = lax.axis_index('col')
    ocol = 1 - col
    has_s = row > 0
    has_n = row < n_row - 1
    dtb = TIME_STEP / n_sub
    total_rows = float(n_row * NR)
    used = []
    ub, vb, tb, sb = (fb.at[f] for f in range(4))
    zero8 = jnp.zeros((SUB, LANE), F32)
    west_of, east_of = movers()
    west_all, east_all = movers(NR)
    all_rows = pl.ds(RO, NR)
    cnt, depth = near.at[0], near.at[1]
    half_row = n_row // 2
    up, down = row == half_row - 1, row == half_row
    first_row, last_row = row == 0, row == n_row - 1

    def dev(step, c):
        return {'row': row + step, 'col': c}

    def remote(src, dst, device):
        used.append(0)
        idx = len(used) - 1
        return pltpu.make_async_remote_copy(src, dst, send.at[idx], recv.at[idx], device_id=device, device_id_type=MESH)

    def start(copies):
        for cp in copies:
            cp.start()

    def both(south, north, action):
        @pl.when(has_s)
        def _():
            for cp in south:
                action(cp)

        @pl.when(has_n)
        def _():
            for cp in north:
                action(cp)

    def arrived(south_from, north_from):
        both(south_from, north_from, lambda cp: cp.wait_recv())

    wloads, loads = {}, {}
    for f, src in enumerate((eta_in, tv_in, tu_in, dep_in, cnt_in)):
        for t in range(NT):
            dst = wide.at[f, t, pl.ds(WO, NR), :] if f < 4 else cnt_i.at[t]
            wloads[f, t] = pltpu.make_async_copy(src.at[:, pl.ds(LANE * t, LANE)], dst, w_sem.at[f * NT + t])
    for f, src in enumerate((u_in, v_in, t_in, s_in)):
        for t in range(NT):
            loads[f, t] = pltpu.make_async_copy(src.at[:, :, pl.ds(LANE * t, LANE)], fb.at[f, t, :, pl.ds(RO, NR), :], in_sem.at[f * NT + t])
    for t in range(NT):
        wloads[5, t] = pltpu.make_async_copy(dep_in.at[:, pl.ds(LANE * t, LANE)], near.at[1, t, pl.ds(RO, NR), :], w_sem.at[5 * NT + t])
    start(wloads.values())
    order = [(f, t) for g in (0, 2) for tiles in ((0, 3), (1, 2)) for f in (g, g + 1) for t in tiles]
    start([loads[key] for key in order])

    for i in range(5):
        for rr in (0, SUB, WR - 2 * SUB, WR - SUB):
            for f in range(4):
                wide[f, i, pl.ds(rr, SUB), :] = zero8
            for f in range(2):
                abuf[f, i, pl.ds(rr, SUB), :] = zero8

    barrier = pltpu.get_barrier_semaphore()
    pl.semaphore_signal(barrier, inc=1, device_id=dev(0, ocol), device_id_type=MESH)

    @pl.when(has_n)
    def _():
        for c in (col, ocol):
            pl.semaphore_signal(barrier, inc=1, device_id=dev(1, c), device_id_type=MESH)

    @pl.when(has_s)
    def _():
        for c in (col, ocol):
            pl.semaphore_signal(barrier, inc=1, device_id=dev(-1, c), device_id_type=MESH)

    def greet(rows_of):
        for d in rows_of:
            pl.semaphore_signal(barrier, inc=1, device_id=dev(d, col), device_id_type=MESH)

    pl.when(up)(lambda: greet((half_row, 1 - half_row)))
    pl.when(down)(lambda: greet((half_row - 1, -half_row)))
    pl.when(first_row)(lambda: greet((half_row - 1, half_row)))
    pl.when(last_row)(lambda: greet((-half_row, 1 - half_row)))

    def fill(first3, first2):
        def body(i, _):
            for f in range(4):
                fb[f, i, :, pl.ds(first3, SUB), :] = jnp.zeros((NL, SUB, LANE), F32)
            return 0
        lax.fori_loop(0, 5, body, 0)
        for i in range(5):
            for f in range(4):
                wide[f, i, pl.ds(first2, NR), :] = jnp.zeros((NR, LANE), F32)
            for f in range(2):
                abuf[f, i, pl.ds(first2, NR), :] = jnp.zeros((NR, LANE), F32)
            for f in range(2):
                near[f, i, pl.ds(first3, SUB), :] = zero8

    @pl.when(jnp.logical_not(has_s))
    def _():
        fill(0, WO - NR)

    @pl.when(jnp.logical_not(has_n))
    def _():
        fill(RO + NR, WO + NR)

    for cp in wloads.values():
        cp.wait()
    for t in range(NT):
        cnt[t, pl.ds(RO, NR), :] = cnt_i[t].astype(F32)
    lane = lanes()
    outer = lane < LANE // 2
    middle = jnp.logical_and(lane >= NR, lane < LANE - NR)

    def edges(buf, f, first):
        rows = pl.ds(first, SUB)
        return jnp.where(outer, buf[f, 0, rows, :], buf[f, 3, rows, :])

    def paired(buf, f, g, first):
        return jnp.where(middle, pltpu.roll(edges(buf, g, first), LANE // 2, 1), edges(buf, f, first))

    for j in range(4):
        mine = pl.ds(SUB * j, SUB)
        first = WO + SUB * j
        for f in range(2):
            wsend[f, mine, :] = paired(wide, f, f + 2, first)
        own = pl.ds(RO + SUB * j, SUB)
        for f in range(2):
            wsend[2 + f, mine, :] = jnp.where(outer, near[f, 0, own, :], near[f, 3, own, :])

    round_about = jnp.logical_or(jnp.logical_or(up, down), jnp.logical_or(first_row, last_row))
    barrier_count = 1 + 2 * has_n.astype(jnp.int32) + 2 * has_s.astype(jnp.int32) + 2 * round_about.astype(jnp.int32)
    pl.semaphore_wait(barrier, barrier_count)

    own4 = pl.ds(0, NT)
    two = pl.ds(0, 2)
    top, low, north, south = RO + NR - 1, RO, RO + NR, RO - 1
    n_src, n_dst, s_src, s_dst = WO + NR - NH, WO - NH, WO, WO + NR

    def rows3(f, a, b, d):
        return remote(fb.at[f, own4, :, pl.ds(a, 1), :], fb.at[f, own4, :, pl.ds(b, 1), :], dev(d, col))

    def rows2(buf, f, nf, a, b, d):
        return remote(buf.at[pl.ds(f, nf), own4, pl.ds(a, NH), :], buf.at[pl.ds(f, nf), own4, pl.ds(b, NH), :], dev(d, col))

    def row1(a, b, d):
        return remote(near.at[:, own4, pl.ds(a, 1), :], near.at[:, own4, pl.ds(b, 1), :], dev(d, col))

    def corner(a, b, d):
        return remote(wsend.at[two, pl.ds(a - WO, NH), :], wide.at[two, 4, pl.ds(b, NH), :], dev(d, ocol))

    z_wide = [
        remote(wsend.at[pl.ds(2, 2)], near.at[:, 4, pl.ds(RO, NR), :], dev(0, ocol)),
        remote(wsend.at[two], wide.at[two, 4, pl.ds(WO, NR), :], dev(0, ocol)),
    ]
    n_first = [row1(top, south, 1)]
    s_first = [row1(low, north, -1)]

    def via(src_row, dst_row, there, onward):
        leg1 = remote(wide.at[:, own4, pl.ds(src_row, NH), :], relay, dev(there, col))
        leg2 = remote(relay, wide.at[:, own4, pl.ds(dst_row, NH), :], dev(onward, col))
        return leg1, leg2

    n_leg1, n_leg2 = via(n_src, n_dst, half_row, 1 - half_row)
    s_leg1, s_leg2 = via(s_src, s_dst, -half_row, half_row - 1)
    pl.when(up)(n_leg1.start)
    pl.when(down)(s_leg1.start)
    start(z_wide)
    both(s_first, n_first, lambda cp: cp.start())

    def slot(k, j):
        return (4 * k + j) // 64, 2 * ((4 * k + j) % 64)

    def pack(half_of, _):
        @pl.when(half_of == 1)
        def _():
            for t in (0, 3):
                for f in (2, 3):
                    loads[f, t].wait()

        here = lanes()
        first = lax.broadcasted_iota(jnp.int32, (NR, LANE), 1) == 0
        acc = {}
        for k in range(NL):
            for f in range(2):
                field = 2 * half_of + f
                both_edges = lax.select(first, fb[field, 0, k, all_rows, :], fb[field, 3, k, all_rows, :])
                for j in range(4):
                    word, at = slot(k, j)
                    pair = both_edges[SUB * j:SUB * (j + 1)]
                    if at:
                        mine = jnp.logical_or(here == at, here == at - 1)
                        acc[f, word] = lax.select(mine, pltpu.roll(pair, at, 1), acc[f, word])
                    else:
                        acc[f, word] = pair
        for f, word in acc:
            pk_s[2 * half_of + f, word] = acc[f, word]
        return 0

    def unpack(half_of, _):
        for f in range(2):
            field = 2 * half_of + f
            got = [pk_r[field, word] for word in range(2)]
            for k in range(NL):
                parts = []
                for j in range(4):
                    word, at = slot(k, j)
                    parts.append(pltpu.roll(got[word], LANE - at, 1) if at else got[word])
                fb[field, 4, k, all_rows, :] = jnp.concatenate(parts, axis=0)
        return 0

    def shift_u(t):
        for k in range(NL):
            uw_b[t, k, all_rows, :] = west_all(ub[t, k, all_rows, :], ub[lax.rem(t + 4, 5), k, all_rows, :])

    def shift_v(t):
        for k in range(NL):
            ve_b[t, k, all_rows, :] = east_all(vb[t, k, all_rows, :], vb[t + 1, k, all_rows, :])

    for t in (0, 3, 1, 2):
        for f in (0, 1):
            loads[f, t].wait()
    n_vel = [rows3(0, top, south, 1), rows3(1, top, south, 1),
             remote(fb.at[1, 0, :, pl.ds(top, 1), :], fb.at[1, 4, :, pl.ds(south, 1), :], dev(1, ocol))]
    s_vel = [rows3(0, low, north, -1), rows3(1, low, north, -1),
             remote(fb.at[0, 3, :, pl.ds(low, 1), :], fb.at[0, 4, :, pl.ds(north, 1), :], dev(-1, ocol))]
    both(s_vel, n_vel, lambda cp: cp.start())

    def shift_own(t, _):
        shift_u(t + 1)
        shift_v(t)
        return 0
    lax.fori_loop(0, 3, shift_own, 0)

    n_tra = [rows3(2, top, south, 1), rows3(3, top, south, 1)]
    s_tra = [rows3(2, low, north, -1), rows3(3, low, north, -1)]
    n_far, s_far = rows2(wide, 0, 4, n_src, n_dst, 1), rows2(wide, 0, 4, s_src, s_dst, -1)
    n_cor, s_cor = corner(n_src, n_dst, 1), corner(s_src, s_dst, -1)
    far_n, far_s = jnp.logical_and(has_n, jnp.logical_not(up)), jnp.logical_and(has_s, jnp.logical_not(down))
    lax.fori_loop(0, 2, pack, 0)
    z_col = remote(pk_s, pk_r, dev(0, ocol))
    z_col.start()
    for t in (1, 2):
        for f in (2, 3):
            loads[f, t].wait()
    both(s_tra, [], lambda cp: cp.start())

    p_unit = 0.5 * BC_GRAVITY / NL

    def pressure(t, rows, height):
        total = jnp.zeros((height, LANE), F32)
        for k in range(NL):
            part = (p_unit * CONTRACT_S) * sb[t, k, rows, :] - (p_unit * EXPAND_T) * tb[t, k, rows, :]
            here = total + part
            pb[t, k, rows, :] = here
            total = here + part

    def pressure_own(t, _):
        pressure(t, all_rows, NR)
        return 0
    lax.fori_loop(0, NT, pressure_own, 0)

    def chooser(height):
        nothing = jnp.zeros((height, LANE), F32)

        def pick(mask, inner, last):
            return lax.select(mask, jnp.full((height, LANE), inner, F32), jnp.full((height, LANE), last, F32))

        def keep(mask, value):
            return lax.select(mask, value, nothing)

        return nothing, pick, keep

    def momentum(lt, j, height=SUB, at_south=False, at_north=False):
        west_of, east_of = movers(height)
        zero8, pick, keep = chooser(height)

        def near2d(buf):
            c = buf[lt, rc, :]
            return c, east_of(c, buf[lt + 1, rc, :]), buf[lt, rn, :]

        rc, rn, rs = pl.ds(RO + SUB * j, height), pl.ds(RO + 1 + SUB * j, height), pl.ds(RO - 1 + SUB * j, height)
        ro = pl.ds(SUB * j, height)
        t, right, left = lt, lax.rem(lt + 1, 5), lax.rem(lt + 4, 5)
        fu, fv = corio(row * NR + SUB * j, total_rows, height)
        fu4 = 0.25 * fu
        fv4 = 0.25 * fv
        c0, ce, cn = near2d(cnt)
        lu = jnp.minimum(c0, ce)
        lv = jnp.minimum(c0, cn)
        d0, de, dn = near2d(depth)
        hu = 0.5 * (d0 + de)
        hv = 0.5 * (d0 + dn)
        lu_o[lt, ro, :] = lu
        lv_o[lt, ro, :] = lv
        hu_s[lt, ro, :] = hu
        hv_s[lt, ro, :] = hv
        yu, yv = zero8, zero8
        su, sv = zero8, zero8
        for k in range(NL):
            u = ub[t, k, rc, :]
            v = vb[t, k, rc, :]
            uw = uw_b[t, k, rc, :]
            ue = east_of(u, ub[right, k, rc, :])
            un = ub[t, k, rn, :]
            us = ub[t, k, rs, :]
            unw = west_of(un, ub[left, k, rn, :]) if at_north else uw_b[t, k, rn, :]
            vw = west_of(v, vb[left, k, rc, :])
            ve = ve_b[t, k, rc, :]
            vn = vb[t, k, rn, :]
            vs = vb[t, k, rs, :]
            vse = east_of(vs, vb[right, k, rs, :]) if at_south else ve_b[t, k, rs, :]
            v4 = (v + ve) + (vs + vse)
            u4 = (u + uw) + (un + unw)
            p = pb[t, k, rc, :]
            pe = east_of(p, pb[right, k, rc, :])
            pn = pb[t, k, rn, :]
            ustar = u + (v4 * (fu4 - 0.125 * (un - us)) - 0.5 * u * (ue - uw) - (pe - p))
            vstar = v - (u4 * (fv4 + 0.125 * (ve - vw)) + 0.5 * v * (vn - vs) + (pn - p))
            yu = (ustar + yu) * (pick(lu > k + 1, VISC_IN[k], VISC_END[k]) if k < NL - 1 else VISC_END[k])
            yv = (vstar + yv) * (pick(lv > k + 1, VISC_IN[k], VISC_END[k]) if k < NL - 1 else VISC_END[k])
            if k < NL - 1:
                us_o[lt, k, ro, :] = yu
                vs_o[lt, k, ro, :] = yv
            su = su + keep(lu > k, u)
            sv = sv + keep(lv > k, v)
        mu, mv = zero8, zero8
        xu, xv = zero8, zero8
        for k in reversed(range(NL)):
            xu = yu if k == NL - 1 else us_o[lt, k, ro, :] + (keep(lu > k + 1, VISC_IN[k] * xu))
            xv = yv if k == NL - 1 else vs_o[lt, k, ro, :] + (keep(lv > k + 1, VISC_IN[k] * xv))
            us_o[lt, k, ro, :] = xu
            vs_o[lt, k, ro, :] = xv
            mu = mu + keep(lu > k, xu)
            mv = mv + keep(lv > k, xv)
        mu, mv = (ONE / VISC_R) * mu, (ONE / VISC_R) * mv
        iu = ONE / jnp.maximum(lu, ONE)
        iv = ONE / jnp.maximum(lv, ONE)
        mu_s[lt, ro, :] = mu * iu
        mv_s[lt, ro, :] = mv * iv
        scale = dtb * dtb / TIME_STEP
        rw = pl.ds(WO + SUB * j, height)
        abuf[0, lt, rw, :] = jnp.where(lu > ZERO, scale * hu * ((mu - su) * iu), ZERO)
        abuf[1, lt, rw, :] = jnp.where(lv > ZERO, scale * hv * ((mv - sv) * iv), ZERO)

    def middle_rows(i, _):
        odd, later = lax.rem(i, 2), i // 2

        @pl.when(jnp.logical_and(i == 3, last_row))
        def _():
            n_leg1.wait_recv()
            n_leg2.start()

        @pl.when(jnp.logical_and(i == 3, first_row))
        def _():
            s_leg1.wait_recv()
            s_leg2.start()

        @pl.when(i == LATE)
        def _():
            both([], n_tra, lambda cp: cp.start())
            pl.when(far_n)(n_far.start)
            pl.when(far_s)(s_far.start)
            both([s_cor], [n_cor], lambda cp: cp.start())

        @pl.when(i == 2)
        def _():
            for cp in (z_wide[0], z_col):
                cp.wait_recv()
            lax.fori_loop(0, 2, unpack, 0)
            shift_u(0)
            shift_v(3)
            pressure(4, all_rows, NR)

        momentum(1 + odd + later * (2 * odd - 1), 1, 2 * SUB)
        return 0

    lax.fori_loop(0, NT, middle_rows, 0)

    arrived(n_first + n_vel, s_first + s_vel + s_tra)

    def pressure_north(i, _):
        for odd in range(2):
            pressure(2 * i + odd, pl.ds(RO + NR, SUB), SUB)
        return 0
    lax.fori_loop(0, 2, pressure_north, 0)

    def force_corner(a, b, d):
        return remote(asend.at[pl.ds(a - WO, NH), :], abuf.at[0, 4, pl.ds(b, NH), :], dev(d, ocol))

    def force_rows(t, a, b, d):
        return remote(abuf.at[:, t, pl.ds(a, NH), :], abuf.at[:, t, pl.ds(b, NH), :], dev(d, col))

    def force_pair(t):
        return force_rows(t, n_src, n_dst, 1), force_rows(t, s_src, s_dst, -1)

    z_force = remote(asend, abuf.at[0, 4, pl.ds(WO, NR), :], dev(0, ocol))
    n_fcor, s_fcor = force_corner(n_src, n_dst, 1), force_corner(s_src, s_dst, -1)

    force = [force_pair(t) for t in range(NT)]
    n_force = [p[0] for p in force] + [n_fcor]
    s_force = [p[1] for p in force] + [s_fcor]

    def send_force(which):
        both([s_force[i] for i in which], [n_force[i] for i in which], lambda cp: cp.start())

    def ends(i, _):
        t = lax.rem(3 * i, 4)
        momentum(t, 0, at_south=True)
        momentum(t, 3, at_north=True)

        @pl.when(i == 1)
        def _():
            for j in range(4):
                asend[pl.ds(SUB * j, SUB), :] = paired(abuf, 0, 1, WO + SUB * j)
            z_force.start()
            send_force((0, 3, 4))

        @pl.when(i == 2)
        def _():
            send_force((2,))
        return 0

    lax.fori_loop(0, NT, ends, 0)
    send_force((1,))

    arrived(n_tra, [])

    def tracers(lt, j, height):
        west_of, east_of = movers(height)
        zero8, pick, keep = chooser(height)
        rc, rn, rs = pl.ds(RO + SUB * j, height), pl.ds(RO + 1 + SUB * j, height), pl.ds(RO - 1 + SUB * j, height)
        ro = pl.ds(SUB * j, height)
        t, right, left = lt, lax.rem(lt + 1, 5), lax.rem(lt + 4, 5)
        c0 = cnt[lt, rc, :]
        luw = jnp.minimum(c0, west_of(c0, cnt[left, rc, :]))
        lvs = jnp.minimum(c0, cnt[lt, rs, :])
        lu = lu_o[lt, ro, :]
        lv = lv_o[lt, ro, :]
        yt, ys = zero8, zero8
        for k in range(NL):
            here = c0 > k
            me = keep(lu > k, ub[t, k, rc, :])
            mw = keep(luw > k, uw_b[t, k, rc, :])
            mn = keep(lv > k, vb[t, k, rc, :])
            ms = keep(lvs > k, vb[t, k, rs, :])
            own = 2.0 - ((me - mw) + (mn - ms))

            def advect(buf):
                q = buf[t, k, rc, :]
                qe = east_of(q, buf[right, k, rc, :])
                qw = west_of(q, buf[left, k, rc, :])
                return (own * q + (mw * qw - me * qe)) + (ms * buf[t, k, rs, :] - mn * buf[t, k, rn, :])

            end = pick(here, DIFF_END[k], 0.5)
            fac = lax.select(c0 > k + 1, jnp.full_like(end, DIFF_IN[k]), end) if k < NL - 1 else end
            yt = (advect(tb) + keep(here, yt)) * fac
            ys = (advect(sb) + keep(here, ys)) * fac
            if k < NL - 1:
                tn_o[lt, k, ro, :] = yt
                sn_o[lt, k, ro, :] = ys
        xt, xs_ = zero8, zero8
        for k in reversed(range(NL)):
            xt = yt if k == NL - 1 else tn_o[lt, k, ro, :] + keep(c0 > k + 1, DIFF_IN[k] * xt)
            xs_ = ys if k == NL - 1 else sn_o[lt, k, ro, :] + keep(c0 > k + 1, DIFF_IN[k] * xs_)
            tn_o[lt, k, ro, :] = xt
            sn_o[lt, k, ro, :] = xs_

    def tracers_all(i, _):
        tracers(lax.rem(i, NT), T_TILES * (i // NT), T_TILES * SUB)
        return 0
    lax.fori_loop(0, 16 // T_TILES, tracers_all, 0)

    z_wide[1].wait_recv()
    z_force.wait_recv()
    pl.when(far_s)(n_far.wait_recv)
    pl.when(far_n)(s_far.wait_recv)
    pl.when(down)(n_leg2.wait_recv)
    pl.when(up)(s_leg2.wait_recv)
    arrived([n_cor] + n_force, [s_cor] + s_force)

    for cp in z_wide + [z_col, z_force]:
        cp.wait_send()
    both(s_first + s_vel + s_tra + [s_cor] + s_force, n_first + n_vel + n_tra + [n_cor] + n_force, lambda cp: cp.wait_send())
    pl.when(far_n)(n_far.wait_send)
    pl.when(far_s)(s_far.wait_send)
    pl.when(up)(n_leg1.wait_send)
    pl.when(down)(s_leg1.wait_send)
    pl.when(last_row)(n_leg2.wait_send)
    pl.when(first_row)(s_leg2.wait_send)


def finish_kernel(n_row, n_sub, w_ref,
                  us, vs, tn, sn, wide, abuf, lu, lv, hu_s, hv_s, mu_s, mv_s,
                  eta_o, tu_o, tv_o, u_o, v_o, t_o, s_o,
                  bu, bv, cfu, cfv, mku, mkv, tu, tv, xs, acu, acv, cu, cv, flat_b, ubuf, vbuf, sem):
    row = lax.axis_index('row')
    dtb = TIME_STEP / n_sub
    total_rows = float(n_row * NR)
    zero8 = jnp.zeros((SUB, LANE), F32)
    west_of, east_of = movers()
    copies = []

    def put(src, dst):
        cp = pltpu.make_async_copy(src, dst, sem.at[len(copies)])
        cp.start()
        copies.append(cp)

    for src, dst in ((tn, t_o), (sn, s_o)):
        for t in range(NT):
            put(src.at[t], dst.at[:, :, pl.ds(LANE * t, LANE)])

    def setup(i):
        base = SUB + SUB * i
        rows = pl.ds(base, SUB)
        rown = pl.ds(base + 1, SUB)
        first = row * NR + SUB * i - NR
        fu, fv = corio(first, total_rows)
        place = first + lax.broadcasted_iota(jnp.int32, (SUB, LANE), 0)
        inside = place >= 0
        wet_u = jnp.logical_and(inside, place < n_row * NR).astype(F32)
        wet_v = jnp.logical_and(inside, place < n_row * NR - 1).astype(F32)
        cfu[rows, :] = wet_u * ((0.25 * dtb) * fu)
        cfv[rows, :] = wet_v * ((0.25 * dtb) * fv)
        mku[rows, :] = wet_u
        mkv[rows, :] = wet_v
        for t in range(5):
            right = (t + 1) % 5
            d0 = wide[3, t, rows, :]
            scale = 0.5 * dtb * dtb * GRAVITY
            bu[t, rows, :] = wet_u * (scale * (d0 + east_of(d0, wide[3, right, rows, :])))
            bv[t, rows, :] = wet_v * (scale * (d0 + wide[3, t, rown, :]))
            tu[0, t, rows, :] = dtb * wide[2, t, rows, :]
            tv[0, t, rows, :] = dtb * wide[1, t, rows, :]

    for i in range(12):
        rows = pl.ds(SUB + SUB * i, SUB)
        for f in range(2):
            wide[f + 2, 4, rows, :] = pltpu.roll(wide[f, 4, rows, :], LANE // 2, 1)
        abuf[1, 4, rows, :] = pltpu.roll(abuf[0, 4, rows, :], LANE // 2, 1)
    for i in range(12):
        setup(i)
    for t in range(NT):
        acu[t] = jnp.zeros((NR, LANE), F32)
        acv[t] = jnp.zeros((NR, LANE), F32)

    def subcycle(n, cur, lo, hi, first=False):
        nxt = 1 - cur
        weight = w_ref[n] * (ONE / dtb)
        def eta_part(i):
            rows, rows_s = pl.ds(SUB + SUB * i, SUB), pl.ds(7 + SUB * i, SUB)
            u0 = [tu[cur, t, rows, :] for t in range(5)]
            v0 = [tv[cur, t, rows, :] for t in range(5)]
            vs = [tv[cur, t, rows_s, :] for t in range(5)]
            uw = [west_of(u0[t], u0[(t + 4) % 5]) for t in range(5)]
            u2 = [u0[t] + uw[t] for t in range(5)]
            es = [wide[0, t, rows, :] - ((u0[t] - uw[t]) + (v0[t] - vs[t])) for t in range(5)]
            for t in range(5):
                wide[0, t, rows, :] = es[t]
                xs[t, rows, :] = u2[t]

        def flow_part(i):
            rows, rows_n = pl.ds(SUB + SUB * i, SUB), pl.ds(9 + SUB * i, SUB)
            f_u, f_v = cfu[rows, :], cfv[rows, :]
            rows_s = pl.ds(7 + SUB * i, SUB)
            v0 = [tv[cur, t, rows, :] for t in range(5)]
            v2 = [v0[t] + tv[cur, t, rows_s, :] for t in range(5)]
            v4 = [v2[t] + east_of(v2[t], v2[(t + 1) % 5]) for t in range(5)]
            es = [wide[0, t, rows, :] for t in range(5)]
            for t in range(5):
                slope_u = east_of(es[t], es[(t + 1) % 5]) - es[t]
                slope_v = wide[0, t, rows_n, :] - es[t]
                u4 = xs[t, rows, :] + xs[t, rows_n, :]
                u_old, v_old = tu[cur, t, rows, :], tv[cur, t, rows, :]
                if first:
                    u_old = mku[rows, :] * u_old
                    v_old = mkv[rows, :] * v_old
                u_new = (u_old + abuf[0, t, rows, :]) + (f_u * v4[t] - bu[t, rows, :] * slope_u)
                v_new = (v_old + abuf[1, t, rows, :]) - (f_v * u4 + bv[t, rows, :] * slope_v)
                tu[nxt, t, rows, :] = u_new
                tv[nxt, t, rows, :] = v_new
                if 4 <= i < SUB and t < NT:
                    ro = pl.ds(SUB * (i - 4), SUB)
                    acu[t, ro, :] += weight * u_new
                    acv[t, ro, :] += weight * v_new

        for part in (eta_part, flow_part):
            for i in reversed(range(lo, hi)):
                part(i)

    def pairs(first_n, count, lo, hi):
        def body(i, _):
            n = first_n + 2 * i
            subcycle(n, 0, lo, hi)
            subcycle(n + 1, 1, lo, hi)
            return 0
        lax.fori_loop(0, count, body, 0)

    subcycle(0, 0, 0, 12, first=True)
    subcycle(1, 1, 0, 12)
    pairs(2, 2, 0, 12)
    pairs(6, 4, 1, 11)
    pairs(14, 4, 2, 10)
    pairs(22, 4, 3, 9)

    for t in range(NT):
        for j in range(4):
            rw = pl.ds(WO + SUB * j, SUB)
            ro = pl.ds(SUB * j, SUB)
            flat_b[0, t, ro, :] = wide[0, t, rw, :]
            flat_b[1, t, ro, :] = (ONE / dtb) * tu[0, t, rw, :]
            flat_b[2, t, ro, :] = (ONE / dtb) * tv[0, t, rw, :]
            cu[t, ro, :] = acu[t, ro, :] / hu_s[t, ro, :] - mu_s[t, ro, :]
            hv = hv_s[t, ro, :]
            cv[t, ro, :] = acv[t, ro, :] / hv - mv_s[t, ro, :]

    for f, dst in enumerate((eta_o, tu_o, tv_o)):
        for t in range(NT):
            put(flat_b.at[f, t], dst.at[:, pl.ds(LANE * t, LANE)])
    for lev, cor, src, buf, dst in ((lu, cu, us, ubuf, u_o), (lv, cv, vs, vbuf, v_o)):
        for t in range(NT):
            for j in range(4):
                ro = pl.ds(SUB * j, SUB)
                count = lev[t, ro, :]
                shift = cor[t, ro, :]
                for k in range(NL):
                    buf[t, k, ro, :] = jnp.where(count > k, (ONE / VISC_R) * src[t, k, ro, :] + shift, ZERO)
            put(buf.at[t], dst.at[:, :, pl.ds(LANE * t, LANE)])
    for cp in copies:
        cp.wait()


def solution(mesh):
    n_row = mesh.shape['row']

    def step(vel_u, vel_v, temperature, salinity, surf_eta, trans_u, trans_v, bottom_depth, level_count, avg_weights):
        n_sub = avg_weights.shape[0]
        hbm = pl.BlockSpec(memory_space=pltpu.HBM)
        vmem = pl.BlockSpec(memory_space=pltpu.VMEM)
        smem = pl.BlockSpec(memory_space=pltpu.SMEM)
        cube_v = pltpu.VMEM((NT, NL, NR, LANE), F32)
        flat_v = pltpu.VMEM((NT, NR, LANE), F32)
        wide1 = pltpu.VMEM((5, WR, LANE), F32)
        wide_v = pltpu.VMEM((4, 5, WR, LANE), F32)
        force_v = pltpu.VMEM((2, 5, WR, LANE), F32)
        sems = pltpu.SemaphoreType.DMA
        outs = [cube_v] * 4 + [wide_v, force_v] + [flat_v] * 6
        mids = pl.pallas_call(
            functools.partial(ocean_kernel, n_row, n_sub),
            out_shape=outs,
            in_specs=[hbm] * 9,
            out_specs=[vmem] * len(outs),
            scratch_shapes=[
                pltpu.VMEM((4, 5, NL, RO + NR + SUB, LANE), F32),
                pltpu.VMEM((5, NL, RO + NR + SUB, LANE), F32),
                pltpu.VMEM((NT, NL, RO + NR + SUB, LANE), F32),
                pltpu.VMEM((NT, NL, RO + NR + SUB, LANE), F32),
                pltpu.VMEM((2, 5, RO + NR + SUB, LANE), F32),
                pltpu.VMEM((4, NT, NH, LANE), F32),
                pltpu.VMEM((4, NR, LANE), F32),
                pltpu.VMEM((NT, NR, LANE), jnp.int32),
                pltpu.VMEM((4, 2, SUB, LANE), F32),
                pltpu.VMEM((4, 2, SUB, LANE), F32),
                pltpu.VMEM((NR, LANE), F32),
                sems((16,)), sems((24,)), sems((N_COPY,)), sems((N_COPY,)),
            ],
            compiler_params=pltpu.CompilerParams(collective_id=0, has_side_effects=True, vmem_limit_bytes=VMEM_MAIN),
            name='ocean',
        )(*[pltpu.with_memory_space_constraint(x, pltpu.HBM) for x in (vel_u, vel_v, temperature, salinity, surf_eta, trans_u, trans_v, bottom_depth, level_count)])
        cube = jax.ShapeDtypeStruct((NL, NR, NT * LANE), F32)
        flat = jax.ShapeDtypeStruct((NR, NT * LANE), F32)
        return pl.pallas_call(
            functools.partial(finish_kernel, n_row, n_sub),
            out_shape=[flat] * 3 + [cube] * 4,
            in_specs=[smem] + [vmem] * len(outs),
            out_specs=[hbm] * 7,
            scratch_shapes=[wide1] * 2 + [pltpu.VMEM((WR, LANE), F32)] * 4 + [force_v, force_v, wide1] + [flat_v] * 4 + [pltpu.VMEM((3, NT, NR, LANE), F32), cube_v, cube_v, sems((28,))],
            compiler_params=pltpu.CompilerParams(vmem_limit_bytes=VMEM_FINISH),
            name='finish',
        )(avg_weights, *mids)

    cube = P(None, 'row', 'col')
    flat = P('row', 'col')
    return jax.shard_map(step, mesh=mesh, in_specs=(cube, cube, cube, cube, flat, flat, flat, flat, flat, P()), out_specs=(flat, flat, flat, cube, cube, cube, cube), check_vma=False)
```

```python
import functools

import jax
import jax.numpy as jnp
from jax import lax
from jax.experimental import pallas as pl
from jax.experimental.pallas import tpu as pltpu
from jax.sharding import PartitionSpec as P

TIME_STEP = 1.0
GRAVITY = 16.0
BC_GRAVITY = 4.0
EXPAND_T = 0.2
CONTRACT_S = 0.6
CORIO_F0 = 0.4
CORIO_BETA = 0.4
VISC_R = 2.0
DIFF_R = 0.5

MESH = pl.DeviceIdType.MESH
F32 = jnp.float32

SUB = 8
LANE = 128
ZERO = 0.0
ONE = 1.0
NL = 31
NR = 32
NT = 4
RO = 8
WO = 40
WR = 112
N_COPY = 40
LATE = 2
T_TILES = 4
NH = 30
VMEM_MAIN = 40 * 1024 * 1024
VMEM_FINISH = 12 * 1024 * 1024


def factors(strength):
    inner, last = [], []
    before = ZERO
    for level in range(NL):
        low = ZERO if level == 0 else strength
        inner.append(strength / (ONE + low + strength - low * before))
        last.append(strength / (ONE + low - low * before))
        before = inner[-1]
    return inner, last


VISC_IN, VISC_END = factors(VISC_R)
DIFF_IN, DIFF_END = factors(DIFF_R)


def lanes():
    return lax.broadcasted_iota(jnp.int32, (SUB, LANE), 1)


def movers(height=SUB):
    here = lax.broadcasted_iota(jnp.int32, (height, LANE), 1)
    first, last = here == 0, here == LANE - 1

    def west_of(own, left):
        return pltpu.roll(lax.select(last, left, own), 1, 1)

    def east_of(own, right):
        return pltpu.roll(lax.select(first, right, own), LANE - 1, 1)

    return west_of, east_of


def corio(first, total_rows, height=SUB):
    pos = (first + lax.broadcasted_iota(jnp.int32, (height, LANE), 0)).astype(F32)
    fu = CORIO_F0 + CORIO_BETA * ((pos + 0.5) / total_rows - 0.5)
    fv = CORIO_F0 + CORIO_BETA * ((pos + ONE) / total_rows - 0.5)
    return fu, fv


def ocean_kernel(n_row, n_sub,
                 u_in, v_in, t_in, s_in, eta_in, tu_in, tv_in, dep_in, cnt_in,
                 us_o, vs_o, tn_o, sn_o, wide, abuf, lu_o, lv_o, hu_s, hv_s, mu_s, mv_s,
                 fb, pb, uw_b, ve_b, near, relay, wsend, cnt_i, pk_s, pk_r, asend,
                 in_sem, w_sem, send, recv):
    row = lax.axis_index('row')
    col = lax.axis_index('col')
    ocol = 1 - col
    has_s = row > 0
    has_n = row < n_row - 1
    dtb = TIME_STEP / n_sub
    total_rows = float(n_row * NR)
    used = []
    ub, vb, tb, sb = (fb.at[f] for f in range(4))
    zero8 = jnp.zeros((SUB, LANE), F32)
    west_of, east_of = movers()
    west_all, east_all = movers(NR)
    all_rows = pl.ds(RO, NR)
    cnt, depth = near.at[0], near.at[1]
    half_row = n_row // 2
    up, down = row == half_row - 1, row == half_row
    first_row, last_row = row == 0, row == n_row - 1

    def dev(step, c):
        return {'row': row + step, 'col': c}

    def remote(src, dst, device):
        used.append(0)
        idx = len(used) - 1
        return pltpu.make_async_remote_copy(src, dst, send.at[idx], recv.at[idx], device_id=device, device_id_type=MESH)

    def start(copies):
        for cp in copies:
            cp.start()

    def both(south, north, action):
        @pl.when(has_s)
        def _():
            for cp in south:
                action(cp)

        @pl.when(has_n)
        def _():
            for cp in north:
                action(cp)

    def arrived(south_from, north_from):
        both(south_from, north_from, lambda cp: cp.wait_recv())

    wloads, loads = {}, {}
    for f, src in enumerate((eta_in, tv_in, tu_in, dep_in, cnt_in)):
        for t in range(NT):
            dst = wide.at[f, t, pl.ds(WO, NR), :] if f < 4 else cnt_i.at[t]
            wloads[f, t] = pltpu.make_async_copy(src.at[:, pl.ds(LANE * t, LANE)], dst, w_sem.at[f * NT + t])
    for f, src in enumerate((u_in, v_in, t_in, s_in)):
        for t in range(NT):
            loads[f, t] = pltpu.make_async_copy(src.at[:, :, pl.ds(LANE * t, LANE)], fb.at[f, t, :, pl.ds(RO, NR), :], in_sem.at[f * NT + t])
    for t in range(NT):
        wloads[5, t] = pltpu.make_async_copy(dep_in.at[:, pl.ds(LANE * t, LANE)], near.at[1, t, pl.ds(RO, NR), :], w_sem.at[5 * NT + t])
    start(wloads.values())
    order = [(f, t) for g in (0, 2) for tiles in ((0, 3), (1, 2)) for f in (g, g + 1) for t in tiles]
    start([loads[key] for key in order])

    for i in range(5):
        for rr in (0, SUB, WR - 2 * SUB, WR - SUB):
            for f in range(4):
                wide[f, i, pl.ds(rr, SUB), :] = zero8
            for f in range(2):
                abuf[f, i, pl.ds(rr, SUB), :] = zero8

    barrier = pltpu.get_barrier_semaphore()
    pl.semaphore_signal(barrier, inc=1, device_id=dev(0, ocol), device_id_type=MESH)

    @pl.when(has_n)
    def _():
        for c in (col, ocol):
            pl.semaphore_signal(barrier, inc=1, device_id=dev(1, c), device_id_type=MESH)

    @pl.when(has_s)
    def _():
        for c in (col, ocol):
            pl.semaphore_signal(barrier, inc=1, device_id=dev(-1, c), device_id_type=MESH)

    def greet(rows_of):
        for d in rows_of:
            pl.semaphore_signal(barrier, inc=1, device_id=dev(d, col), device_id_type=MESH)

    pl.when(up)(lambda: greet((half_row, 1 - half_row)))
    pl.when(down)(lambda: greet((half_row - 1, -half_row)))
    pl.when(first_row)(lambda: greet((half_row - 1, half_row)))
    pl.when(last_row)(lambda: greet((-half_row, 1 - half_row)))

    def fill(first3, first2):
        def body(i, _):
            for f in range(4):
                fb[f, i, :, pl.ds(first3, SUB), :] = jnp.zeros((NL, SUB, LANE), F32)
            return 0
        lax.fori_loop(0, 5, body, 0)
        for i in range(5):
            for f in range(4):
                wide[f, i, pl.ds(first2, NR), :] = jnp.zeros((NR, LANE), F32)
            for f in range(2):
                abuf[f, i, pl.ds(first2, NR), :] = jnp.zeros((NR, LANE), F32)
            for f in range(2):
                near[f, i, pl.ds(first3, SUB), :] = zero8

    @pl.when(jnp.logical_not(has_s))
    def _():
        fill(0, WO - NR)

    @pl.when(jnp.logical_not(has_n))
    def _():
        fill(RO + NR, WO + NR)

    for cp in wloads.values():
        cp.wait()
    for t in range(NT):
        cnt[t, pl.ds(RO, NR), :] = cnt_i[t].astype(F32)
    lane = lanes()
    outer = lane < LANE // 2
    middle = jnp.logical_and(lane >= NR, lane < LANE - NR)

    def edges(buf, f, first):
        rows = pl.ds(first, SUB)
        return jnp.where(outer, buf[f, 0, rows, :], buf[f, 3, rows, :])

    def paired(buf, f, g, first):
        return jnp.where(middle, pltpu.roll(edges(buf, g, first), LANE // 2, 1), edges(buf, f, first))

    for j in range(4):
        mine = pl.ds(SUB * j, SUB)
        first = WO + SUB * j
        for f in range(2):
            wsend[f, mine, :] = paired(wide, f, f + 2, first)
        own = pl.ds(RO + SUB * j, SUB)
        for f in range(2):
            wsend[2 + f, mine, :] = jnp.where(outer, near[f, 0, own, :], near[f, 3, own, :])

    round_about = jnp.logical_or(jnp.logical_or(up, down), jnp.logical_or(first_row, last_row))
    barrier_count = 1 + 2 * has_n.astype(jnp.int32) + 2 * has_s.astype(jnp.int32) + 2 * round_about.astype(jnp.int32)
    pl.semaphore_wait(barrier, barrier_count)

    own4 = pl.ds(0, NT)
    two = pl.ds(0, 2)
    top, low, north, south = RO + NR - 1, RO, RO + NR, RO - 1
    n_src, n_dst, s_src, s_dst = WO + NR - NH, WO - NH, WO, WO + NR

    def rows3(f, a, b, d):
        return remote(fb.at[f, own4, :, pl.ds(a, 1), :], fb.at[f, own4, :, pl.ds(b, 1), :], dev(d, col))

    def rows2(buf, f, nf, a, b, d):
        return remote(buf.at[pl.ds(f, nf), own4, pl.ds(a, NH), :], buf.at[pl.ds(f, nf), own4, pl.ds(b, NH), :], dev(d, col))

    def row1(a, b, d):
        return remote(near.at[:, own4, pl.ds(a, 1), :], near.at[:, own4, pl.ds(b, 1), :], dev(d, col))

    def corner(a, b, d):
        return remote(wsend.at[two, pl.ds(a - WO, NH), :], wide.at[two, 4, pl.ds(b, NH), :], dev(d, ocol))

    z_wide = [
        remote(wsend.at[pl.ds(2, 2)], near.at[:, 4, pl.ds(RO, NR), :], dev(0, ocol)),
        remote(wsend.at[two], wide.at[two, 4, pl.ds(WO, NR), :], dev(0, ocol)),
    ]
    n_first = [row1(top, south, 1)]
    s_first = [row1(low, north, -1)]

    def via(src_row, dst_row, there, onward):
        leg1 = remote(wide.at[:, own4, pl.ds(src_row, NH), :], relay, dev(there, col))
        leg2 = remote(relay, wide.at[:, own4, pl.ds(dst_row, NH), :], dev(onward, col))
        return leg1, leg2

    n_leg1, n_leg2 = via(n_src, n_dst, half_row, 1 - half_row)
    s_leg1, s_leg2 = via(s_src, s_dst, -half_row, half_row - 1)
    pl.when(up)(n_leg1.start)
    pl.when(down)(s_leg1.start)
    start(z_wide)
    both(s_first, n_first, lambda cp: cp.start())

    def slot(k, j):
        return (4 * k + j) // 64, 2 * ((4 * k + j) % 64)

    def pack(half_of, _):
        @pl.when(half_of == 1)
        def _():
            for t in (0, 3, 1, 2):
                for f in (2, 3):
                    loads[f, t].wait()
            both(s_tra, [], lambda cp: cp.start())

        here = lanes()
        first = lax.broadcasted_iota(jnp.int32, (NR, LANE), 1) == 0
        acc = {}
        for k in range(NL):
            for f in range(2):
                field = 2 * half_of + f
                both_edges = lax.select(first, fb[field, 0, k, all_rows, :], fb[field, 3, k, all_rows, :])
                for j in range(4):
                    word, at = slot(k, j)
                    pair = both_edges[SUB * j:SUB * (j + 1)]
                    if at:
                        mine = jnp.logical_or(here == at, here == at - 1)
                        acc[f, word] = lax.select(mine, pltpu.roll(pair, at, 1), acc[f, word])
                    else:
                        acc[f, word] = pair
        for f, word in acc:
            pk_s[2 * half_of + f, word] = acc[f, word]
        return 0

    def unpack(half_of, _):
        for f in range(2):
            field = 2 * half_of + f
            got = [pk_r[field, word] for word in range(2)]
            for k in range(NL):
                parts = []
                for j in range(4):
                    word, at = slot(k, j)
                    parts.append(pltpu.roll(got[word], LANE - at, 1) if at else got[word])
                fb[field, 4, k, all_rows, :] = jnp.concatenate(parts, axis=0)
        return 0

    def shift_u(t):
        for k in range(NL):
            uw_b[t, k, all_rows, :] = west_all(ub[t, k, all_rows, :], ub[lax.rem(t + 4, 5), k, all_rows, :])

    def shift_v(t):
        for k in range(NL):
            ve_b[t, k, all_rows, :] = east_all(vb[t, k, all_rows, :], vb[t + 1, k, all_rows, :])

    for t in (0, 3, 1, 2):
        for f in (0, 1):
            loads[f, t].wait()
    n_vel = [rows3(0, top, south, 1), rows3(1, top, south, 1),
             remote(fb.at[1, 0, :, pl.ds(top, 1), :], fb.at[1, 4, :, pl.ds(south, 1), :], dev(1, ocol))]
    s_vel = [rows3(0, low, north, -1), rows3(1, low, north, -1),
             remote(fb.at[0, 3, :, pl.ds(low, 1), :], fb.at[0, 4, :, pl.ds(north, 1), :], dev(-1, ocol))]
    both(s_vel, n_vel, lambda cp: cp.start())

    def shift_own(t, _):
        shift_u(t + 1)
        shift_v(t)
        return 0
    lax.fori_loop(0, 3, shift_own, 0)

    n_tra = [rows3(2, top, south, 1), rows3(3, top, south, 1)]
    s_tra = [rows3(2, low, north, -1), rows3(3, low, north, -1)]
    n_far, s_far = rows2(wide, 0, 4, n_src, n_dst, 1), rows2(wide, 0, 4, s_src, s_dst, -1)
    n_cor, s_cor = corner(n_src, n_dst, 1), corner(s_src, s_dst, -1)
    far_n, far_s = jnp.logical_and(has_n, jnp.logical_not(up)), jnp.logical_and(has_s, jnp.logical_not(down))
    lax.fori_loop(0, 2, pack, 0)
    z_col = remote(pk_s, pk_r, dev(0, ocol))
    z_col.start()

    p_unit = 0.5 * BC_GRAVITY / NL

    def pressure(t, rows, height):
        total = jnp.zeros((height, LANE), F32)
        for k in range(NL):
            part = (p_unit * CONTRACT_S) * sb[t, k, rows, :] - (p_unit * EXPAND_T) * tb[t, k, rows, :]
            here = total + part
            pb[t, k, rows, :] = here
            total = here + part

    def pressure_own(t, _):
        pressure(t, all_rows, NR)
        return 0
    lax.fori_loop(0, NT, pressure_own, 0)

    def chooser(height):
        nothing = jnp.zeros((height, LANE), F32)

        def pick(mask, inner, last):
            return lax.select(mask, jnp.full((height, LANE), inner, F32), jnp.full((height, LANE), last, F32))

        def keep(mask, value):
            return lax.select(mask, value, nothing)

        return nothing, pick, keep

    def momentum(lt, j, height=SUB, at_south=False, at_north=False):
        west_of, east_of = movers(height)
        zero8, pick, keep = chooser(height)

        def near2d(buf):
            c = buf[lt, rc, :]
            return c, east_of(c, buf[lt + 1, rc, :]), buf[lt, rn, :]

        rc, rn, rs = pl.ds(RO + SUB * j, height), pl.ds(RO + 1 + SUB * j, height), pl.ds(RO - 1 + SUB * j, height)
        ro = pl.ds(SUB * j, height)
        t, right, left = lt, lax.rem(lt + 1, 5), lax.rem(lt + 4, 5)
        fu, fv = corio(row * NR + SUB * j, total_rows, height)
        fu4 = 0.25 * fu
        fv4 = 0.25 * fv
        c0, ce, cn = near2d(cnt)
        lu = jnp.minimum(c0, ce)
        lv = jnp.minimum(c0, cn)
        d0, de, dn = near2d(depth)
        hu = 0.5 * (d0 + de)
        hv = 0.5 * (d0 + dn)
        lu_o[lt, ro, :] = lu
        lv_o[lt, ro, :] = lv
        hu_s[lt, ro, :] = hu
        hv_s[lt, ro, :] = hv
        yu, yv = zero8, zero8
        su, sv = zero8, zero8
        for k in range(NL):
            u = ub[t, k, rc, :]
            v = vb[t, k, rc, :]
            uw = uw_b[t, k, rc, :]
            ue = east_of(u, ub[right, k, rc, :])
            un = ub[t, k, rn, :]
            us = ub[t, k, rs, :]
            unw = west_of(un, ub[left, k, rn, :]) if at_north else uw_b[t, k, rn, :]
            vw = west_of(v, vb[left, k, rc, :])
            ve = ve_b[t, k, rc, :]
            vn = vb[t, k, rn, :]
            vs = vb[t, k, rs, :]
            vse = east_of(vs, vb[right, k, rs, :]) if at_south else ve_b[t, k, rs, :]
            v4 = (v + ve) + (vs + vse)
            u4 = (u + uw) + (un + unw)
            p = pb[t, k, rc, :]
            pe = east_of(p, pb[right, k, rc, :])
            pn = pb[t, k, rn, :]
            ustar = u + (v4 * (fu4 - 0.125 * (un - us)) - 0.5 * u * (ue - uw) - (pe - p))
            vstar = v - (u4 * (fv4 + 0.125 * (ve - vw)) + 0.5 * v * (vn - vs) + (pn - p))
            yu = (ustar + yu) * (pick(lu > k + 1, VISC_IN[k], VISC_END[k]) if k < NL - 1 else VISC_END[k])
            yv = (vstar + yv) * (pick(lv > k + 1, VISC_IN[k], VISC_END[k]) if k < NL - 1 else VISC_END[k])
            if k < NL - 1:
                us_o[lt, k, ro, :] = yu
                vs_o[lt, k, ro, :] = yv
            su = su + keep(lu > k, u)
            sv = sv + keep(lv > k, v)
        mu, mv = zero8, zero8
        xu, xv = zero8, zero8
        for k in reversed(range(NL)):
            xu = yu if k == NL - 1 else us_o[lt, k, ro, :] + (keep(lu > k + 1, VISC_IN[k] * xu))
            xv = yv if k == NL - 1 else vs_o[lt, k, ro, :] + (keep(lv > k + 1, VISC_IN[k] * xv))
            us_o[lt, k, ro, :] = xu
            vs_o[lt, k, ro, :] = xv
            mu = mu + keep(lu > k, xu)
            mv = mv + keep(lv > k, xv)
        mu, mv = (ONE / VISC_R) * mu, (ONE / VISC_R) * mv
        iu = ONE / jnp.maximum(lu, ONE)
        iv = ONE / jnp.maximum(lv, ONE)
        mu_s[lt, ro, :] = mu * iu
        mv_s[lt, ro, :] = mv * iv
        scale = dtb * dtb / TIME_STEP
        rw = pl.ds(WO + SUB * j, height)
        abuf[0, lt, rw, :] = jnp.where(lu > ZERO, scale * hu * ((mu - su) * iu), ZERO)
        abuf[1, lt, rw, :] = jnp.where(lv > ZERO, scale * hv * ((mv - sv) * iv), ZERO)

    def middle_rows(i, _):
        odd, later = lax.rem(i, 2), i // 2

        @pl.when(jnp.logical_and(i == 3, last_row))
        def _():
            n_leg1.wait_recv()
            n_leg2.start()

        @pl.when(jnp.logical_and(i == 3, first_row))
        def _():
            s_leg1.wait_recv()
            s_leg2.start()

        @pl.when(i == LATE)
        def _():
            both([], n_tra, lambda cp: cp.start())
            pl.when(far_n)(n_far.start)
            pl.when(far_s)(s_far.start)
            both([s_cor], [n_cor], lambda cp: cp.start())

        @pl.when(i == 2)
        def _():
            for cp in (z_wide[0], z_col):
                cp.wait_recv()
            lax.fori_loop(0, 2, unpack, 0)
            shift_u(0)
            shift_v(3)
            pressure(4, all_rows, NR)

        momentum(1 + odd + later * (2 * odd - 1), 1, 2 * SUB)
        return 0

    lax.fori_loop(0, NT, middle_rows, 0)

    arrived(n_first + n_vel, s_first + s_vel + s_tra)

    def pressure_north(i, _):
        for odd in range(2):
            pressure(2 * i + odd, pl.ds(RO + NR, SUB), SUB)
        return 0
    lax.fori_loop(0, 2, pressure_north, 0)

    def force_corner(a, b, d):
        return remote(asend.at[pl.ds(a - WO, NH), :], abuf.at[0, 4, pl.ds(b, NH), :], dev(d, ocol))

    def force_rows(t, a, b, d):
        return remote(abuf.at[:, t, pl.ds(a, NH), :], abuf.at[:, t, pl.ds(b, NH), :], dev(d, col))

    def force_pair(t):
        return force_rows(t, n_src, n_dst, 1), force_rows(t, s_src, s_dst, -1)

    z_force = remote(asend, abuf.at[0, 4, pl.ds(WO, NR), :], dev(0, ocol))
    n_fcor, s_fcor = force_corner(n_src, n_dst, 1), force_corner(s_src, s_dst, -1)

    force = [force_pair(t) for t in range(NT)]
    n_force = [p[0] for p in force] + [n_fcor]
    s_force = [p[1] for p in force] + [s_fcor]

    def send_force(which):
        both([s_force[i] for i in which], [n_force[i] for i in which], lambda cp: cp.start())

    def ends(i, _):
        t = lax.rem(3 * i, 4)
        momentum(t, 0, at_south=True)
        momentum(t, 3, at_north=True)

        @pl.when(i == 1)
        def _():
            for j in range(4):
                asend[pl.ds(SUB * j, SUB), :] = paired(abuf, 0, 1, WO + SUB * j)
            z_force.start()
            send_force((0, 3, 4))

        @pl.when(i == 2)
        def _():
            send_force((2,))
        return 0

    lax.fori_loop(0, NT, ends, 0)
    send_force((1,))

    arrived(n_tra, [])

    def tracers(lt, j, height):
        west_of, east_of = movers(height)
        zero8, pick, keep = chooser(height)
        rc, rn, rs = pl.ds(RO + SUB * j, height), pl.ds(RO + 1 + SUB * j, height), pl.ds(RO - 1 + SUB * j, height)
        ro = pl.ds(SUB * j, height)
        t, right, left = lt, lax.rem(lt + 1, 5), lax.rem(lt + 4, 5)
        c0 = cnt[lt, rc, :]
        luw = jnp.minimum(c0, west_of(c0, cnt[left, rc, :]))
        lvs = jnp.minimum(c0, cnt[lt, rs, :])
        lu = lu_o[lt, ro, :]
        lv = lv_o[lt, ro, :]
        yt, ys = zero8, zero8
        for k in range(NL):
            here = c0 > k
            me = keep(lu > k, ub[t, k, rc, :])
            mw = keep(luw > k, uw_b[t, k, rc, :])
            mn = keep(lv > k, vb[t, k, rc, :])
            ms = keep(lvs > k, vb[t, k, rs, :])
            own = 2.0 - ((me - mw) + (mn - ms))

            def advect(buf):
                q = buf[t, k, rc, :]
                qe = east_of(q, buf[right, k, rc, :])
                qw = west_of(q, buf[left, k, rc, :])
                return (own * q + (mw * qw - me * qe)) + (ms * buf[t, k, rs, :] - mn * buf[t, k, rn, :])

            end = pick(here, DIFF_END[k], 0.5)
            fac = lax.select(c0 > k + 1, jnp.full_like(end, DIFF_IN[k]), end) if k < NL - 1 else end
            yt = (advect(tb) + keep(here, yt)) * fac
            ys = (advect(sb) + keep(here, ys)) * fac
            if k < NL - 1:
                tn_o[lt, k, ro, :] = yt
                sn_o[lt, k, ro, :] = ys
        xt, xs_ = zero8, zero8
        for k in reversed(range(NL)):
            xt = yt if k == NL - 1 else tn_o[lt, k, ro, :] + keep(c0 > k + 1, DIFF_IN[k] * xt)
            xs_ = ys if k == NL - 1 else sn_o[lt, k, ro, :] + keep(c0 > k + 1, DIFF_IN[k] * xs_)
            tn_o[lt, k, ro, :] = xt
            sn_o[lt, k, ro, :] = xs_

    def tracers_all(i, _):
        tracers(lax.rem(i, NT), T_TILES * (i // NT), T_TILES * SUB)
        return 0
    lax.fori_loop(0, 16 // T_TILES, tracers_all, 0)

    z_wide[1].wait_recv()
    z_force.wait_recv()
    pl.when(far_s)(n_far.wait_recv)
    pl.when(far_n)(s_far.wait_recv)
    pl.when(down)(n_leg2.wait_recv)
    pl.when(up)(s_leg2.wait_recv)
    arrived([n_cor] + n_force, [s_cor] + s_force)

    for cp in z_wide + [z_col, z_force]:
        cp.wait_send()
    both(s_first + s_vel + s_tra + [s_cor] + s_force, n_first + n_vel + n_tra + [n_cor] + n_force, lambda cp: cp.wait_send())
    pl.when(far_n)(n_far.wait_send)
    pl.when(far_s)(s_far.wait_send)
    pl.when(up)(n_leg1.wait_send)
    pl.when(down)(s_leg1.wait_send)
    pl.when(last_row)(n_leg2.wait_send)
    pl.when(first_row)(s_leg2.wait_send)


def finish_kernel(n_row, n_sub, w_ref,
                  us, vs, tn, sn, wide, abuf, lu, lv, hu_s, hv_s, mu_s, mv_s,
                  eta_o, tu_o, tv_o, u_o, v_o, t_o, s_o,
                  bu, bv, cfu, cfv, mku, mkv, tu, tv, xs, acu, acv, cu, cv, flat_b, ubuf, vbuf, sem):
    row = lax.axis_index('row')
    dtb = TIME_STEP / n_sub
    total_rows = float(n_row * NR)
    zero8 = jnp.zeros((SUB, LANE), F32)
    west_of, east_of = movers()
    copies = []

    def put(src, dst):
        cp = pltpu.make_async_copy(src, dst, sem.at[len(copies)])
        cp.start()
        copies.append(cp)

    for src, dst in ((tn, t_o), (sn, s_o)):
        for t in range(NT):
            put(src.at[t], dst.at[:, :, pl.ds(LANE * t, LANE)])

    def setup(i):
        base = SUB + SUB * i
        rows = pl.ds(base, SUB)
        rown = pl.ds(base + 1, SUB)
        first = row * NR + SUB * i - NR
        fu, fv = corio(first, total_rows)
        place = first + lax.broadcasted_iota(jnp.int32, (SUB, LANE), 0)
        inside = place >= 0
        wet_u = jnp.logical_and(inside, place < n_row * NR).astype(F32)
        wet_v = jnp.logical_and(inside, place < n_row * NR - 1).astype(F32)
        cfu[rows, :] = wet_u * ((0.25 * dtb) * fu)
        cfv[rows, :] = wet_v * ((0.25 * dtb) * fv)
        mku[rows, :] = wet_u
        mkv[rows, :] = wet_v
        for t in range(5):
            right = (t + 1) % 5
            d0 = wide[3, t, rows, :]
            scale = 0.5 * dtb * dtb * GRAVITY
            bu[t, rows, :] = wet_u * (scale * (d0 + east_of(d0, wide[3, right, rows, :])))
            bv[t, rows, :] = wet_v * (scale * (d0 + wide[3, t, rown, :]))
            tu[0, t, rows, :] = dtb * wide[2, t, rows, :]
            tv[0, t, rows, :] = dtb * wide[1, t, rows, :]

    for i in range(12):
        rows = pl.ds(SUB + SUB * i, SUB)
        for f in range(2):
            wide[f + 2, 4, rows, :] = pltpu.roll(wide[f, 4, rows, :], LANE // 2, 1)
        abuf[1, 4, rows, :] = pltpu.roll(abuf[0, 4, rows, :], LANE // 2, 1)
    for i in range(12):
        setup(i)
    for t in range(NT):
        acu[t] = jnp.zeros((NR, LANE), F32)
        acv[t] = jnp.zeros((NR, LANE), F32)

    def subcycle(n, cur, lo, hi, first=False):
        nxt = 1 - cur
        weight = w_ref[n] * (ONE / dtb)
        def eta_part(i):
            rows, rows_s = pl.ds(SUB + SUB * i, SUB), pl.ds(7 + SUB * i, SUB)
            u0 = [tu[cur, t, rows, :] for t in range(5)]
            v0 = [tv[cur, t, rows, :] for t in range(5)]
            vs = [tv[cur, t, rows_s, :] for t in range(5)]
            uw = [west_of(u0[t], u0[(t + 4) % 5]) for t in range(5)]
            u2 = [u0[t] + uw[t] for t in range(5)]
            es = [wide[0, t, rows, :] - ((u0[t] - uw[t]) + (v0[t] - vs[t])) for t in range(5)]
            for t in range(5):
                wide[0, t, rows, :] = es[t]
                xs[t, rows, :] = u2[t]

        def flow_part(i):
            rows, rows_n = pl.ds(SUB + SUB * i, SUB), pl.ds(9 + SUB * i, SUB)
            f_u, f_v = cfu[rows, :], cfv[rows, :]
            rows_s = pl.ds(7 + SUB * i, SUB)
            v0 = [tv[cur, t, rows, :] for t in range(5)]
            v2 = [v0[t] + tv[cur, t, rows_s, :] for t in range(5)]
            v4 = [v2[t] + east_of(v2[t], v2[(t + 1) % 5]) for t in range(5)]
            es = [wide[0, t, rows, :] for t in range(5)]
            for t in range(5):
                slope_u = east_of(es[t], es[(t + 1) % 5]) - es[t]
                slope_v = wide[0, t, rows_n, :] - es[t]
                u4 = xs[t, rows, :] + xs[t, rows_n, :]
                u_old, v_old = tu[cur, t, rows, :], tv[cur, t, rows, :]
                if first:
                    u_old = mku[rows, :] * u_old
                    v_old = mkv[rows, :] * v_old
                u_new = (u_old + abuf[0, t, rows, :]) + (f_u * v4[t] - bu[t, rows, :] * slope_u)
                v_new = (v_old + abuf[1, t, rows, :]) - (f_v * u4 + bv[t, rows, :] * slope_v)
                tu[nxt, t, rows, :] = u_new
                tv[nxt, t, rows, :] = v_new
                if 4 <= i < SUB and t < NT:
                    ro = pl.ds(SUB * (i - 4), SUB)
                    acu[t, ro, :] += weight * u_new
                    acv[t, ro, :] += weight * v_new

        for part in (eta_part, flow_part):
            for i in reversed(range(lo, hi)):
                part(i)

    def pairs(first_n, count, lo, hi):
        def body(i, _):
            n = first_n + 2 * i
            subcycle(n, 0, lo, hi)
            subcycle(n + 1, 1, lo, hi)
            return 0
        lax.fori_loop(0, count, body, 0)

    subcycle(0, 0, 0, 12, first=True)
    subcycle(1, 1, 0, 12)
    pairs(2, 2, 0, 12)
    pairs(6, 4, 1, 11)
    pairs(14, 4, 2, 10)
    pairs(22, 4, 3, 9)

    for t in range(NT):
        for j in range(4):
            rw = pl.ds(WO + SUB * j, SUB)
            ro = pl.ds(SUB * j, SUB)
            flat_b[0, t, ro, :] = wide[0, t, rw, :]
            flat_b[1, t, ro, :] = (ONE / dtb) * tu[0, t, rw, :]
            flat_b[2, t, ro, :] = (ONE / dtb) * tv[0, t, rw, :]
            cu[t, ro, :] = acu[t, ro, :] / hu_s[t, ro, :] - mu_s[t, ro, :]
            hv = hv_s[t, ro, :]
            cv[t, ro, :] = acv[t, ro, :] / hv - mv_s[t, ro, :]

    for f, dst in enumerate((eta_o, tu_o, tv_o)):
        for t in range(NT):
            put(flat_b.at[f, t], dst.at[:, pl.ds(LANE * t, LANE)])
    for lev, cor, src, buf, dst in ((lu, cu, us, ubuf, u_o), (lv, cv, vs, vbuf, v_o)):
        for t in range(NT):
            for j in range(4):
                ro = pl.ds(SUB * j, SUB)
                count = lev[t, ro, :]
                shift = cor[t, ro, :]
                for k in range(NL):
                    buf[t, k, ro, :] = jnp.where(count > k, (ONE / VISC_R) * src[t, k, ro, :] + shift, ZERO)
            put(buf.at[t], dst.at[:, :, pl.ds(LANE * t, LANE)])
    for cp in copies:
        cp.wait()


def solution(mesh):
    n_row = mesh.shape['row']

    def step(vel_u, vel_v, temperature, salinity, surf_eta, trans_u, trans_v, bottom_depth, level_count, avg_weights):
        n_sub = avg_weights.shape[0]
        hbm = pl.BlockSpec(memory_space=pltpu.HBM)
        vmem = pl.BlockSpec(memory_space=pltpu.VMEM)
        smem = pl.BlockSpec(memory_space=pltpu.SMEM)
        cube_v = pltpu.VMEM((NT, NL, NR, LANE), F32)
        flat_v = pltpu.VMEM((NT, NR, LANE), F32)
        wide1 = pltpu.VMEM((5, WR, LANE), F32)
        wide_v = pltpu.VMEM((4, 5, WR, LANE), F32)
        force_v = pltpu.VMEM((2, 5, WR, LANE), F32)
        sems = pltpu.SemaphoreType.DMA
        outs = [cube_v] * 4 + [wide_v, force_v] + [flat_v] * 6
        mids = pl.pallas_call(
            functools.partial(ocean_kernel, n_row, n_sub),
            out_shape=outs,
            in_specs=[hbm] * 9,
            out_specs=[vmem] * len(outs),
            scratch_shapes=[
                pltpu.VMEM((4, 5, NL, RO + NR + SUB, LANE), F32),
                pltpu.VMEM((5, NL, RO + NR + SUB, LANE), F32),
                pltpu.VMEM((NT, NL, RO + NR + SUB, LANE), F32),
                pltpu.VMEM((NT, NL, RO + NR + SUB, LANE), F32),
                pltpu.VMEM((2, 5, RO + NR + SUB, LANE), F32),
                pltpu.VMEM((4, NT, NH, LANE), F32),
                pltpu.VMEM((4, NR, LANE), F32),
                pltpu.VMEM((NT, NR, LANE), jnp.int32),
                pltpu.VMEM((4, 2, SUB, LANE), F32),
                pltpu.VMEM((4, 2, SUB, LANE), F32),
                pltpu.VMEM((NR, LANE), F32),
                sems((16,)), sems((24,)), sems((N_COPY,)), sems((N_COPY,)),
            ],
            compiler_params=pltpu.CompilerParams(collective_id=0, has_side_effects=True, vmem_limit_bytes=VMEM_MAIN),
            name='ocean',
        )(*[pltpu.with_memory_space_constraint(x, pltpu.HBM) for x in (vel_u, vel_v, temperature, salinity, surf_eta, trans_u, trans_v, bottom_depth, level_count)])
        cube = jax.ShapeDtypeStruct((NL, NR, NT * LANE), F32)
        flat = jax.ShapeDtypeStruct((NR, NT * LANE), F32)
        return pl.pallas_call(
            functools.partial(finish_kernel, n_row, n_sub),
            out_shape=[flat] * 3 + [cube] * 4,
            in_specs=[smem] + [vmem] * len(outs),
            out_specs=[hbm] * 7,
            scratch_shapes=[wide1] * 2 + [pltpu.VMEM((WR, LANE), F32)] * 4 + [force_v, force_v, wide1] + [flat_v] * 4 + [pltpu.VMEM((3, NT, NR, LANE), F32), cube_v, cube_v, sems((28,))],
            compiler_params=pltpu.CompilerParams(vmem_limit_bytes=VMEM_FINISH),
            name='finish',
        )(avg_weights, *mids)

    cube = P(None, 'row', 'col')
    flat = P('row', 'col')
    return jax.shard_map(step, mesh=mesh, in_specs=(cube, cube, cube, cube, flat, flat, flat, flat, flat, P()), out_specs=(flat, flat, flat, cube, cube, cube, cube), check_vma=False)
```
